128 devices in a mesh: gx: 8 (over x, core), gy: 16 (over y, z).
Axes of the slice: x: 4, y: 4, z: 4, core: 2. Of those that a mesh axis runs over, the one named last changes fastest.
Arguments:
- slot_tiles: int32 [128, 128], P(('gx', 'gy')), may hold values from -1 to 255, as said below
- owner_map: int32 [128], replicated, may hold values from 0 to 127, each once
- slot_depth: int32 [128, 128, 16, 128], P(('gx', 'gy')), may hold values from 0 to 1073741823
- slot_color: bfloat16 [128, 128, 16, 3, 128], P(('gx', 'gy')), may hold values from 0 to 1
Outputs:
- region_depth: int32 [128, 2, 16, 128], P(('gx', 'gy'))
- region_color: bfloat16 [128, 2, 16, 3, 128], P(('gx', 'gy'))
- thumbnail: float32 [128, 3, 64], replicated
The draws below stay inside these ranges and needn't reach their ends.
Inputs may be any that keep to these rules, and one draw needn't show every extreme that they name: `slot_tiles`: each rank's used slots name the tiles of one rectangle of at least 8 tile rows of the 16 x 16 tile grid, each once, in row-major order, followed by -1 in the unused slots; all ranks' rectangles contain a common region. `owner_map`: each rank owns exactly one region.
All inputs are finite; a program needn't handle non-finite values.
Results may differ from the reference program's by a relative error of at most 0.001.
Values may be sent and summed in bfloat16 or wider, within the bound.
A program may use at most 64 MiB of HBM per device.

```python
import jax
import jax.numpy as jnp
from jax import lax

TILE = 128
BAND = 16
TROWS = 16
TCOLS = 16
TILES = 256
SLOTS = 128
REGIONS = 128
THUMB = 64
DEVICES = 128


def box_tiles(key):
    keys = jax.random.split(jax.random.fold_in(key, 11), 9)
    focus_pair = jax.random.randint(keys[0], (), 0, TROWS // 2)
    focus_col = jax.random.randint(keys[1], (), 0, TCOLS)
    lowest = max(3, TROWS // 2)
    box_height = lowest + jax.random.randint(keys[2], (DEVICES,), 0, 1 << 20) % (TROWS - lowest + 1)
    widest = jnp.minimum(SLOTS // box_height, TCOLS)
    narrowing = jax.random.randint(keys[8], (DEVICES,), 0, 2)
    box_width = jnp.maximum(1, widest - narrowing)
    row_low = jnp.maximum(0, 2 * focus_pair + 2 - box_height)
    row_high = jnp.minimum(2 * focus_pair, TROWS - box_height)
    row_span = row_high - row_low + 1
    first_draw = jax.random.randint(keys[4], (DEVICES,), 0, 1 << 20) % row_span
    second_draw = jax.random.randint(keys[5], (DEVICES,), 0, 1 << 20) % row_span
    top_row = row_low + (first_draw + second_draw) // 2
    col_low = jnp.maximum(0, focus_col - box_width + 1)
    col_high = jnp.minimum(focus_col, TCOLS - box_width)
    col_span = col_high - col_low + 1
    third_draw = jax.random.randint(keys[6], (DEVICES,), 0, 1 << 20) % col_span
    fourth_draw = jax.random.randint(keys[7], (DEVICES,), 0, 1 << 20) % col_span
    left_col = col_low + (third_draw + fourth_draw) // 2
    slot_index = jnp.arange(SLOTS, dtype=jnp.int32)[None, :]
    inner_row = slot_index // box_width[:, None]
    inner_col = slot_index % box_width[:, None]
    is_live = slot_index < (box_height * box_width)[:, None]
    tile_ids = (top_row[:, None] + inner_row) * TCOLS + left_col[:, None] + inner_col
    return jnp.where(is_live, tile_ids, -1).astype(jnp.int32)


def draw_slot_tiles(key, part):
    return box_tiles(key)


def draw_slot_depth(key, part):
    tile_ids = box_tiles(key)
    keys = jax.random.split(jax.random.fold_in(key, 23), 3)
    surface = jax.random.randint(keys[0], (TILES, BAND, TILE), 0, 1073741823).astype(jnp.int32)
    safe_tile = jnp.where(tile_ids >= 0, tile_ids, 0).astype(jnp.int32)
    front = surface[safe_tile]
    coin = jax.random.randint(keys[1], (DEVICES, SLOTS, BAND, TILE), 0, 8)
    room = (1073741823 - front).astype(jnp.int32)
    raw_extra = jax.random.randint(keys[2], (DEVICES, SLOTS, BAND, TILE), 0, 1 << 30).astype(jnp.int32)
    extra = 1 + raw_extra % room
    return (front + jnp.where(coin == 0, 0, extra)).astype(jnp.int32)


def block_levels(own_key, extent, shards, least, top_value):
    factor_of, own = 1.0, jax.random.fold_in(own_key, 6)
    for position, parts in shards:
        steps = jnp.exp(jax.random.uniform(jax.random.fold_in(own, position), (parts,), jnp.float32, least / len(shards), top_value / len(shards)))
        factor_of = factor_of * jnp.repeat(steps, extent[position] // parts).reshape([-1 if axis == position else 1 for axis in range(len(extent))])
    return factor_of


def setup_inputs(seed: int = 0) -> dict:
    seeds = jax.random.split(jax.random.key(seed), 5)
    return {
        "slot_tiles": draw_slot_tiles(jax.random.fold_in(seeds[4], 71), 0),
        "owner_map": jax.random.permutation(seeds[1], REGIONS).astype(jnp.int32),
        "slot_depth": draw_slot_depth(jax.random.fold_in(seeds[4], 71), 0),
        "slot_color": jnp.clip(1.0 * jax.random.uniform(seeds[3], (DEVICES, SLOTS, BAND, 3, TILE), jnp.float32) ** block_levels(seeds[3], (DEVICES, SLOTS, BAND, 3, TILE), ((0, 128),), -0.2, 0.2), 0.0, 1.0).astype(jnp.bfloat16),
    }


far_depth = 1073741824


def reference(slot_tiles, owner_map, slot_depth, slot_color):
    tile_count = TROWS * TCOLS

    def place_rank(frame_state, rank_data):
        frame_depth, frame_color = frame_state
        rank_tiles, rank_depth, rank_color = rank_data
        gather_index = jnp.where(rank_tiles >= 0, rank_tiles, tile_count).astype(jnp.int32)
        current = frame_depth[gather_index]
        nearer = rank_depth < current
        new_depth = jnp.where(nearer, rank_depth, current)
        new_color = jnp.where(nearer[:, :, None, :], rank_color, frame_color[gather_index])
        return (frame_depth.at[gather_index].set(new_depth), frame_color.at[gather_index].set(new_color)), None

    start_depth = jnp.full((tile_count + 1, BAND, TILE), far_depth, jnp.int32)
    start_color = jnp.zeros((tile_count + 1, BAND, 3, TILE), jnp.bfloat16)
    final_state, unused = lax.scan(place_rank, (start_depth, start_color), (slot_tiles, slot_depth, slot_color))
    frame_depth = final_state[0][:tile_count]
    frame_color = final_state[1][:tile_count]
    by_region_depth = jnp.transpose(frame_depth.reshape(TROWS // 2, 2, TCOLS, BAND, TILE), (0, 2, 1, 3, 4)).reshape(REGIONS, 2, BAND, TILE)
    by_region_color = jnp.transpose(frame_color.reshape(TROWS // 2, 2, TCOLS, BAND, 3, TILE), (0, 2, 1, 3, 4, 5)).reshape(REGIONS, 2, BAND, 3, TILE)
    inverse = jnp.zeros((REGIONS,), jnp.int32).at[owner_map].set(jnp.arange(REGIONS, dtype=jnp.int32))
    region_depth = by_region_depth[inverse]
    region_color = by_region_color[inverse]
    block_means = by_region_color.astype(jnp.float32).reshape(REGIONS, 2, BAND // 8, 8, 3, TILE // 8, 8).mean(axis=(3, 6))
    thumbnail = jnp.transpose(block_means, (0, 3, 1, 2, 4)).reshape(REGIONS, 3, THUMB)
    return region_depth, region_color, thumbnail
```

```python
import jax
import jax.numpy as jnp
import numpy as np
from jax import lax
from jax.experimental import pallas as pl
from jax.experimental.pallas import tpu as pltpu
from jax.sharding import PartitionSpec as P

MESH = pl.DeviceIdType.MESH
FAR = 1073741824
ORDER = ((0, 1, 2), (1, 2, 0), (2, 0, 1))
STRIDE = (32, 4, 1)
COUNT = (3, 3, 2)
BASE = (0, 48, 96)
CLASS = ((0, 0, 3), (1, 1, 3), (2, 2))
HALF = ((0, 1, 0), (0, 1, 1), (0, 1))
CHUNKS = tuple((stream, off) for off in (1, 3, 2, 0) for stream in range(3))


def tile_places():
    places = np.zeros((1, 128), np.int32)
    for stream in range(3):
        first, second, third = ORDER[stream]
        count = COUNT[stream]
        for i in range(4):
            for j in range(4):
                for t in range(count):
                    at = [0, 0, 0]
                    at[first], at[second] = i, j
                    at[third] = (CLASS[stream][t] - i - j) % 4
                    owner = sum(a * s for a, s in zip(at, STRIDE))
                    places[0, BASE[stream] + (i * 4 + j) * count + t] = 2 * owner + HALF[stream][t]
    return places


def pick(mask, new, old):
    return jnp.where(mask[None], new, old)


def kernel(
    tiles_ref, owner_ref, place_ref, depth_hbm, color_hbm,
    depth_out, color_out, thumbs_out,
    in_d, in_c, table_v, table, send_d, send_c, got_d, got_c,
    own_d, own_c, one_d, one_c, out1_d, out1_c, two_d, two_c, out2_d, out2_c,
    last_d, last_c, thumbs,
    load_sem, table_sem, core_send, core_recv, send1, recv1, send2, recv2, send3, recv3,
    thumb_send, thumb_recv, store_sem,
):
    gx, gy = lax.axis_index("gx"), lax.axis_index("gy")
    core = lax.rem(gx, 2)
    at = (lax.div(gx, 2), lax.div(gy, 4), lax.rem(gy, 4))
    me = gx * 16 + gy

    def device(x, y, z, c=core):
        return (2 * x + c, 4 * y + z)

    def peer(axis, off):
        moved = [lax.rem(a + off, 4) if k == axis else a for k, a in enumerate(at)]
        return device(*moved)

    partner = device(*at, c=1 - core)

    loads = [
        pltpu.make_async_copy(depth_hbm, in_d.at[pl.ds(0, 128)], load_sem.at[0]),
        pltpu.make_async_copy(color_hbm, in_c.at[pl.ds(0, 128)], load_sem.at[1]),
    ]
    for load in loads:
        load.start()
    barrier = pltpu.get_barrier_semaphore()
    pl.semaphore_signal(barrier, inc=1, device_id=partner, device_id_type=MESH)
    for axis in range(3):
        for off in (1, 2, 3):
            pl.semaphore_signal(barrier, inc=1, device_id=peer(axis, off), device_id_type=MESH)

    in_d[128] = jnp.full((16, 128), FAR, jnp.int32)
    in_c[128] = jnp.zeros((3, 16, 128), jnp.bfloat16)
    tiles = tiles_ref[...]
    live = tiles >= 0
    row = lax.shift_right_arithmetic(tiles, 4)
    region = lax.shift_right_arithmetic(row, 1) * 16 + (tiles & 15)
    down = lax.broadcasted_iota(jnp.int32, (128, 128), 0)
    owner_down = jnp.transpose(jnp.broadcast_to(owner_ref[...], (128, 128)))
    owner = jnp.sum(jnp.where(down == region, owner_down, 0), axis=0, keepdims=True)
    place = jnp.where(live, 2 * owner + (row & 1), -1)
    place_down = jnp.transpose(jnp.broadcast_to(place, (128, 128)))
    for c in range(2):
        hit = place_down == place_ref[...] + 32 * c
        table_v[c : c + 1, :] = jnp.min(jnp.where(hit, down, 128), axis=0, keepdims=True)
    to_table = pltpu.make_async_copy(table_v, table, table_sem)
    to_table.start()
    to_table.wait()
    for load in loads:
        load.wait()
    pl.semaphore_wait(barrier, 10)

    def remote(src, dst, sends, recvs, index, target):
        copy = pltpu.make_async_remote_copy(
            src_ref=src, dst_ref=dst, send_sem=sends.at[index], recv_sem=recvs.at[index],
            device_id=target, device_id_type=MESH,
        )
        copy.start()
        return copy

    def chunk(stream, off):
        size = 4 * COUNT[stream]
        return BASE[stream] + lax.rem(at[ORDER[stream][0]] + off, 4) * size, size

    core_copies = []
    for n, (stream, off) in enumerate(CHUNKS):
        start, size = chunk(stream, off)

        def pack(t, carry):
            q = start + t
            slot = table[1 - core, q]
            send_d[q] = in_d[slot]
            send_c[q] = in_c[slot]
            return carry

        lax.fori_loop(0, size, pack, 0, unroll=4)
        part = pl.ds(start, size)
        core_copies.append((
            remote(send_d.at[part], got_d.at[part], core_send, core_recv, 2 * n, partner),
            remote(send_c.at[part], got_c.at[part], core_send, core_recv, 2 * n + 1, partner),
        ))

    copies1 = {}
    for n, (stream, off) in enumerate(CHUNKS):
        start, size = chunk(stream, off)
        for copy in core_copies[n]:
            copy.wait_recv()
        to_d, to_c = (own_d, own_c) if off else (one_d, one_c)

        def meet(t, carry):
            q = start + t
            slot = table[core, q]
            mine = (in_d[slot] - FAR) * 2 + core
            other = (got_d[q] - FAR) * 2 + (1 - core)
            nearer = other < mine
            to_d[q] = jnp.where(nearer, other, mine)
            to_c[q] = pick(nearer, got_c[q], in_c[slot])
            return carry

        lax.fori_loop(0, size, meet, 0, unroll=2)
        if off:
            axis = ORDER[stream][0]
            src = pl.ds(start, size)
            dst = pl.ds(BASE[stream] + at[axis] * size, size)
            index = 2 * (3 * stream + off - 1)
            copies1[stream, off] = (
                remote(own_d.at[src], one_d.at[dst], send1, recv1, index, peer(axis, off)),
                remote(own_c.at[src], one_c.at[dst], send1, recv1, index + 1, peer(axis, off)),
            )

    copies2 = {}
    for stream in range(3):
        first, second, third = ORDER[stream]
        count, base = COUNT[stream], BASE[stream]
        for off in (1, 2, 3):
            for copy in copies1[stream, off]:
                copy.wait_recv()
        rest = at[second] * STRIDE[second] + at[third] * STRIDE[third]
        for off in (1, 2, 3, 0):
            to = lax.rem(at[second] + off, 4)
            if off:
                to_d, to_c, into = out1_d, out1_c, base // 4 + (off - 1) * count
            else:
                to_d, to_c, into = two_d, two_c, base // 4 + at[second] * count

            def join(t, carry):
                key = tag = color = best = None
                for src in range(4):
                    q = base + src * 4 * count + to * count + t
                    k = one_d[q]
                    depth = lax.shift_right_arithmetic(k, 1)
                    order = depth if first == 0 else k
                    rank = rest + src * STRIDE[first] + (k & 1) * 16
                    if src == 0:
                        key, best, tag, color = order, depth, rank, one_c[q]
                    else:
                        nearer = order < key
                        key = jnp.where(nearer, order, key)
                        best = jnp.where(nearer, depth, best)
                        tag = jnp.where(nearer, rank, tag)
                        color = pick(nearer, one_c[q], color)
                to_d[into + t] = best
                to_c[into + t, 0:3] = color
                to_c[into + t, 3] = tag.astype(jnp.float32).astype(jnp.bfloat16)
                return carry

            lax.fori_loop(0, count, join, 0)
            if off:
                src = pl.ds(into, count)
                dst = pl.ds(base // 4 + at[second] * count, count)
                index = 2 * (3 * stream + off - 1)
                copies2[stream, off] = (
                    remote(out1_d.at[src], two_d.at[dst], send2, recv2, index, peer(second, off)),
                    remote(out1_c.at[src], two_c.at[dst], send2, recv2, index + 1, peer(second, off)),
                )

    def closer(depth, color, best, kept):
        tag, old = color[3].astype(jnp.float32), kept[3].astype(jnp.float32)
        nearer = (depth < best) | ((depth == best) & (tag < old))
        return jnp.where(nearer, depth, best), pick(nearer, color, kept)

    for stream in range(3):
        count, base = COUNT[stream], BASE[stream] // 4
        for off in (1, 2, 3):
            for copy in copies2[stream, off]:
                copy.wait_recv()
        for t in range(count):
            best, kept = two_d[base + t], two_c[base + t]
            for src in (1, 2, 3):
                q = base + src * count + t
                best, kept = closer(two_d[q], two_c[q], best, kept)
            k = 2 * CLASS[stream][t] + HALF[stream][t]
            out2_d[k] = best
            out2_c[k] = kept

    x, y, z = at
    mine = lax.rem(x + y + z, 4)
    copies3 = {}
    for off in (1, 2, 3):
        theirs = lax.rem(mine + off, 4)
        for half in range(2):
            along_z = (theirs == 0) | ((theirs == 3) & (half == 0))
            along_y = theirs == 2
            along_x = (theirs == 1) | ((theirs == 3) & (half == 1))
            target = device(
                lax.rem(x + jnp.where(along_x, off, 0), 4),
                lax.rem(y + jnp.where(along_y, off, 0), 4),
                lax.rem(z + jnp.where(along_z, off, 0), 4),
            )
            k = 2 * theirs + half
            slot = 3 * half + off - 1
            copies3[half, off] = (
                remote(out2_d.at[k], last_d.at[slot], send3, recv3, 2 * slot, target),
                remote(out2_c.at[k], last_c.at[slot], send3, recv3, 2 * slot + 1, target),
            )

    sums = []
    for half in range(2):
        best, kept = out2_d[2 * mine + half], out2_c[2 * mine + half]
        for off in (1, 2, 3):
            for copy in copies3[half, off]:
                copy.wait_recv()
            slot = 3 * half + off - 1
            best, kept = closer(last_d[slot], last_c[slot], best, kept)
        depth_out[half] = best + FAR
        color_out[half] = kept[0:3]
        sums.append(jnp.sum(kept[0:3].astype(jnp.float32).reshape(3, 2, 8, 128), axis=2))
    rows = jnp.concatenate(
        [s for c in range(3) for s in (sums[0][c], sums[1][c])] + [jnp.zeros((4, 128), jnp.float32)], axis=0
    )
    lane_down = lax.broadcasted_iota(jnp.int32, (128, 128), 0)
    lane = lax.broadcasted_iota(jnp.int32, (128, 128), 1)
    spread = jnp.where(lax.shift_right_logical(lane_down, 3) == (lane & 15), 1.0 / 64, 0.0)
    means = jnp.dot(rows, spread, precision=lax.Precision.HIGHEST, preferred_element_type=jnp.float32)
    line = lax.broadcasted_iota(jnp.int32, (16, 128), 0) & 7
    group = lax.shift_right_logical(lax.broadcasted_iota(jnp.int32, (16, 128), 1), 4)
    thumbs[me] = jnp.sum(jnp.where(line == group, means, 0.0).reshape(2, 8, 128), axis=1)

    def tell(i, carry):
        other = lax.rem(me + i, 128)
        pltpu.make_async_remote_copy(
            src_ref=thumbs.at[me], dst_ref=thumbs.at[me], send_sem=thumb_send, recv_sem=thumb_recv,
            device_id=(lax.div(other, 16), lax.rem(other, 16)), device_id_type=MESH,
        ).start()
        return carry

    lax.fori_loop(1, 128, tell, 0)
    for group_of in (core_copies, copies1.values(), copies2.values(), copies3.values()):
        for pair in group_of:
            for copy in pair:
                copy.wait_send()
    most = thumbs.at[pl.ds(0, 127)]
    pltpu.make_async_copy(most, most, thumb_recv).wait()
    pltpu.make_async_copy(most, most, thumb_send).wait()
    thumbs_out[...] = thumbs[...]


def shards(slot_tiles, owner_map, slot_depth, slot_color):
    i32, bf16 = jnp.int32, jnp.bfloat16
    vmem = pl.BlockSpec(memory_space=pltpu.VMEM)
    anywhere = pl.BlockSpec(memory_space=pl.ANY)
    dma = pltpu.SemaphoreType.DMA
    scratch = [
        pltpu.VMEM((129, 16, 128), i32), pltpu.VMEM((129, 3, 16, 128), bf16),
        pltpu.VMEM((2, 128), i32), pltpu.SMEM((2, 128), i32),
    ]
    for tiles, channels in ((128, 3), (128, 3), (128, 3), (128, 3), (32, 4), (32, 4), (8, 4), (6, 4)):
        scratch += [pltpu.VMEM((tiles, 16, 128), i32), pltpu.VMEM((tiles, channels, 16, 128), bf16)]
    scratch += [pltpu.VMEM((128, 2, 128), jnp.float32), dma((2,)), dma]
    scratch += [dma((24,)), dma((24,)), dma((18,)), dma((18,)), dma((18,)), dma((18,)), dma((12,)), dma((12,))]
    scratch += [dma, dma, dma]
    depth, color, thumbs = pl.pallas_call(
        kernel,
        out_shape=(
            jax.ShapeDtypeStruct((2, 16, 128), i32),
            jax.ShapeDtypeStruct((2, 3, 16, 128), bf16),
            jax.ShapeDtypeStruct((128, 2, 128), jnp.float32),
        ),
        in_specs=[vmem, vmem, vmem, anywhere, anywhere],
        out_specs=(vmem, vmem, vmem),
        scratch_shapes=scratch,
        compiler_params=pltpu.CompilerParams(collective_id=0, has_side_effects=True),
        name="composite",
    )(
        slot_tiles,
        owner_map[None],
        jnp.asarray(tile_places()),
        slot_depth[0],
        jnp.swapaxes(slot_color[0], 1, 2),
    )
    thumbnail = thumbs.reshape(128, 256)[:, :192][owner_map].reshape(128, 3, 64)
    return depth[None], jnp.swapaxes(color, 1, 2)[None], thumbnail


def solution(mesh):
    ranks = ("gx", "gy")
    return jax.shard_map(
        shards,
        mesh=mesh,
        in_specs=(P(ranks, None), P(), P(ranks, None, None, None), P(ranks, None, None, None, None)),
        out_specs=(P(ranks, None, None, None), P(ranks, None, None, None, None), P()),
        check_vma=False,
    )
```

```python
import jax
import jax.numpy as jnp
import numpy as np
from jax import lax
from jax.experimental import pallas as pl
from jax.experimental.pallas import tpu as pltpu
from jax.sharding import PartitionSpec as P

MESH = pl.DeviceIdType.MESH
FAR = 1073741824
ORDER = ((0, 1, 2), (1, 2, 0), (2, 0, 1))
STRIDE = (32, 4, 1)
COUNT = (3, 3, 2)
BASE = (0, 48, 96)
CLASS = ((0, 0, 3), (1, 1, 3), (2, 2))
HALF = ((0, 1, 0), (0, 1, 1), (0, 1))
CHUNKS = tuple((stream, off) for off in (1, 3, 2, 0) for stream in range(3))
FAR_FIRST = sorted(np.ndindex(4, 4, 4), key=lambda d: -sum(min(a, 4 - a) for a in d))


def tile_places():
    places = np.zeros((1, 128), np.int32)
    for stream in range(3):
        first, second, third = ORDER[stream]
        count = COUNT[stream]
        for i in range(4):
            for j in range(4):
                for t in range(count):
                    at = [0, 0, 0]
                    at[first], at[second] = i, j
                    at[third] = (CLASS[stream][t] - i - j) % 4
                    owner = sum(a * s for a, s in zip(at, STRIDE))
                    places[0, BASE[stream] + (j * 4 + i) * count + t] = 2 * owner + HALF[stream][t]
    return places


def pick(mask, new, old):
    return jnp.where(mask[None], new, old)


def kernel(
    tiles_ref, owner_ref, place_ref, depth_hbm, color_hbm,
    depth_out, color_out, thumbs_out,
    in_d, in_c, table_v, table, send_d, send_c, got_d, got_c,
    own_d, own_c, one_d, one_c, out1_d, out1_c, two_d, two_c, out2_d, out2_c,
    last_d, last_c, thumbs,
    load_sem, table_sem, core_send, core_recv, send1, recv1, send2, recv2, send3, recv3,
    thumb_send, thumb_recv, store_sem,
):
    gx, gy = lax.axis_index("gx"), lax.axis_index("gy")
    core = lax.rem(gx, 2)
    at = (lax.div(gx, 2), lax.div(gy, 4), lax.rem(gy, 4))
    me = gx * 16 + gy

    def device(x, y, z, c=core):
        return (2 * x + c, 4 * y + z)

    def peer(axis, off):
        moved = [lax.rem(a + off, 4) if k == axis else a for k, a in enumerate(at)]
        return device(*moved)

    partner = device(*at, c=1 - core)

    loads = [
        pltpu.make_async_copy(depth_hbm, in_d.at[pl.ds(0, 128)], load_sem.at[0]),
        pltpu.make_async_copy(color_hbm, in_c.at[pl.ds(0, 128)], load_sem.at[1]),
    ]
    for load in loads:
        load.start()
    barrier = pltpu.get_barrier_semaphore()
    pl.semaphore_signal(barrier, inc=1, device_id=partner, device_id_type=MESH)
    for axis in range(3):
        for off in (1, 2, 3):
            pl.semaphore_signal(barrier, inc=1, device_id=peer(axis, off), device_id_type=MESH)

    in_d[128] = jnp.full((16, 128), FAR, jnp.int32)
    in_c[128] = jnp.zeros((3, 16, 128), jnp.bfloat16)
    tiles = tiles_ref[...]
    live = tiles >= 0
    row = lax.shift_right_arithmetic(tiles, 4)
    region = lax.shift_right_arithmetic(row, 1) * 16 + (tiles & 15)
    down = lax.broadcasted_iota(jnp.int32, (128, 128), 0)
    owner_down = jnp.transpose(jnp.broadcast_to(owner_ref[...], (128, 128)))
    owner = jnp.sum(jnp.where(down == region, owner_down, 0), axis=0, keepdims=True)
    place = jnp.where(live, 2 * owner + (row & 1), -1)
    place_down = jnp.transpose(jnp.broadcast_to(place, (128, 128)))
    for c in range(2):
        hit = place_down == place_ref[...] + 32 * c
        table_v[c : c + 1, :] = jnp.min(jnp.where(hit, down, 128), axis=0, keepdims=True)
    to_table = pltpu.make_async_copy(table_v, table, table_sem)
    to_table.start()
    to_table.wait()
    for load in loads:
        load.wait()
    pl.semaphore_wait(barrier, 10)

    def remote(src, dst, sends, recvs, index, target):
        copy = pltpu.make_async_remote_copy(
            src_ref=src, dst_ref=dst, send_sem=sends.at[index], recv_sem=recvs.at[index],
            device_id=target, device_id_type=MESH,
        )
        copy.start()
        return copy

    def chunk(stream, off):
        size = 4 * COUNT[stream]
        return BASE[stream] + lax.rem(at[ORDER[stream][1]] + off, 4) * size, size

    core_copies = []
    for n, (stream, off) in enumerate(CHUNKS):
        start, size = chunk(stream, off)

        def pack(t, carry):
            q = start + t
            slot = table[1 - core, q]
            send_d[q] = in_d[slot]
            send_c[q] = in_c[slot]
            return carry

        lax.fori_loop(0, size, pack, 0, unroll=4)
        part = pl.ds(start, size)
        core_copies.append((
            remote(send_d.at[part], got_d.at[part], core_send, core_recv, 2 * n, partner),
            remote(send_c.at[part], got_c.at[part], core_send, core_recv, 2 * n + 1, partner),
        ))

    copies1 = {}
    for n, (stream, off) in enumerate(CHUNKS):
        start, size = chunk(stream, off)
        axis, count = ORDER[stream][0], COUNT[stream]
        for copy in core_copies[n]:
            copy.wait_recv()
        for step in (1, 3, 2, 0):
            first = start + lax.rem(at[axis] + step, 4) * count
            to_d, to_c = (own_d, own_c) if step else (one_d, one_c)

            def meet(t, carry):
                q = first + t
                slot = table[core, q]
                mine = (in_d[slot] - FAR) * 2 + core
                other = (got_d[q] - FAR) * 2 + (1 - core)
                nearer = other < mine
                to_d[q] = jnp.where(nearer, other, mine)
                to_c[q] = pick(nearer, got_c[q], in_c[slot])
                return carry

            lax.fori_loop(0, count, meet, 0, unroll=True)
            if step:
                src = pl.ds(first, count)
                dst = pl.ds(start + at[axis] * count, count)
                index = 2 * (3 * n + step - 1)
                copies1[n, step] = (
                    remote(own_d.at[src], one_d.at[dst], send1, recv1, index, peer(axis, step)),
                    remote(own_c.at[src], one_c.at[dst], send1, recv1, index + 1, peer(axis, step)),
                )

    copies2 = {}
    for n, (stream, off) in enumerate(CHUNKS):
        start, size = chunk(stream, off)
        first, second, third = ORDER[stream]
        count, base = COUNT[stream], BASE[stream] // 4
        for step in (1, 3, 2):
            for copy in copies1[n, step]:
                copy.wait_recv()
        rest = at[second] * STRIDE[second] + at[third] * STRIDE[third]
        if off:
            to_d, to_c, into = out1_d, out1_c, base + (off - 1) * count
        else:
            to_d, to_c, into = two_d, two_c, base + at[second] * count

        def join(t, carry):
            key = tag = color = best = None
            for src in range(4):
                q = start + src * count + t
                k = one_d[q]
                depth = lax.shift_right_arithmetic(k, 1)
                order = depth if first == 0 else k
                rank = rest + src * STRIDE[first] + (k & 1) * 16
                if src == 0:
                    key, best, tag, color = order, depth, rank, one_c[q]
                else:
                    nearer = order < key
                    key = jnp.where(nearer, order, key)
                    best = jnp.where(nearer, depth, best)
                    tag = jnp.where(nearer, rank, tag)
                    color = pick(nearer, one_c[q], color)
            to_d[into + t] = best
            to_c[into + t, 0:3] = color
            to_c[into + t, 3] = tag.astype(jnp.float32).astype(jnp.bfloat16)
            return carry

        lax.fori_loop(0, count, join, 0)
        if off:
            src = pl.ds(into, count)
            dst = pl.ds(base + at[second] * count, count)
            index = 2 * (3 * stream + off - 1)
            copies2[stream, off] = (
                remote(out1_d.at[src], two_d.at[dst], send2, recv2, index, peer(second, off)),
                remote(out1_c.at[src], two_c.at[dst], send2, recv2, index + 1, peer(second, off)),
            )

    def closer(depth, color, best, kept):
        tag, old = color[3].astype(jnp.float32), kept[3].astype(jnp.float32)
        nearer = (depth < best) | ((depth == best) & (tag < old))
        return jnp.where(nearer, depth, best), pick(nearer, color, kept)

    for stream in range(3):
        count, base = COUNT[stream], BASE[stream] // 4
        for off in (1, 2, 3):
            for copy in copies2[stream, off]:
                copy.wait_recv()
        for t in range(count):
            best, kept = two_d[base + t], two_c[base + t]
            for src in (1, 2, 3):
                q = base + src * count + t
                best, kept = closer(two_d[q], two_c[q], best, kept)
            k = 2 * CLASS[stream][t] + HALF[stream][t]
            out2_d[k] = best
            out2_c[k] = kept

    x, y, z = at
    mine = lax.rem(x + y + z, 4)
    copies3 = {}
    for off in (1, 2, 3):
        theirs = lax.rem(mine + off, 4)
        for half in range(2):
            along_z = (theirs == 0) | ((theirs == 3) & (half == 0))
            along_y = theirs == 2
            along_x = (theirs == 1) | ((theirs == 3) & (half == 1))
            target = device(
                lax.rem(x + jnp.where(along_x, off, 0), 4),
                lax.rem(y + jnp.where(along_y, off, 0), 4),
                lax.rem(z + jnp.where(along_z, off, 0), 4),
            )
            k = 2 * theirs + half
            slot = 3 * half + off - 1
            copies3[half, off] = (
                remote(out2_d.at[k], last_d.at[slot], send3, recv3, 2 * slot, target),
                remote(out2_c.at[k], last_c.at[slot], send3, recv3, 2 * slot + 1, target),
            )

    sums = []
    for half in range(2):
        best, kept = out2_d[2 * mine + half], out2_c[2 * mine + half]
        for off in (1, 2, 3):
            for copy in copies3[half, off]:
                copy.wait_recv()
            slot = 3 * half + off - 1
            best, kept = closer(last_d[slot], last_c[slot], best, kept)
        depth_out[half] = best + FAR
        color_out[half] = kept[0:3]
        sums.append(jnp.sum(kept[0:3].astype(jnp.float32).reshape(3, 2, 8, 128), axis=2))
    rows = jnp.concatenate(
        [s for c in range(3) for s in (sums[0][c], sums[1][c])] + [jnp.zeros((4, 128), jnp.float32)], axis=0
    )
    lane_down = lax.broadcasted_iota(jnp.int32, (128, 128), 0)
    lane = lax.broadcasted_iota(jnp.int32, (128, 128), 1)
    spread = jnp.where(lax.shift_right_logical(lane_down, 3) == (lane & 15), 1.0 / 64, 0.0)
    means = jnp.dot(rows, spread, precision=lax.Precision.HIGHEST, preferred_element_type=jnp.float32)
    line = lax.broadcasted_iota(jnp.int32, (16, 128), 0) & 7
    group = lax.shift_right_logical(lax.broadcasted_iota(jnp.int32, (16, 128), 1), 4)
    thumbs[me] = jnp.sum(jnp.where(line == group, means, 0.0).reshape(2, 8, 128), axis=1)

    around = [[lax.rem(a + off, 4) for off in range(4)] for a in at]
    across = [[2 * a + c for a in around[0]] for c in (core, 1 - core)]
    along = [[4 * b + c for c in around[2]] for b in around[1]]
    for dx, dy, dz in FAR_FIRST:
        for other in range(2):
            if dx or dy or dz or other:
                pltpu.make_async_remote_copy(
                    src_ref=thumbs.at[me], dst_ref=thumbs.at[me], send_sem=thumb_send, recv_sem=thumb_recv,
                    device_id=(across[other][dx], along[dy][dz]), device_id_type=MESH,
                ).start()
    for group_of in (core_copies, copies1.values(), copies2.values(), copies3.values()):
        for pair in group_of:
            for copy in pair:
                copy.wait_send()
    most = thumbs.at[pl.ds(0, 127)]
    pltpu.make_async_copy(most, most, thumb_recv).wait()
    pltpu.make_async_copy(most, most, thumb_send).wait()
    thumbs_out[...] = thumbs[...]


def settle(owner_ref, depth_ref, color_ref, thumbs_ref, depth_out, color_out, thumbs_out):
    depth_out[...] = depth_ref[...]
    color_out[...] = color_ref[...]
    held = lax.broadcasted_iota(jnp.int32, (128, 128), 0) == owner_ref[...]
    chosen = jnp.where(held, 1.0, 0.0)
    for row, size in ((0, 128), (1, 64)):
        thumbs_out[128 * row : 128 * row + size] = lax.dot_general(
            thumbs_ref[:, row, 0:size], chosen, (((0,), (0,)), ((), ())),
            precision=lax.Precision.HIGHEST, preferred_element_type=jnp.float32,
        )


def shards(slot_tiles, owner_map, slot_depth, slot_color):
    i32, bf16 = jnp.int32, jnp.bfloat16
    vmem = pl.BlockSpec(memory_space=pltpu.VMEM)
    anywhere = pl.BlockSpec(memory_space=pl.ANY)
    dma = pltpu.SemaphoreType.DMA
    scratch = [
        pltpu.VMEM((129, 16, 128), i32), pltpu.VMEM((129, 3, 16, 128), bf16),
        pltpu.VMEM((2, 128), i32), pltpu.SMEM((2, 128), i32),
    ]
    for tiles, channels in ((128, 3), (128, 3), (128, 3), (128, 3), (32, 4), (32, 4), (8, 4), (6, 4)):
        scratch += [pltpu.VMEM((tiles, 16, 128), i32), pltpu.VMEM((tiles, channels, 16, 128), bf16)]
    scratch += [pltpu.VMEM((128, 2, 128), jnp.float32), dma((2,)), dma]
    scratch += [dma((24,)), dma((24,)), dma((72,)), dma((72,)), dma((18,)), dma((18,)), dma((12,)), dma((12,))]
    scratch += [dma, dma, dma]
    depth, color, thumbs = pl.pallas_call(
        kernel,
        out_shape=(
            pltpu.VMEM((2, 16, 128), i32),
            pltpu.VMEM((2, 3, 16, 128), bf16),
            pltpu.VMEM((128, 2, 128), jnp.float32),
        ),
        in_specs=[vmem, vmem, vmem, anywhere, anywhere],
        out_specs=(vmem, vmem, vmem),
        scratch_shapes=scratch,
        compiler_params=pltpu.CompilerParams(collective_id=0, has_side_effects=True),
        name="composite",
    )(
        slot_tiles,
        owner_map[None],
        jnp.asarray(tile_places()),
        slot_depth[0],
        jnp.swapaxes(slot_color[0], 1, 2),
    )
    depth, color, thumbs = pl.pallas_call(
        settle,
        out_shape=(
            jax.ShapeDtypeStruct((2, 16, 128), i32),
            jax.ShapeDtypeStruct((2, 3, 16, 128), bf16),
            jax.ShapeDtypeStruct((192, 128), jnp.float32),
        ),
        in_specs=[vmem] * 4,
        out_specs=(vmem, vmem, vmem),
        compiler_params=pltpu.CompilerParams(vmem_limit_bytes=8 << 20),
        name="settle",
    )(owner_map[None], depth, color, thumbs)
    thumbnail = jnp.transpose(thumbs.reshape(3, 64, 128), (2, 0, 1))
    return depth[None], jnp.swapaxes(color, 1, 2)[None], thumbnail


def solution(mesh):
    ranks = ("gx", "gy")
    return jax.shard_map(
        shards,
        mesh=mesh,
        in_specs=(P(ranks, None), P(), P(ranks, None, None, None), P(ranks, None, None, None, None)),
        out_specs=(P(ranks, None, None, None), P(ranks, None, None, None, None), P()),
        check_vma=False,
    )
```

```python
import jax
import jax.numpy as jnp
import numpy as np
from jax import lax
from jax.experimental import pallas as pl
from jax.experimental.pallas import tpu as pltpu
from jax.sharding import PartitionSpec as P

MESH = pl.DeviceIdType.MESH
FAR = 1073741824
ORDER = ((0, 2, 1), (1, 2, 0), (2, 0, 1))
STRIDE = (32, 4, 1)
COUNT = (3, 3, 2)
BASE = (0, 48, 96)
CLASS = ((0, 0, 3), (1, 1, 3), (2, 2))
HALF = ((0, 1, 0), (0, 1, 1), (0, 1))
CHUNKS = tuple((stream, off) for off in (1, 3, 2, 0) for stream in range(3))
FAR_FIRST = sorted(np.ndindex(4, 4, 4), key=lambda d: -sum(min(a, 4 - a) for a in d))


def tile_places():
    places = np.zeros((1, 128), np.int32)
    for stream in range(3):
        first, second, third = ORDER[stream]
        count = COUNT[stream]
        for i in range(4):
            for j in range(4):
                for t in range(count):
                    at = [0, 0, 0]
                    at[first], at[second] = i, j
                    at[third] = (CLASS[stream][t] - i - j) % 4
                    owner = sum(a * s for a, s in zip(at, STRIDE))
                    places[0, BASE[stream] + (j * 4 + i) * count + t] = 2 * owner + HALF[stream][t]
    return places


def pick(mask, new, old):
    return jnp.where(mask[None], new, old)


def kernel(
    tiles_ref, owner_ref, place_ref, depth_hbm, color_hbm,
    depth_out, color_out, thumbs_out,
    in_d, in_c, table_v, table, send_d, send_c, got_d, got_c,
    own_d, own_c, one_d, one_c, out1_d, out1_c, two_d, two_c, out2_d, out2_c,
    last_d, last_c, thumbs,
    load_sem, table_sem, core_send, core_recv, send1, recv1, send2, recv2, send3, recv3,
    thumb_send, thumb_recv,
):
    gx, gy = lax.axis_index("gx"), lax.axis_index("gy")
    core = lax.rem(gx, 2)
    at = (lax.div(gx, 2), lax.div(gy, 4), lax.rem(gy, 4))
    me = gx * 16 + gy

    def device(x, y, z, c=core):
        return (2 * x + c, 4 * y + z)

    def peer(axis, off):
        moved = [lax.rem(a + off, 4) if k == axis else a for k, a in enumerate(at)]
        return device(*moved)

    partner = device(*at, c=1 - core)

    loads = [
        pltpu.make_async_copy(depth_hbm, in_d.at[pl.ds(0, 128)], load_sem.at[0]),
        pltpu.make_async_copy(color_hbm, in_c.at[pl.ds(0, 128)], load_sem.at[1]),
    ]
    for load in loads:
        load.start()
    barrier = pltpu.get_barrier_semaphore()
    pl.semaphore_signal(barrier, inc=1, device_id=partner, device_id_type=MESH)
    for axis in range(3):
        for off in (1, 2, 3):
            pl.semaphore_signal(barrier, inc=1, device_id=peer(axis, off), device_id_type=MESH)

    in_d[128] = jnp.full((16, 128), FAR, jnp.int32)
    in_c[128] = jnp.zeros((3, 16, 128), jnp.bfloat16)
    tiles = tiles_ref[...]
    live = tiles >= 0
    row = lax.shift_right_arithmetic(tiles, 4)
    region = lax.shift_right_arithmetic(row, 1) * 16 + (tiles & 15)
    down = lax.broadcasted_iota(jnp.int32, (128, 128), 0)
    owner_down = jnp.transpose(jnp.broadcast_to(owner_ref[...], (128, 128)))
    owner = jnp.sum(jnp.where(down == region, owner_down, 0), axis=0, keepdims=True)
    place = jnp.where(live, 2 * owner + (row & 1), -1)
    place_down = jnp.transpose(jnp.broadcast_to(place, (128, 128)))
    for c in range(2):
        hit = place_down == place_ref[...] + 32 * c
        table_v[c : c + 1, :] = jnp.min(jnp.where(hit, down, 128), axis=0, keepdims=True)
    to_table = pltpu.make_async_copy(table_v, table, table_sem)
    to_table.start()
    with jax.named_scope("load"):
        to_table.wait()
        for load in loads:
            load.wait()
    with jax.named_scope("greet"):
        pl.semaphore_wait(barrier, 10)

    def remote(depth, color, sends, recv, target):
        for part, (src, dst) in enumerate((depth, color)):
            pltpu.make_async_remote_copy(
                src_ref=src, dst_ref=dst, send_sem=sends.at[part], recv_sem=recv,
                device_id=target, device_id_type=MESH,
            ).start()

    def wait_bytes(ref, count, sem):
        some = ref.at[pl.ds(0, count)]
        pltpu.make_async_copy(some, some, sem).wait()

    def chunk(stream, off):
        size = 4 * COUNT[stream]
        return BASE[stream] + lax.rem(at[ORDER[stream][1]] + off, 4) * size, size

    for n, (stream, off) in enumerate(CHUNKS):
        start, size = chunk(stream, off)

        def pack(t, carry):
            q = start + t
            slot = table[1 - core, q]
            send_d[q] = in_d[slot]
            send_c[q] = in_c[slot]
            return carry

        lax.fori_loop(0, size, pack, 0, unroll=4)
        part = pl.ds(start, size)
        remote((send_d.at[part], got_d.at[part]), (send_c.at[part], got_c.at[part]), core_send, core_recv.at[n], partner)

    for n, (stream, off) in enumerate(CHUNKS):
        start, size = chunk(stream, off)
        axis, count = ORDER[stream][0], COUNT[stream]
        with jax.named_scope(f"core_wait#n={n}"):
            wait_bytes(got_d, size * 5 // 2, core_recv.at[n])
        for step in (1, 3, 2, 0):
            first = start + lax.rem(at[axis] + step, 4) * count
            to_d, to_c = (own_d, own_c) if step else (one_d, one_c)

            def meet(t, carry):
                q = first + t
                slot = table[core, q]
                mine = (in_d[slot] - FAR) * 2 + core
                other = (got_d[q] - FAR) * 2 + (1 - core)
                nearer = other < mine
                to_d[q] = jnp.where(nearer, other, mine)
                to_c[q] = pick(nearer, got_c[q], in_c[slot])
                return carry

            lax.fori_loop(0, count, meet, 0, unroll=True)
            if step:
                src = pl.ds(first, count)
                dst = pl.ds(start + at[axis] * count, count)
                remote((own_d.at[src], one_d.at[dst]), (own_c.at[src], one_c.at[dst]), send1, recv1.at[n], peer(axis, step))

    for n, (stream, off) in enumerate(CHUNKS):
        start, size = chunk(stream, off)
        first, second, third = ORDER[stream]
        count, base = COUNT[stream], BASE[stream] // 4
        with jax.named_scope(f"wait1#n={n}"):
            wait_bytes(one_c, 5 * count, recv1.at[n])
        rest = at[second] * STRIDE[second] + at[third] * STRIDE[third]
        if off:
            to_d, to_c, into = out1_d, out1_c, base + (off - 1) * count
        else:
            to_d, to_c, into = two_d, two_c, base + at[second] * count

        def join(t, carry):
            key = tag = color = best = None
            for src in range(4):
                q = start + src * count + t
                k = one_d[q]
                depth = lax.shift_right_arithmetic(k, 1)
                order = depth if first == 0 else k
                rank = rest + src * STRIDE[first] + (k & 1) * 16
                if src == 0:
                    key, best, tag, color = order, depth, rank, one_c[q]
                else:
                    nearer = order < key
                    key = jnp.where(nearer, order, key)
                    best = jnp.where(nearer, depth, best)
                    tag = jnp.where(nearer, rank, tag)
                    color = pick(nearer, one_c[q], color)
            to_d[into + t] = best
            to_c[into + t, 0:3] = color
            to_c[into + t, 3] = tag.astype(jnp.float32).astype(jnp.bfloat16)
            return carry

        lax.fori_loop(0, count, join, 0)
        if off:
            src = pl.ds(into, count)
            dst = pl.ds(base + at[second] * count, count)
            remote((out1_d.at[src], two_d.at[dst]), (out1_c.at[src], two_c.at[dst]), send2, recv2.at[stream], peer(second, off))

    def closer(depth, color, best, kept):
        tag, old = color[3].astype(jnp.float32), kept[3].astype(jnp.float32)
        nearer = (depth < best) | ((depth == best) & (tag < old))
        return jnp.where(nearer, depth, best), pick(nearer, color, kept)

    for stream in range(3):
        count, base = COUNT[stream], BASE[stream] // 4
        with jax.named_scope(f"wait2#s={stream}"):
            wait_bytes(two_d, 9 * count, recv2.at[stream])
        for t in range(count):
            best, kept = two_d[base + t], two_c[base + t]
            for src in (1, 2, 3):
                q = base + src * count + t
                best, kept = closer(two_d[q], two_c[q], best, kept)
            k = 2 * CLASS[stream][t] + HALF[stream][t]
            out2_d[k] = best
            out2_c[k] = kept

    def is_third(axis, group, half):
        found = False
        for stream in range(3):
            if ORDER[stream][2] == axis:
                for c, h in zip(CLASS[stream], HALF[stream]):
                    if h == half:
                        found = found | (group == c)
        return found

    mine = lax.rem(at[0] + at[1] + at[2], 4)
    for off in (1, 2, 3):
        theirs = lax.rem(mine + off, 4)
        for half in range(2):
            target = device(*(
                lax.rem(a + jnp.where(is_third(axis, theirs, half), off, 0), 4) for axis, a in enumerate(at)
            ))
            k = 2 * theirs + half
            slot = 3 * half + off - 1
            remote((out2_d.at[k], last_d.at[slot]), (out2_c.at[k], last_c.at[slot]), send3, recv3, target)

    with jax.named_scope("wait3"):
        wait_bytes(one_d, 18, recv3)
    sums = []
    for half in range(2):
        best, kept = out2_d[2 * mine + half], out2_c[2 * mine + half]
        for off in (1, 2, 3):
            slot = 3 * half + off - 1
            best, kept = closer(last_d[slot], last_c[slot], best, kept)
        depth_out[half] = best + FAR
        color_out[half] = kept[0:3]
        sums.append(jnp.sum(kept[0:3].astype(jnp.float32).reshape(3, 2, 8, 128), axis=2))
    rows = jnp.concatenate(
        [s for c in range(3) for s in (sums[0][c], sums[1][c])] + [jnp.zeros((4, 128), jnp.float32)], axis=0
    )
    lane_down = lax.broadcasted_iota(jnp.int32, (128, 128), 0)
    lane = lax.broadcasted_iota(jnp.int32, (128, 128), 1)
    spread = jnp.where(lax.shift_right_logical(lane_down, 3) == (lane & 15), 1.0 / 64, 0.0)
    means = jnp.dot(rows, spread, precision=lax.Precision.HIGHEST, preferred_element_type=jnp.float32)
    line = lax.broadcasted_iota(jnp.int32, (16, 128), 0) & 7
    group = lax.shift_right_logical(lax.broadcasted_iota(jnp.int32, (16, 128), 1), 4)
    thumbs[me] = jnp.sum(jnp.where(line == group, means, 0.0).reshape(2, 8, 128), axis=1)

    around = [[lax.rem(a + off, 4) for off in range(4)] for a in at]
    across = [[2 * a + c for a in around[0]] for c in (core, 1 - core)]
    along = [[4 * b + c for c in around[2]] for b in around[1]]
    for dx, dy, dz in FAR_FIRST:
        for other in range(2):
            if dx or dy or dz or other:
                pltpu.make_async_remote_copy(
                    src_ref=thumbs.at[me], dst_ref=thumbs.at[me], send_sem=thumb_send, recv_sem=thumb_recv,
                    device_id=(across[other][dx], along[dy][dz]), device_id_type=MESH,
                ).start()
    for sends, depth_ref, color_ref, count in (
        (core_send, send_d, send_c, 128), (send1, own_d, own_c, 96),
        (send2, two_d, two_c, 24), (send3, last_d, last_c, 6),
    ):
        wait_bytes(depth_ref, count, sends.at[0])
        wait_bytes(color_ref, count, sends.at[1])
    with jax.named_scope("thumb_wait"):
        wait_bytes(thumbs, 127, thumb_recv)
    wait_bytes(thumbs, 127, thumb_send)
    thumbs_out[...] = thumbs[...]


def settle(owner_ref, depth_ref, color_ref, thumbs_ref, depth_out, color_out, thumbs_out):
    depth_out[...] = depth_ref[...]
    color_out[...] = color_ref[...]
    held = lax.broadcasted_iota(jnp.int32, (128, 128), 0) == owner_ref[...]
    chosen = jnp.where(held, 1.0, 0.0)
    for row, size in ((0, 128), (1, 64)):
        thumbs_out[128 * row : 128 * row + size] = lax.dot_general(
            thumbs_ref[:, row, 0:size], chosen, (((0,), (0,)), ((), ())),
            precision=lax.Precision.HIGHEST, preferred_element_type=jnp.float32,
        )


def shards(slot_tiles, owner_map, slot_depth, slot_color):
    i32, bf16 = jnp.int32, jnp.bfloat16
    vmem = pl.BlockSpec(memory_space=pltpu.VMEM)
    anywhere = pl.BlockSpec(memory_space=pl.ANY)
    dma = pltpu.SemaphoreType.DMA
    scratch = [
        pltpu.VMEM((129, 16, 128), i32), pltpu.VMEM((129, 3, 16, 128), bf16),
        pltpu.VMEM((2, 128), i32), pltpu.SMEM((2, 128), i32),
    ]
    for tiles, channels in ((128, 3), (128, 3), (128, 3), (128, 3), (32, 4), (32, 4), (8, 4), (6, 4)):
        scratch += [pltpu.VMEM((tiles, 16, 128), i32), pltpu.VMEM((tiles, channels, 16, 128), bf16)]
    scratch += [pltpu.VMEM((128, 2, 128), jnp.float32), dma((2,)), dma]
    scratch += [dma((2,)), dma((12,)), dma((2,)), dma((12,)), dma((2,)), dma((3,)), dma((2,)), dma]
    scratch += [dma, dma]
    depth, color, thumbs = pl.pallas_call(
        kernel,
        out_shape=(
            pltpu.VMEM((2, 16, 128), i32),
            pltpu.VMEM((2, 3, 16, 128), bf16),
            pltpu.VMEM((128, 2, 128), jnp.float32),
        ),
        in_specs=[vmem, vmem, vmem, anywhere, anywhere],
        out_specs=(vmem, vmem, vmem),
        scratch_shapes=scratch,
        compiler_params=pltpu.CompilerParams(collective_id=0, has_side_effects=True),
        name="composite",
    )(
        slot_tiles,
        owner_map[None],
        jnp.asarray(tile_places()),
        slot_depth[0],
        jnp.swapaxes(slot_color[0], 1, 2),
    )
    depth, color, thumbs = pl.pallas_call(
        settle,
        out_shape=(
            jax.ShapeDtypeStruct((2, 16, 128), i32),
            jax.ShapeDtypeStruct((2, 3, 16, 128), bf16),
            jax.ShapeDtypeStruct((192, 128), jnp.float32),
        ),
        in_specs=[vmem] * 4,
        out_specs=(vmem, vmem, vmem),
        compiler_params=pltpu.CompilerParams(vmem_limit_bytes=8 << 20),
        name="settle",
    )(owner_map[None], depth, color, thumbs)
    thumbnail = jnp.transpose(thumbs.reshape(3, 64, 128), (2, 0, 1))
    return depth[None], jnp.swapaxes(color, 1, 2)[None], thumbnail


def solution(mesh):
    ranks = ("gx", "gy")
    return jax.shard_map(
        shards,
        mesh=mesh,
        in_specs=(P(ranks, None), P(), P(ranks, None, None, None), P(ranks, None, None, None, None)),
        out_specs=(P(ranks, None, None, None), P(ranks, None, None, None, None), P()),
        check_vma=False,
    )
```

```python
import jax
import jax.numpy as jnp
import numpy as np
from jax import lax
from jax.experimental import pallas as pl
from jax.experimental.pallas import tpu as pltpu
from jax.sharding import PartitionSpec as P

MESH = pl.DeviceIdType.MESH
FAR = 1073741824
ORDER = ((0, 1, 2), (1, 2, 0), (2, 0, 1))
STRIDE = (32, 4, 1)
COUNT = (3, 3, 2)
BASE = (0, 48, 96)
CLASS = ((0, 0, 3), (1, 1, 3), (2, 2))
HALF = ((0, 1, 0), (0, 1, 1), (0, 1))
CHUNKS = tuple((stream, off) for off in (1, 3, 2, 0) for stream in range(3))
PLAIN = (1, 2)
STARTS = tuple(sum(4 * COUNT[s] for s, _ in CHUNKS[:n]) for n in range(12))
FAR_FIRST = sorted(np.ndindex(4, 4, 4), key=lambda d: -sum(min(a, 4 - a) for a in d))


def tile_places():
    places = np.zeros((1, 128), np.int32)
    for stream in range(3):
        first, second, third = ORDER[stream]
        count = COUNT[stream]
        for i in range(4):
            for j in range(4):
                for t in range(count):
                    at = [0, 0, 0]
                    at[first], at[second] = i, j
                    at[third] = (CLASS[stream][t] - i - j) % 4
                    owner = sum(a * s for a, s in zip(at, STRIDE))
                    places[0, BASE[stream] + (j * 4 + i) * count + t] = 2 * owner + HALF[stream][t]
    return places


def pick(mask, new, old):
    return jnp.where(mask[None], new, old)


def kernel(
    tiles_ref, owner_ref, place_ref, depth_hbm, color_hbm,
    depth_out, color_out, thumbs_out,
    in_d, in_c, table_v, table, send_d, send_c, got_d, got_c,
    own_d, own_c, one_d, one_c, mid_d, mid_c, pass_d, pass_c, met_d, met_c, out1_d, out1_c, two_d, two_c, out2_d, out2_c,
    last_d, last_c, thumbs,
    load_sem, table_sem, core_send, core_recv, send1, recv1, send1b, recv1b, send2, recv2, send3, recv3,
    thumb_send, thumb_recv,
):
    gx, gy = lax.axis_index("gx"), lax.axis_index("gy")
    core = lax.rem(gx, 2)
    at = (lax.div(gx, 2), lax.div(gy, 4), lax.rem(gy, 4))
    me = gx * 16 + gy

    def device(x, y, z, c=core):
        return (2 * x + c, 4 * y + z)

    def peer(axis, off):
        moved = [lax.rem(a + off, 4) if k == axis else a for k, a in enumerate(at)]
        return device(*moved)

    partner = device(*at, c=1 - core)

    loads = [
        pltpu.make_async_copy(depth_hbm, in_d.at[pl.ds(0, 128)], load_sem.at[0]),
        pltpu.make_async_copy(color_hbm, in_c.at[pl.ds(0, 128)], load_sem.at[1]),
    ]
    for load in loads:
        load.start()
    barrier = pltpu.get_barrier_semaphore()
    pl.semaphore_signal(barrier, inc=1, device_id=partner, device_id_type=MESH)
    for axis in range(3):
        for off in (1, 2, 3):
            pl.semaphore_signal(barrier, inc=1, device_id=peer(axis, off), device_id_type=MESH)

    in_d[128] = jnp.full((16, 128), FAR, jnp.int32)
    in_c[128] = jnp.zeros((3, 16, 128), jnp.bfloat16)
    tiles = tiles_ref[...]
    live = tiles >= 0
    row = lax.shift_right_arithmetic(tiles, 4)
    region = lax.shift_right_arithmetic(row, 1) * 16 + (tiles & 15)
    down = lax.broadcasted_iota(jnp.int32, (128, 128), 0)
    owner_down = jnp.transpose(jnp.broadcast_to(owner_ref[...], (128, 128)))
    owner = jnp.sum(jnp.where(down == region, owner_down, 0), axis=0, keepdims=True)
    place = jnp.where(live, 2 * owner + (row & 1), -1)
    place_down = jnp.transpose(jnp.broadcast_to(place, (128, 128)))
    for c in range(2):
        hit = place_down == place_ref[...] + 32 * c
        table_v[c : c + 1, :] = jnp.min(jnp.where(hit, down, 128), axis=0, keepdims=True)
    to_table = pltpu.make_async_copy(table_v, table, table_sem)
    to_table.start()
    with jax.named_scope("load"):
        to_table.wait()
        for load in loads:
            load.wait()
    with jax.named_scope("greet"):
        pl.semaphore_wait(barrier, 10)

    def remote(depth, color, sends, recv, target):
        for part, (src, dst) in enumerate((depth, color)):
            pltpu.make_async_remote_copy(
                src_ref=src, dst_ref=dst, send_sem=sends.at[part], recv_sem=recv,
                device_id=target, device_id_type=MESH,
            ).start()

    def wait_bytes(ref, count, sem):
        some = ref.at[pl.ds(0, count)]
        pltpu.make_async_copy(some, some, sem).wait()

    def chunk(stream, off):
        size = 4 * COUNT[stream]
        return BASE[stream] + lax.rem(at[ORDER[stream][1]] + off, 4) * size, size

    for n, (stream, off) in enumerate(CHUNKS):
        start, size = chunk(stream, off)

        def pack(t, carry):
            q = start + t
            slot = table[1 - core, q]
            send_d[q] = in_d[slot]
            send_c[q] = in_c[slot]
            return carry

        lax.fori_loop(0, size, pack, 0, unroll=4)
        part = pl.ds(start, size)
        remote((send_d.at[part], got_d.at[part]), (send_c.at[part], got_c.at[part]), core_send, core_recv.at[n], partner)

    def others(axis):
        c = at[axis]
        return c, c + 1 - 2 * lax.rem(c, 2), lax.rem(c + 2, 4), 3 - c

    def seat(axis, place):
        return device(*(place if k == axis else a for k, a in enumerate(at)))

    for n, (stream, off) in enumerate(CHUNKS):
        start, size = chunk(stream, off)
        axis, count = ORDER[stream][0], COUNT[stream]
        with jax.named_scope(f"core_wait#n={n}"):
            wait_bytes(got_d, size * 5 // 2, core_recv.at[n])
        sent = (1, 2) if off in PLAIN else (2, 3)
        places = others(axis)
        for rel in sent + tuple(r for r in range(4) if r not in sent):
            first, into = start + places[rel] * count, STARTS[n] + rel * count

            def meet(t, carry):
                slot = table[core, first + t]
                mine = (in_d[slot] - FAR) * 2 + core
                other = (got_d[first + t] - FAR) * 2 + (1 - core)
                nearer = other < mine
                own_d[into + t] = jnp.where(nearer, other, mine)
                own_c[into + t] = pick(nearer, got_c[first + t], in_c[slot])
                return carry

            lax.fori_loop(0, count, meet, 0, unroll=True)
            if rel == sent[1]:
                src = pl.ds(STARTS[n] + sent[0] * count, 2 * count)
                dst = pl.ds(STARTS[n] // 2, 2 * count)
                remote(
                    (own_d.at[src], one_d.at[dst]), (own_c.at[src], one_c.at[dst]),
                    send1, recv1.at[n], seat(axis, places[1 if off in PLAIN else 3]),
                )

    def closer(depth, color, best, kept):
        tag, old = color[3].astype(jnp.float32), kept[3].astype(jnp.float32)
        nearer = (depth < best) | ((depth == best) & (tag < old))
        return jnp.where(nearer, depth, best), pick(nearer, color, kept)

    def first_join(n):
        stream, off = CHUNKS[n]
        first, second, third = ORDER[stream]
        count = COUNT[stream]
        places = others(first)
        near, away = (1, 3) if off in PLAIN else (3, 1)
        mine, theirs = places[0], places[near]
        rest = at[second] * STRIDE[second] + at[third] * STRIDE[third]
        lower = jnp.where(theirs < mine, 1, 0)
        with jax.named_scope(f"wait1#n={n}"):
            wait_bytes(one_d, 5 * count, recv1.at[n])
        for part, rel in enumerate((0, 3) if off in PLAIN else (1, 0)):
            to_d, to_c = (pass_d, pass_c) if rel else (mid_d, mid_c)
            base = STARTS[n] // 4

            def join(t, carry):
                p, q = STARTS[n] + rel * count + t, STARTS[n] // 2 + part * count + t
                k, other = own_d[p], one_d[q]
                depth, far_depth = lax.shift_right_arithmetic(k, 1), lax.shift_right_arithmetic(other, 1)
                nearer = far_depth < depth + lower if first == 0 else other < k + lower
                own_rank = rest + mine * STRIDE[first] + (k & 1) * 16
                other_rank = rest + theirs * STRIDE[first] + (other & 1) * 16
                to_d[base + t] = jnp.where(nearer, far_depth, depth)
                to_c[base + t, 0:3] = pick(nearer, one_c[q], own_c[p])
                to_c[base + t, 3] = jnp.where(nearer, other_rank, own_rank).astype(jnp.float32).astype(jnp.bfloat16)
                return carry

            lax.fori_loop(0, count, join, 0)
        part = pl.ds(STARTS[n] // 4, count)
        remote(
            (pass_d.at[part], met_d.at[part]), (pass_c.at[part], met_c.at[part]),
            send1b, recv1b.at[n], seat(first, places[away]),
        )

    def second_join(n):
        stream, off = CHUNKS[n]
        second, count = ORDER[stream][1], COUNT[stream]
        base, into = STARTS[n] // 4, BASE[stream] // 4
        if off:
            to_d, to_c, into = out1_d, out1_c, into + (off - 1) * count
        else:
            to_d, to_c, into = two_d, two_c, into + at[second] * count
        with jax.named_scope(f"wait1b#n={n}"):
            wait_bytes(one_d, 3 * count, recv1b.at[n])

        def join(t, carry):
            q = base + t
            to_d[into + t], to_c[into + t] = closer(met_d[q], met_c[q], mid_d[q], mid_c[q])
            return carry

        lax.fori_loop(0, count, join, 0)
        if off:
            src = pl.ds(into, count)
            dst = pl.ds(BASE[stream] // 4 + at[second] * count, count)
            remote((out1_d.at[src], two_d.at[dst]), (out1_c.at[src], two_c.at[dst]), send2, recv2.at[stream], peer(second, off))

    for group in range(5):
        if group < 4:
            for n in range(3 * group, 3 * group + 3):
                first_join(n)
        if group:
            for n in range(3 * group - 3, 3 * group):
                second_join(n)

    for stream in range(3):
        count, base = COUNT[stream], BASE[stream] // 4
        with jax.named_scope(f"wait2#s={stream}"):
            wait_bytes(two_d, 9 * count, recv2.at[stream])
        for t in range(count):
            best, kept = two_d[base + t], two_c[base + t]
            for src in (1, 2, 3):
                q = base + src * count + t
                best, kept = closer(two_d[q], two_c[q], best, kept)
            k = 2 * CLASS[stream][t] + HALF[stream][t]
            out2_d[k] = best
            out2_c[k] = kept

    def is_third(axis, group, half):
        found = False
        for stream in range(3):
            if ORDER[stream][2] == axis:
                for c, h in zip(CLASS[stream], HALF[stream]):
                    if h == half:
                        found = found | (group == c)
        return found

    mine = lax.rem(at[0] + at[1] + at[2], 4)
    for off in (1, 2, 3):
        theirs = lax.rem(mine + off, 4)
        for half in range(2):
            target = device(*(
                lax.rem(a + jnp.where(is_third(axis, theirs, half), off, 0), 4) for axis, a in enumerate(at)
            ))
            k = 2 * theirs + half
            slot = 3 * half + off - 1
            remote((out2_d.at[k], last_d.at[slot]), (out2_c.at[k], last_c.at[slot]), send3, recv3, target)

    with jax.named_scope("wait3"):
        wait_bytes(one_d, 18, recv3)
    sums = []
    for half in range(2):
        best, kept = out2_d[2 * mine + half], out2_c[2 * mine + half]
        for off in (1, 2, 3):
            slot = 3 * half + off - 1
            best, kept = closer(last_d[slot], last_c[slot], best, kept)
        depth_out[half] = best + FAR
        color_out[half] = kept[0:3]
        sums.append(jnp.sum(kept[0:3].astype(jnp.float32).reshape(3, 2, 8, 128), axis=2))
    rows = jnp.concatenate(
        [s for c in range(3) for s in (sums[0][c], sums[1][c])] + [jnp.zeros((4, 128), jnp.float32)], axis=0
    )
    lane_down = lax.broadcasted_iota(jnp.int32, (128, 128), 0)
    lane = lax.broadcasted_iota(jnp.int32, (128, 128), 1)
    spread = jnp.where(lax.shift_right_logical(lane_down, 3) == (lane & 15), 1.0 / 64, 0.0)
    means = jnp.dot(rows, spread, precision=lax.Precision.HIGHEST, preferred_element_type=jnp.float32)
    line = lax.broadcasted_iota(jnp.int32, (16, 128), 0) & 7
    group = lax.shift_right_logical(lax.broadcasted_iota(jnp.int32, (16, 128), 1), 4)
    thumbs[me] = jnp.sum(jnp.where(line == group, means, 0.0).reshape(2, 8, 128), axis=1)

    around = [[lax.rem(a + off, 4) for off in range(4)] for a in at]
    across = [[2 * a + c for a in around[0]] for c in (core, 1 - core)]
    along = [[4 * b + c for c in around[2]] for b in around[1]]
    for dx, dy, dz in FAR_FIRST:
        for other in range(2):
            if dx or dy or dz or other:
                pltpu.make_async_remote_copy(
                    src_ref=thumbs.at[me], dst_ref=thumbs.at[me], send_sem=thumb_send, recv_sem=thumb_recv,
                    device_id=(across[other][dx], along[dy][dz]), device_id_type=MESH,
                ).start()
    for sends, depth_ref, color_ref, count in (
        (core_send, send_d, send_c, 128), (send1, own_d, own_c, 64), (send1b, met_d, met_c, 32),
        (send2, two_d, two_c, 24), (send3, last_d, last_c, 6),
    ):
        wait_bytes(depth_ref, count, sends.at[0])
        wait_bytes(color_ref, count, sends.at[1])
    with jax.named_scope("thumb_wait"):
        wait_bytes(thumbs, 127, thumb_recv)
    wait_bytes(thumbs, 127, thumb_send)
    thumbs_out[...] = thumbs[...]


def settle(owner_ref, depth_ref, color_ref, thumbs_ref, depth_out, color_out, thumbs_out):
    depth_out[...] = depth_ref[...]
    color_out[...] = color_ref[...]
    held = lax.broadcasted_iota(jnp.int32, (128, 128), 0) == owner_ref[...]
    chosen = jnp.where(held, 1.0, 0.0)
    for row, size in ((0, 128), (1, 64)):
        thumbs_out[128 * row : 128 * row + size] = lax.dot_general(
            thumbs_ref[:, row, 0:size], chosen, (((0,), (0,)), ((), ())),
            precision=lax.Precision.HIGHEST, preferred_element_type=jnp.float32,
        )


def shards(slot_tiles, owner_map, slot_depth, slot_color):
    i32, bf16 = jnp.int32, jnp.bfloat16
    vmem = pl.BlockSpec(memory_space=pltpu.VMEM)
    anywhere = pl.BlockSpec(memory_space=pl.ANY)
    dma = pltpu.SemaphoreType.DMA
    scratch = [
        pltpu.VMEM((129, 16, 128), i32), pltpu.VMEM((129, 3, 16, 128), bf16),
        pltpu.VMEM((2, 128), i32), pltpu.SMEM((2, 128), i32),
    ]
    for tiles, channels in ((128, 3), (128, 3), (128, 3), (64, 3), (32, 4), (32, 4), (32, 4), (32, 4), (32, 4), (8, 4), (6, 4)):
        scratch += [pltpu.VMEM((tiles, 16, 128), i32), pltpu.VMEM((tiles, channels, 16, 128), bf16)]
    scratch += [pltpu.VMEM((128, 2, 128), jnp.float32), dma((2,)), dma]
    scratch += [dma((2,)), dma((12,)), dma((2,)), dma((12,)), dma((2,)), dma((12,)), dma((2,)), dma((3,)), dma((2,)), dma]
    scratch += [dma, dma]
    depth, color, thumbs = pl.pallas_call(
        kernel,
        out_shape=(
            pltpu.VMEM((2, 16, 128), i32),
            pltpu.VMEM((2, 3, 16, 128), bf16),
            pltpu.VMEM((128, 2, 128), jnp.float32),
        ),
        in_specs=[vmem, vmem, vmem, anywhere, anywhere],
        out_specs=(vmem, vmem, vmem),
        scratch_shapes=scratch,
        compiler_params=pltpu.CompilerParams(collective_id=0, has_side_effects=True),
        name="composite",
    )(
        slot_tiles,
        owner_map[None],
        jnp.asarray(tile_places()),
        slot_depth[0],
        jnp.swapaxes(slot_color[0], 1, 2),
    )
    depth, color, thumbs = pl.pallas_call(
        settle,
        out_shape=(
            jax.ShapeDtypeStruct((2, 16, 128), i32),
            jax.ShapeDtypeStruct((2, 3, 16, 128), bf16),
            jax.ShapeDtypeStruct((192, 128), jnp.float32),
        ),
        in_specs=[vmem] * 4,
        out_specs=(vmem, vmem, vmem),
        compiler_params=pltpu.CompilerParams(vmem_limit_bytes=8 << 20),
        name="settle",
    )(owner_map[None], depth, color, thumbs)
    thumbnail = jnp.transpose(thumbs.reshape(3, 64, 128), (2, 0, 1))
    return depth[None], jnp.swapaxes(color, 1, 2)[None], thumbnail


def solution(mesh):
    ranks = ("gx", "gy")
    return jax.shard_map(
        shards,
        mesh=mesh,
        in_specs=(P(ranks, None), P(), P(ranks, None, None, None), P(ranks, None, None, None, None)),
        out_specs=(P(ranks, None, None, None), P(ranks, None, None, None, None), P()),
        check_vma=False,
    )
```

```python
import jax
import jax.numpy as jnp
import numpy as np
from jax import lax
from jax.experimental import pallas as pl
from jax.experimental.pallas import tpu as pltpu
from jax.sharding import PartitionSpec as P

MESH = pl.DeviceIdType.MESH
FAR = 1073741824
ORDER = ((0, 1, 2), (1, 2, 0), (2, 0, 1))
STRIDE = (32, 4, 1)
COUNT = (3, 3, 2)
BASE = (0, 48, 96)
CLASS = ((0, 0, 3), (1, 1, 3), (2, 2))
HALF = ((0, 1, 0), (0, 1, 1), (0, 1))
CHUNKS = tuple((stream, off) for off in (2, 1, 3, 0) for stream in range(3))
PLAIN = (2, 3)
STARTS = tuple(sum(4 * COUNT[s] for s, _ in CHUNKS[:n]) for n in range(12))
FAR_FIRST = sorted(np.ndindex(4, 4, 4), key=lambda d: -sum(min(a, 4 - a) for a in d))


def tile_places():
    places = np.zeros((1, 128), np.int32)
    for stream in range(3):
        first, second, third = ORDER[stream]
        count = COUNT[stream]
        for i in range(4):
            for j in range(4):
                for t in range(count):
                    at = [0, 0, 0]
                    at[first], at[second] = i, j
                    at[third] = (CLASS[stream][t] - i - j) % 4
                    owner = sum(a * s for a, s in zip(at, STRIDE))
                    places[0, BASE[stream] + (j * 4 + i) * count + t] = 2 * owner + HALF[stream][t]
    return places


def pick(mask, new, old):
    return jnp.where(mask[None], new, old)


def kernel(
    tiles_ref, owner_ref, place_ref, depth_hbm, color_hbm,
    depth_out, color_out, thumbs_out,
    in_d, in_c, table_v, table, send_d, send_c, got_d, got_c,
    own_d, own_c, one_d, one_c, mid_d, mid_c, pass_d, pass_c, met_d, met_c, out1_d, out1_c, two_d, two_c, out2_d, out2_c,
    last_d, last_c, thumbs,
    load_sem, table_sem, core_send, core_recv, send1, recv1, send1b, recv1b, send2, recv2, send3, recv3,
    thumb_send, thumb_recv,
):
    gx, gy = lax.axis_index("gx"), lax.axis_index("gy")
    core = lax.rem(gx, 2)
    at = (lax.div(gx, 2), lax.div(gy, 4), lax.rem(gy, 4))
    me = gx * 16 + gy

    def device(x, y, z, c=core):
        return (2 * x + c, 4 * y + z)

    def peer(axis, off):
        moved = [lax.rem(a + off, 4) if k == axis else a for k, a in enumerate(at)]
        return device(*moved)

    partner = device(*at, c=1 - core)

    loads = [
        pltpu.make_async_copy(depth_hbm, in_d.at[pl.ds(0, 128)], load_sem.at[0]),
        pltpu.make_async_copy(color_hbm, in_c.at[pl.ds(0, 128)], load_sem.at[1]),
    ]
    for load in loads:
        load.start()
    barrier = pltpu.get_barrier_semaphore()
    pl.semaphore_signal(barrier, inc=1, device_id=partner, device_id_type=MESH)
    for axis in range(3):
        for off in (1, 2, 3):
            pl.semaphore_signal(barrier, inc=1, device_id=peer(axis, off), device_id_type=MESH)

    in_d[128] = jnp.full((16, 128), FAR, jnp.int32)
    in_c[128] = jnp.zeros((3, 16, 128), jnp.bfloat16)
    tiles = tiles_ref[...]
    live = tiles >= 0
    row = lax.shift_right_arithmetic(tiles, 4)
    region = lax.shift_right_arithmetic(row, 1) * 16 + (tiles & 15)
    down = lax.broadcasted_iota(jnp.int32, (128, 128), 0)
    owner_down = jnp.transpose(jnp.broadcast_to(owner_ref[...], (128, 128)))
    owner = jnp.sum(jnp.where(down == region, owner_down, 0), axis=0, keepdims=True)
    place = jnp.where(live, 2 * owner + (row & 1), -1)
    place_down = jnp.transpose(jnp.broadcast_to(place, (128, 128)))
    for c in range(2):
        hit = place_down == place_ref[...] + 32 * c
        table_v[c : c + 1, :] = jnp.min(jnp.where(hit, down, 128), axis=0, keepdims=True)
    to_table = pltpu.make_async_copy(table_v, table, table_sem)
    to_table.start()
    with jax.named_scope("load"):
        to_table.wait()
        for load in loads:
            load.wait()
    with jax.named_scope("greet"):
        pl.semaphore_wait(barrier, 10)

    def remote(depth, color, sends, recv, target):
        for part, (src, dst) in enumerate((depth, color)):
            pltpu.make_async_remote_copy(
                src_ref=src, dst_ref=dst, send_sem=sends.at[part], recv_sem=recv,
                device_id=target, device_id_type=MESH,
            ).start()

    def wait_bytes(ref, count, sem):
        some = ref.at[pl.ds(0, count)]
        pltpu.make_async_copy(some, some, sem).wait()

    def chunk(stream, off):
        size = 4 * COUNT[stream]
        return BASE[stream] + lax.rem(at[ORDER[stream][1]] + off, 4) * size, size

    for n, (stream, off) in enumerate(CHUNKS):
        start, size = chunk(stream, off)

        def pack(t, carry):
            q = start + t
            slot = table[1 - core, q]
            send_d[q] = in_d[slot]
            send_c[q] = in_c[slot]
            return carry

        lax.fori_loop(0, size, pack, 0, unroll=4)
        part = pl.ds(start, size)
        remote((send_d.at[part], got_d.at[part]), (send_c.at[part], got_c.at[part]), core_send, core_recv.at[n], partner)

    def others(axis):
        c = at[axis]
        return c, c + 1 - 2 * lax.rem(c, 2), lax.rem(c + 2, 4), 3 - c

    def seat(axis, place):
        return device(*(place if k == axis else a for k, a in enumerate(at)))

    for n, (stream, off) in enumerate(CHUNKS):
        start, size = chunk(stream, off)
        axis, count = ORDER[stream][0], COUNT[stream]
        with jax.named_scope(f"core_wait#n={n}"):
            wait_bytes(got_d, size * 5 // 2, core_recv.at[n])
        sent = (1, 2) if off in PLAIN else (2, 3)
        places = others(axis)
        for rel in sent + tuple(r for r in range(4) if r not in sent):
            first, into = start + places[rel] * count, STARTS[n] + rel * count

            def meet(t, carry):
                slot = table[core, first + t]
                mine = (in_d[slot] - FAR) * 2 + core
                other = (got_d[first + t] - FAR) * 2 + (1 - core)
                nearer = other < mine
                own_d[into + t] = jnp.where(nearer, other, mine)
                own_c[into + t] = pick(nearer, got_c[first + t], in_c[slot])
                return carry

            lax.fori_loop(0, count, meet, 0, unroll=True)
            if rel == sent[1]:
                src = pl.ds(STARTS[n] + sent[0] * count, 2 * count)
                dst = pl.ds(STARTS[n] // 2, 2 * count)
                remote(
                    (own_d.at[src], one_d.at[dst]), (own_c.at[src], one_c.at[dst]),
                    send1, recv1.at[n], seat(axis, places[1 if off in PLAIN else 3]),
                )

    def closer(depth, color, best, kept):
        tag, old = color[3].astype(jnp.float32), kept[3].astype(jnp.float32)
        nearer = (depth < best) | ((depth == best) & (tag < old))
        return jnp.where(nearer, depth, best), pick(nearer, color, kept)

    def first_join(n):
        stream, off = CHUNKS[n]
        first, second, third = ORDER[stream]
        count = COUNT[stream]
        places = others(first)
        near, away = (1, 3) if off in PLAIN else (3, 1)
        mine, theirs = places[0], places[near]
        rest = at[second] * STRIDE[second] + at[third] * STRIDE[third]
        lower = jnp.where(theirs < mine, 1, 0)
        with jax.named_scope(f"wait1#n={n}"):
            wait_bytes(one_d, 5 * count, recv1.at[n])
        for part, rel in enumerate((0, 3) if off in PLAIN else (1, 0)):
            to_d, to_c = (pass_d, pass_c) if rel else (mid_d, mid_c)
            base = STARTS[n] // 4

            def join(t, carry):
                p, q = STARTS[n] + rel * count + t, STARTS[n] // 2 + part * count + t
                k, other = own_d[p], one_d[q]
                depth, far_depth = lax.shift_right_arithmetic(k, 1), lax.shift_right_arithmetic(other, 1)
                nearer = far_depth < depth + lower if first == 0 else other < k + lower
                own_rank = rest + mine * STRIDE[first] + (k & 1) * 16
                other_rank = rest + theirs * STRIDE[first] + (other & 1) * 16
                to_d[base + t] = jnp.where(nearer, far_depth, depth)
                to_c[base + t, 0:3] = pick(nearer, one_c[q], own_c[p])
                to_c[base + t, 3] = jnp.where(nearer, other_rank, own_rank).astype(jnp.float32).astype(jnp.bfloat16)
                return carry

            lax.fori_loop(0, count, join, 0)
        part = pl.ds(STARTS[n] // 4, count)
        remote(
            (pass_d.at[part], met_d.at[part]), (pass_c.at[part], met_c.at[part]),
            send1b, recv1b.at[n], seat(first, places[away]),
        )

    def second_join(n):
        stream, off = CHUNKS[n]
        second, count = ORDER[stream][1], COUNT[stream]
        base, into = STARTS[n] // 4, BASE[stream] // 4
        if off:
            to_d, to_c, into = out1_d, out1_c, into + (off - 1) * count
        else:
            to_d, to_c, into = two_d, two_c, into + at[second] * count
        with jax.named_scope(f"wait1b#n={n}"):
            wait_bytes(one_d, 3 * count, recv1b.at[n])

        def join(t, carry):
            q = base + t
            to_d[into + t], to_c[into + t] = closer(met_d[q], met_c[q], mid_d[q], mid_c[q])
            return carry

        lax.fori_loop(0, count, join, 0)
        if off:
            src = pl.ds(into, count)
            dst = pl.ds(BASE[stream] // 4 + at[second] * count, count)
            remote((out1_d.at[src], two_d.at[dst]), (out1_c.at[src], two_c.at[dst]), send2, recv2.at[stream], peer(second, off))

    for n in range(12):
        first_join(n)
    for n in range(12):
        second_join(n)

    for stream in range(3):
        count, base = COUNT[stream], BASE[stream] // 4
        with jax.named_scope(f"wait2#s={stream}"):
            wait_bytes(two_d, 9 * count, recv2.at[stream])
        for t in range(count):
            best, kept = two_d[base + t], two_c[base + t]
            for src in (1, 2, 3):
                q = base + src * count + t
                best, kept = closer(two_d[q], two_c[q], best, kept)
            k = 2 * CLASS[stream][t] + HALF[stream][t]
            out2_d[k] = best
            out2_c[k] = kept

    def is_third(axis, group, half):
        found = False
        for stream in range(3):
            if ORDER[stream][2] == axis:
                for c, h in zip(CLASS[stream], HALF[stream]):
                    if h == half:
                        found = found | (group == c)
        return found

    mine = lax.rem(at[0] + at[1] + at[2], 4)
    for off in (2, 1, 3):
        theirs = lax.rem(mine + off, 4)
        for half in range(2):
            target = device(*(
                lax.rem(a + jnp.where(is_third(axis, theirs, half), off, 0), 4) for axis, a in enumerate(at)
            ))
            k = 2 * theirs + half
            slot = 3 * half + off - 1
            remote((out2_d.at[k], last_d.at[slot]), (out2_c.at[k], last_c.at[slot]), send3, recv3, target)

    with jax.named_scope("wait3"):
        wait_bytes(one_d, 18, recv3)
    sums = []
    for half in range(2):
        best, kept = out2_d[2 * mine + half], out2_c[2 * mine + half]
        for off in (1, 2, 3):
            slot = 3 * half + off - 1
            best, kept = closer(last_d[slot], last_c[slot], best, kept)
        depth_out[half] = best + FAR
        color_out[half] = kept[0:3]
        sums.append(jnp.sum(kept[0:3].astype(jnp.float32).reshape(3, 2, 8, 128), axis=2))
    rows = jnp.concatenate(
        [s for c in range(3) for s in (sums[0][c], sums[1][c])] + [jnp.zeros((4, 128), jnp.float32)], axis=0
    )
    lane_down = lax.broadcasted_iota(jnp.int32, (128, 128), 0)
    lane = lax.broadcasted_iota(jnp.int32, (128, 128), 1)
    spread = jnp.where(lax.shift_right_logical(lane_down, 3) == (lane & 15), 1.0 / 64, 0.0)
    means = jnp.dot(rows, spread, precision=lax.Precision.HIGHEST, preferred_element_type=jnp.float32)
    line = lax.broadcasted_iota(jnp.int32, (16, 128), 0) & 7
    group = lax.shift_right_logical(lax.broadcasted_iota(jnp.int32, (16, 128), 1), 4)
    thumbs[me] = jnp.sum(jnp.where(line == group, means, 0.0).reshape(2, 8, 128), axis=1)

    around = [[lax.rem(a + off, 4) for off in range(4)] for a in at]
    across = [[2 * a + c for a in around[0]] for c in (core, 1 - core)]
    along = [[4 * b + c for c in around[2]] for b in around[1]]
    for dx, dy, dz in FAR_FIRST:
        for other in range(2):
            if dx or dy or dz or other:
                pltpu.make_async_remote_copy(
                    src_ref=thumbs.at[me], dst_ref=thumbs.at[me], send_sem=thumb_send, recv_sem=thumb_recv,
                    device_id=(across[other][dx], along[dy][dz]), device_id_type=MESH,
                ).start()
    for sends, depth_ref, color_ref, count in (
        (core_send, send_d, send_c, 128), (send1, own_d, own_c, 64), (send1b, met_d, met_c, 32),
        (send2, two_d, two_c, 24), (send3, last_d, last_c, 6),
    ):
        wait_bytes(depth_ref, count, sends.at[0])
        wait_bytes(color_ref, count, sends.at[1])
    with jax.named_scope("thumb_wait"):
        wait_bytes(thumbs, 127, thumb_recv)
    wait_bytes(thumbs, 127, thumb_send)
    thumbs_out[...] = thumbs[...]


def settle(owner_ref, depth_ref, color_ref, thumbs_ref, depth_out, color_out, thumbs_out):
    depth_out[...] = depth_ref[...]
    color_out[...] = color_ref[...]
    held = lax.broadcasted_iota(jnp.int32, (128, 128), 0) == owner_ref[...]
    chosen = jnp.where(held, 1.0, 0.0)
    for row, size in ((0, 128), (1, 64)):
        thumbs_out[128 * row : 128 * row + size] = lax.dot_general(
            thumbs_ref[:, row, 0:size], chosen, (((0,), (0,)), ((), ())),
            precision=lax.Precision.HIGHEST, preferred_element_type=jnp.float32,
        )


def shards(slot_tiles, owner_map, slot_depth, slot_color):
    i32, bf16 = jnp.int32, jnp.bfloat16
    vmem = pl.BlockSpec(memory_space=pltpu.VMEM)
    anywhere = pl.BlockSpec(memory_space=pl.ANY)
    dma = pltpu.SemaphoreType.DMA
    scratch = [
        pltpu.VMEM((129, 16, 128), i32), pltpu.VMEM((129, 3, 16, 128), bf16),
        pltpu.VMEM((2, 128), i32), pltpu.SMEM((2, 128), i32),
    ]
    for tiles, channels in ((128, 3), (128, 3), (128, 3), (64, 3), (32, 4), (32, 4), (32, 4), (32, 4), (32, 4), (8, 4), (6, 4)):
        scratch += [pltpu.VMEM((tiles, 16, 128), i32), pltpu.VMEM((tiles, channels, 16, 128), bf16)]
    scratch += [pltpu.VMEM((128, 2, 128), jnp.float32), dma((2,)), dma]
    scratch += [dma((2,)), dma((12,)), dma((2,)), dma((12,)), dma((2,)), dma((12,)), dma((2,)), dma((3,)), dma((2,)), dma]
    scratch += [dma, dma]
    depth, color, thumbs = pl.pallas_call(
        kernel,
        out_shape=(
            pltpu.VMEM((2, 16, 128), i32),
            pltpu.VMEM((2, 3, 16, 128), bf16),
            pltpu.VMEM((128, 2, 128), jnp.float32),
        ),
        in_specs=[vmem, vmem, vmem, anywhere, anywhere],
        out_specs=(vmem, vmem, vmem),
        scratch_shapes=scratch,
        compiler_params=pltpu.CompilerParams(collective_id=0, has_side_effects=True),
        name="composite",
    )(
        slot_tiles,
        owner_map[None],
        jnp.asarray(tile_places()),
        slot_depth[0],
        jnp.swapaxes(slot_color[0], 1, 2),
    )
    depth, color, thumbs = pl.pallas_call(
        settle,
        out_shape=(
            jax.ShapeDtypeStruct((2, 16, 128), i32),
            jax.ShapeDtypeStruct((2, 3, 16, 128), bf16),
            jax.ShapeDtypeStruct((192, 128), jnp.float32),
        ),
        in_specs=[vmem] * 4,
        out_specs=(vmem, vmem, vmem),
        compiler_params=pltpu.CompilerParams(vmem_limit_bytes=8 << 20),
        name="settle",
    )(owner_map[None], depth, color, thumbs)
    thumbnail = jnp.transpose(thumbs.reshape(3, 64, 128), (2, 0, 1))
    return depth[None], jnp.swapaxes(color, 1, 2)[None], thumbnail


def solution(mesh):
    ranks = ("gx", "gy")
    return jax.shard_map(
        shards,
        mesh=mesh,
        in_specs=(P(ranks, None), P(), P(ranks, None, None, None), P(ranks, None, None, None, None)),
        out_specs=(P(ranks, None, None, None), P(ranks, None, None, None, None), P()),
        check_vma=False,
    )
```

```python
import jax
import jax.numpy as jnp
import numpy as np
from jax import lax
from jax.experimental import pallas as pl
from jax.experimental.pallas import tpu as pltpu
from jax.sharding import PartitionSpec as P

MESH = pl.DeviceIdType.MESH
FAR = 1073741824
ORDER = ((0, 1, 2), (1, 2, 0), (2, 0, 1))
STRIDE = (32, 4, 1)
COUNT = (3, 3, 2)
BASE = (0, 48, 96)
CLASS = ((0, 2, 3), (0, 1, 3), (1, 2))
HALF = ((0, 1, 0), (1, 0, 1), (1, 0))
CHUNKS = tuple((stream, off) for off in (2, 1, 3, 0) for stream in range(3))
PLAIN = (2, 3)
STARTS = tuple(sum(4 * COUNT[s] for s, _ in CHUNKS[:n]) for n in range(12))
FAR_FIRST = sorted(np.ndindex(4, 4, 4), key=lambda d: -sum(min(a, 4 - a) for a in d))


def tile_places():
    places = np.zeros((1, 128), np.int32)
    for stream in range(3):
        first, second, third = ORDER[stream]
        count = COUNT[stream]
        for i in range(4):
            for j in range(4):
                for t in range(count):
                    at = [0, 0, 0]
                    at[first], at[second] = i, j
                    at[third] = (CLASS[stream][t] - i - j) % 4
                    owner = sum(a * s for a, s in zip(at, STRIDE))
                    places[0, BASE[stream] + (j * 4 + i) * count + t] = 2 * owner + HALF[stream][t]
    return places


def pick(mask, new, old):
    return jnp.where(mask[None], new, old)


def kernel(
    tiles_ref, owner_ref, place_ref, depth_hbm, color_hbm,
    depth_out, color_out, thumbs_out,
    in_d, in_c, table_v, table, send_d, send_c, got_d, got_c,
    own_d, own_c, one_d, one_c, mid_d, mid_c, pass_d, pass_c, met_d, met_c, out1_d, out1_c, two_d, two_c, out2_d, out2_c,
    last_d, last_c, thumbs,
    load_sem, table_sem, core_send, core_recv, send1, recv1, send1b, recv1b, send2, recv2, send3, recv3,
    thumb_send, thumb_recv,
):
    gx, gy = lax.axis_index("gx"), lax.axis_index("gy")
    core = lax.rem(gx, 2)
    at = (lax.div(gx, 2), lax.div(gy, 4), lax.rem(gy, 4))
    me = gx * 16 + gy

    def device(x, y, z, c=core):
        return (2 * x + c, 4 * y + z)

    def peer(axis, off):
        moved = [lax.rem(a + off, 4) if k == axis else a for k, a in enumerate(at)]
        return device(*moved)

    partner = device(*at, c=1 - core)

    loads = [
        pltpu.make_async_copy(depth_hbm, in_d.at[pl.ds(0, 128)], load_sem.at[0]),
        pltpu.make_async_copy(color_hbm, in_c.at[pl.ds(0, 128)], load_sem.at[1]),
    ]
    for load in loads:
        load.start()
    barrier = pltpu.get_barrier_semaphore()
    pl.semaphore_signal(barrier, inc=1, device_id=partner, device_id_type=MESH)
    for axis in range(3):
        for off in (1, 2, 3):
            pl.semaphore_signal(barrier, inc=1, device_id=peer(axis, off), device_id_type=MESH)

    in_d[128] = jnp.full((16, 128), FAR, jnp.int32)
    in_c[128] = jnp.zeros((3, 16, 128), jnp.bfloat16)
    tiles = tiles_ref[...]
    live = tiles >= 0
    row = lax.shift_right_arithmetic(tiles, 4)
    region = lax.shift_right_arithmetic(row, 1) * 16 + (tiles & 15)
    down = lax.broadcasted_iota(jnp.int32, (128, 128), 0)
    owner_down = jnp.transpose(jnp.broadcast_to(owner_ref[...], (128, 128)))
    owner = jnp.sum(jnp.where(down == region, owner_down, 0), axis=0, keepdims=True)
    place = jnp.where(live, 2 * owner + (row & 1), -1)
    place_down = jnp.transpose(jnp.broadcast_to(place, (128, 128)))
    for c in range(2):
        hit = place_down == place_ref[...] + 32 * c
        table_v[c : c + 1, :] = jnp.min(jnp.where(hit, down, 128), axis=0, keepdims=True)
    to_table = pltpu.make_async_copy(table_v, table, table_sem)
    to_table.start()
    with jax.named_scope("load"):
        to_table.wait()
        for load in loads:
            load.wait()
    with jax.named_scope("greet"):
        pl.semaphore_wait(barrier, 10)

    def remote(depth, color, sends, recv, target):
        for part, (src, dst) in enumerate((depth, color)):
            pltpu.make_async_remote_copy(
                src_ref=src, dst_ref=dst, send_sem=sends.at[part], recv_sem=recv,
                device_id=target, device_id_type=MESH,
            ).start()

    def wait_bytes(ref, count, sem):
        some = ref.at[pl.ds(0, count)]
        pltpu.make_async_copy(some, some, sem).wait()

    def chunk(stream, off):
        size = 4 * COUNT[stream]
        return BASE[stream] + lax.rem(at[ORDER[stream][1]] + off, 4) * size, size

    for n, (stream, off) in enumerate(CHUNKS):
        start, size = chunk(stream, off)

        def pack(t, carry):
            q = start + t
            slot = table[1 - core, q]
            send_d[q] = in_d[slot]
            send_c[q] = in_c[slot]
            return carry

        lax.fori_loop(0, size, pack, 0, unroll=4)
        part = pl.ds(start, size)
        remote((send_d.at[part], got_d.at[part]), (send_c.at[part], got_c.at[part]), core_send, core_recv.at[n], partner)

    def others(axis):
        c = at[axis]
        return c, c + 1 - 2 * lax.rem(c, 2), lax.rem(c + 2, 4), 3 - c

    def seat(axis, place):
        return device(*(place if k == axis else a for k, a in enumerate(at)))

    for n, (stream, off) in enumerate(CHUNKS):
        start, size = chunk(stream, off)
        axis, count = ORDER[stream][0], COUNT[stream]
        with jax.named_scope(f"core_wait#n={n}"):
            wait_bytes(got_d, size * 5 // 2, core_recv.at[n])
        sent = (1, 2) if off in PLAIN else (2, 3)
        places = others(axis)
        for rel in sent + tuple(r for r in range(4) if r not in sent):
            first, into = start + places[rel] * count, STARTS[n] + rel * count

            def meet(t, carry):
                slot = table[core, first + t]
                mine = (in_d[slot] - FAR) * 2 + core
                other = (got_d[first + t] - FAR) * 2 + (1 - core)
                nearer = other < mine
                own_d[into + t] = jnp.where(nearer, other, mine)
                own_c[into + t] = pick(nearer, got_c[first + t], in_c[slot])
                return carry

            lax.fori_loop(0, count, meet, 0, unroll=True)
            if rel == sent[1]:
                src = pl.ds(STARTS[n] + sent[0] * count, 2 * count)
                dst = pl.ds(STARTS[n] // 2, 2 * count)
                remote(
                    (own_d.at[src], one_d.at[dst]), (own_c.at[src], one_c.at[dst]),
                    send1, recv1.at[n], seat(axis, places[1 if off in PLAIN else 3]),
                )

    def closer(depth, color, best, kept):
        tag, old = color[3].astype(jnp.float32), kept[3].astype(jnp.float32)
        nearer = (depth < best) | ((depth == best) & (tag < old))
        return jnp.where(nearer, depth, best), pick(nearer, color, kept)

    def first_join(n):
        stream, off = CHUNKS[n]
        first, second, third = ORDER[stream]
        count = COUNT[stream]
        places = others(first)
        near, away = (1, 3) if off in PLAIN else (3, 1)
        mine, theirs = places[0], places[near]
        rest = at[second] * STRIDE[second] + at[third] * STRIDE[third]
        lower = jnp.where(theirs < mine, 1, 0)
        with jax.named_scope(f"wait1#n={n}"):
            wait_bytes(one_d, 5 * count, recv1.at[n])
        for part, rel in enumerate((0, 3) if off in PLAIN else (1, 0)):
            to_d, to_c = (pass_d, pass_c) if rel else (mid_d, mid_c)
            base = STARTS[n] // 4

            def join(t, carry):
                p, q = STARTS[n] + rel * count + t, STARTS[n] // 2 + part * count + t
                k, other = own_d[p], one_d[q]
                depth, far_depth = lax.shift_right_arithmetic(k, 1), lax.shift_right_arithmetic(other, 1)
                nearer = far_depth < depth + lower if first == 0 else other < k + lower
                own_rank = rest + mine * STRIDE[first] + (k & 1) * 16
                other_rank = rest + theirs * STRIDE[first] + (other & 1) * 16
                to_d[base + t] = jnp.where(nearer, far_depth, depth)
                to_c[base + t, 0:3] = pick(nearer, one_c[q], own_c[p])
                to_c[base + t, 3] = jnp.where(nearer, other_rank, own_rank).astype(jnp.float32).astype(jnp.bfloat16)
                return carry

            lax.fori_loop(0, count, join, 0)
        part = pl.ds(STARTS[n] // 4, count)
        remote(
            (pass_d.at[part], met_d.at[part]), (pass_c.at[part], met_c.at[part]),
            send1b, recv1b.at[n], seat(first, places[away]),
        )

    def second_join(n):
        stream, off = CHUNKS[n]
        second, count = ORDER[stream][1], COUNT[stream]
        base, into = STARTS[n] // 4, BASE[stream] // 4
        if off:
            to_d, to_c, into = out1_d, out1_c, into + (off - 1) * count
        else:
            to_d, to_c, into = two_d, two_c, into + at[second] * count
        with jax.named_scope(f"wait1b#n={n}"):
            wait_bytes(one_d, 3 * count, recv1b.at[n])

        def join(t, carry):
            q = base + t
            to_d[into + t], to_c[into + t] = closer(met_d[q], met_c[q], mid_d[q], mid_c[q])
            return carry

        lax.fori_loop(0, count, join, 0)
        if off:
            src = pl.ds(into, count)
            dst = pl.ds(BASE[stream] // 4 + at[second] * count, count)
            remote((out1_d.at[src], two_d.at[dst]), (out1_c.at[src], two_c.at[dst]), send2, recv2.at[stream], peer(second, off))

    for n in range(12):
        first_join(n)
    for n in range(12):
        second_join(n)

    mine = lax.rem(at[0] + at[1] + at[2], 4)
    for stream in (2, 1, 0):
        count, base = COUNT[stream], BASE[stream] // 4
        with jax.named_scope(f"wait2#s={stream}"):
            wait_bytes(two_d, 9 * count, recv2.at[stream])
        for t in range(count):
            best, kept = two_d[base + t], two_c[base + t]
            for src in (1, 2, 3):
                q = base + src * count + t
                best, kept = closer(two_d[q], two_c[q], best, kept)
            group, half = CLASS[stream][t], HALF[stream][t]
            k = 2 * group + half
            out2_d[k] = best
            out2_c[k] = kept
            off = lax.rem(group - mine + 4, 4)

            @pl.when(off != 0)
            def send():
                slot = 3 * half + off - 1
                remote(
                    (out2_d.at[k], last_d.at[slot]), (out2_c.at[k], last_c.at[slot]),
                    send3, recv3, peer(ORDER[stream][2], off),
                )

    with jax.named_scope("wait3"):
        wait_bytes(one_d, 18, recv3)
    sums = []
    for half in range(2):
        best, kept = out2_d[2 * mine + half], out2_c[2 * mine + half]
        for off in (1, 2, 3):
            slot = 3 * half + off - 1
            best, kept = closer(last_d[slot], last_c[slot], best, kept)
        depth_out[half] = best + FAR
        color_out[half] = kept[0:3]
        sums.append(jnp.sum(kept[0:3].astype(jnp.float32).reshape(3, 2, 8, 128), axis=2))
    rows = jnp.concatenate(
        [s for c in range(3) for s in (sums[0][c], sums[1][c])] + [jnp.zeros((4, 128), jnp.float32)], axis=0
    )
    lane_down = lax.broadcasted_iota(jnp.int32, (128, 128), 0)
    lane = lax.broadcasted_iota(jnp.int32, (128, 128), 1)
    spread = jnp.where(lax.shift_right_logical(lane_down, 3) == (lane & 15), 1.0 / 64, 0.0)
    means = jnp.dot(rows, spread, precision=lax.Precision.HIGHEST, preferred_element_type=jnp.float32)
    line = lax.broadcasted_iota(jnp.int32, (16, 128), 0) & 7
    group = lax.shift_right_logical(lax.broadcasted_iota(jnp.int32, (16, 128), 1), 4)
    thumbs[me] = jnp.sum(jnp.where(line == group, means, 0.0).reshape(2, 8, 128), axis=1)

    around = [[lax.rem(a + off, 4) for off in range(4)] for a in at]
    across = [[2 * a + c for a in around[0]] for c in (core, 1 - core)]
    along = [[4 * b + c for c in around[2]] for b in around[1]]
    for dx, dy, dz in FAR_FIRST:
        for other in range(2):
            if dx or dy or dz or other:
                pltpu.make_async_remote_copy(
                    src_ref=thumbs.at[me], dst_ref=thumbs.at[me], send_sem=thumb_send, recv_sem=thumb_recv,
                    device_id=(across[other][dx], along[dy][dz]), device_id_type=MESH,
                ).start()
    for sends, depth_ref, color_ref, count in (
        (core_send, send_d, send_c, 128), (send1, own_d, own_c, 64), (send1b, met_d, met_c, 32),
        (send2, two_d, two_c, 24), (send3, last_d, last_c, 6),
    ):
        wait_bytes(depth_ref, count, sends.at[0])
        wait_bytes(color_ref, count, sends.at[1])
    with jax.named_scope("thumb_wait"):
        wait_bytes(thumbs, 127, thumb_recv)
    wait_bytes(thumbs, 127, thumb_send)
    thumbs_out[...] = thumbs[...]


def settle(owner_ref, depth_ref, color_ref, thumbs_ref, depth_out, color_out, thumbs_out):
    depth_out[...] = depth_ref[...]
    color_out[...] = color_ref[...]
    held = lax.broadcasted_iota(jnp.int32, (128, 128), 0) == owner_ref[...]
    chosen = jnp.where(held, 1.0, 0.0)
    for row, size in ((0, 128), (1, 64)):
        thumbs_out[128 * row : 128 * row + size] = lax.dot_general(
            thumbs_ref[:, row, 0:size], chosen, (((0,), (0,)), ((), ())),
            precision=lax.Precision.HIGHEST, preferred_element_type=jnp.float32,
        )


def shards(slot_tiles, owner_map, slot_depth, slot_color):
    i32, bf16 = jnp.int32, jnp.bfloat16
    vmem = pl.BlockSpec(memory_space=pltpu.VMEM)
    anywhere = pl.BlockSpec(memory_space=pl.ANY)
    dma = pltpu.SemaphoreType.DMA
    scratch = [
        pltpu.VMEM((129, 16, 128), i32), pltpu.VMEM((129, 3, 16, 128), bf16),
        pltpu.VMEM((2, 128), i32), pltpu.SMEM((2, 128), i32),
    ]
    for tiles, channels in ((128, 3), (128, 3), (128, 3), (64, 3), (32, 4), (32, 4), (32, 4), (32, 4), (32, 4), (8, 4), (6, 4)):
        scratch += [pltpu.VMEM((tiles, 16, 128), i32), pltpu.VMEM((tiles, channels, 16, 128), bf16)]
    scratch += [pltpu.VMEM((128, 2, 128), jnp.float32), dma((2,)), dma]
    scratch += [dma((2,)), dma((12,)), dma((2,)), dma((12,)), dma((2,)), dma((12,)), dma((2,)), dma((3,)), dma((2,)), dma]
    scratch += [dma, dma]
    depth, color, thumbs = pl.pallas_call(
        kernel,
        out_shape=(
            pltpu.VMEM((2, 16, 128), i32),
            pltpu.VMEM((2, 3, 16, 128), bf16),
            pltpu.VMEM((128, 2, 128), jnp.float32),
        ),
        in_specs=[vmem, vmem, vmem, anywhere, anywhere],
        out_specs=(vmem, vmem, vmem),
        scratch_shapes=scratch,
        compiler_params=pltpu.CompilerParams(collective_id=0, has_side_effects=True),
        name="composite",
    )(
        slot_tiles,
        owner_map[None],
        jnp.asarray(tile_places()),
        slot_depth[0],
        jnp.swapaxes(slot_color[0], 1, 2),
    )
    depth, color, thumbs = pl.pallas_call(
        settle,
        out_shape=(
            jax.ShapeDtypeStruct((2, 16, 128), i32),
            jax.ShapeDtypeStruct((2, 3, 16, 128), bf16),
            jax.ShapeDtypeStruct((192, 128), jnp.float32),
        ),
        in_specs=[vmem] * 4,
        out_specs=(vmem, vmem, vmem),
        compiler_params=pltpu.CompilerParams(vmem_limit_bytes=8 << 20),
        name="settle",
    )(owner_map[None], depth, color, thumbs)
    thumbnail = jnp.transpose(thumbs.reshape(3, 64, 128), (2, 0, 1))
    return depth[None], jnp.swapaxes(color, 1, 2)[None], thumbnail


def solution(mesh):
    ranks = ("gx", "gy")
    return jax.shard_map(
        shards,
        mesh=mesh,
        in_specs=(P(ranks, None), P(), P(ranks, None, None, None), P(ranks, None, None, None, None)),
        out_specs=(P(ranks, None, None, None), P(ranks, None, None, None, None), P()),
        check_vma=False,
    )
```

```python
import jax
import jax.numpy as jnp
import numpy as np
from jax import lax
from jax.experimental import pallas as pl
from jax.experimental.pallas import tpu as pltpu
from jax.sharding import PartitionSpec as P

MESH = pl.DeviceIdType.MESH
FAR = 1073741824
ORDER = ((0, 1, 2), (1, 2, 0), (2, 0, 1))
STRIDE = (32, 4, 1)
COUNT = (3, 3, 2)
BASE = (0, 48, 96)
CLASS = ((0, 2, 3), (0, 1, 3), (1, 2))
HALF = ((0, 1, 0), (1, 0, 1), (1, 0))
CHUNKS = tuple((stream, off) for off in (2, 1, 3, 0) for stream in range(3))
PLAIN = (2, 3)
SINGLE = (2, 1, 3)


def parts():
    out = []
    for first in range(0, 12, 3):
        chunks = range(first, first + 3)
        if CHUNKS[first][1] in SINGLE:
            out += [(n, t, 1) for t in range(3) for n in chunks if t < COUNT[CHUNKS[n][0]]]
        else:
            out += [(n, 0, COUNT[CHUNKS[n][0]]) for n in chunks]
    return tuple(out)


PARTS = parts()
STARTS = tuple(sum(4 * count for _, _, count in PARTS[:m]) for m in range(len(PARTS)))
KEPT = len(PARTS) - 3
FAR_FIRST = sorted(np.ndindex(4, 4, 4), key=lambda d: -sum(min(a, 4 - a) for a in d))


def tile_places():
    places = np.zeros((1, 128), np.int32)
    for stream in range(3):
        first, second, third = ORDER[stream]
        count = COUNT[stream]
        for i in range(4):
            for j in range(4):
                for t in range(count):
                    at = [0, 0, 0]
                    at[first], at[second] = i, j
                    at[third] = (CLASS[stream][t] - i - j) % 4
                    owner = sum(a * s for a, s in zip(at, STRIDE))
                    places[0, BASE[stream] + (j * 4 + i) * count + t] = 2 * owner + HALF[stream][t]
    return places


def pick(mask, new, old):
    return jnp.where(mask[None], new, old)


def kernel(
    tiles_ref, owner_ref, place_ref, depth_hbm, color_hbm,
    depth_out, color_out, thumbs_out,
    in_d, in_c, table_v, table, send_d, send_c, got_d, got_c,
    own_d, own_c, one_d, one_c, mid_d, mid_c, pass_d, pass_c, met_d, met_c, keep_d, keep_c, out1_d, out1_c, two_d, two_c, out2_d, out2_c,
    last_d, last_c, thumbs,
    load_sem, table_sem, core_send, core_recv, send1, recv1, send1b, recv1b, send2, recv2, send3, recv3,
    thumb_send, thumb_recv,
):
    gx, gy = lax.axis_index("gx"), lax.axis_index("gy")
    core = lax.rem(gx, 2)
    at = (lax.div(gx, 2), lax.div(gy, 4), lax.rem(gy, 4))
    me = gx * 16 + gy

    def device(x, y, z, c=core):
        return (2 * x + c, 4 * y + z)

    def peer(axis, off):
        moved = [lax.rem(a + off, 4) if k == axis else a for k, a in enumerate(at)]
        return device(*moved)

    partner = device(*at, c=1 - core)

    loads = [
        pltpu.make_async_copy(depth_hbm, in_d.at[pl.ds(0, 128)], load_sem.at[0]),
        pltpu.make_async_copy(color_hbm, in_c.at[pl.ds(0, 128)], load_sem.at[1]),
    ]
    for load in loads:
        load.start()
    barrier = pltpu.get_barrier_semaphore()
    pl.semaphore_signal(barrier, inc=1, device_id=partner, device_id_type=MESH)
    for axis in range(3):
        for off in (1, 2, 3):
            pl.semaphore_signal(barrier, inc=1, device_id=peer(axis, off), device_id_type=MESH)

    in_d[128] = jnp.full((16, 128), FAR, jnp.int32)
    in_c[128] = jnp.zeros((3, 16, 128), jnp.bfloat16)
    tiles = tiles_ref[...]
    live = tiles >= 0
    row = lax.shift_right_arithmetic(tiles, 4)
    region = lax.shift_right_arithmetic(row, 1) * 16 + (tiles & 15)
    down = lax.broadcasted_iota(jnp.int32, (128, 128), 0)
    owner_down = jnp.transpose(jnp.broadcast_to(owner_ref[...], (128, 128)))
    owner = jnp.sum(jnp.where(down == region, owner_down, 0), axis=0, keepdims=True)
    place = jnp.where(live, 2 * owner + (row & 1), -1)
    place_down = jnp.transpose(jnp.broadcast_to(place, (128, 128)))
    for c in range(2):
        hit = place_down == place_ref[...] + 32 * c
        table_v[c : c + 1, :] = jnp.min(jnp.where(hit, down, 128), axis=0, keepdims=True)
    to_table = pltpu.make_async_copy(table_v, table, table_sem)
    to_table.start()
    with jax.named_scope("load"):
        to_table.wait()
        for load in loads:
            load.wait()
    with jax.named_scope("greet"):
        pl.semaphore_wait(barrier, 10)

    def remote(depth, color, sends, recv, target):
        for part, (src, dst) in enumerate((depth, color)):
            pltpu.make_async_remote_copy(
                src_ref=src, dst_ref=dst, send_sem=sends.at[part], recv_sem=recv,
                device_id=target, device_id_type=MESH,
            ).start()

    def wait_bytes(ref, count, sem):
        some = ref.at[pl.ds(0, count)]
        pltpu.make_async_copy(some, some, sem).wait()

    def chunk(stream, off):
        size = 4 * COUNT[stream]
        return BASE[stream] + lax.rem(at[ORDER[stream][1]] + off, 4) * size, size

    for n, (stream, off) in enumerate(CHUNKS):
        start, size = chunk(stream, off)

        def pack(t, carry):
            q = start + t
            slot = table[1 - core, q]
            send_d[q] = in_d[slot]
            send_c[q] = in_c[slot]
            return carry

        lax.fori_loop(0, size, pack, 0, unroll=4)
        part = pl.ds(start, size)
        remote((send_d.at[part], got_d.at[part]), (send_c.at[part], got_c.at[part]), core_send, core_recv.at[n], partner)

    def others(axis):
        c = at[axis]
        return c, c + 1 - 2 * lax.rem(c, 2), lax.rem(c + 2, 4), 3 - c

    def seat(axis, place):
        return device(*(place if k == axis else a for k, a in enumerate(at)))

    def piece(m):
        n, skip, count = PARTS[m]
        return *CHUNKS[n], skip, count

    def first_send(n):
        stream, off, _, count = piece(n)
        axis = ORDER[stream][0]
        near, skip = (1, 1) if off in PLAIN else (3, 2)
        src = pl.ds(STARTS[n] + skip * count, 2 * count)
        dst = pl.ds(STARTS[n] // 2, 2 * count)
        remote(
            (own_d.at[src], one_d.at[dst]), (own_c.at[src], one_c.at[dst]),
            send1, recv1.at[n], seat(axis, others(axis)[near]),
        )

    def keep_send(n, rel):
        stream, off, _, count = piece(n)
        axis = ORDER[stream][0]
        src = pl.ds(STARTS[n] + rel * count, count)
        dst = pl.ds((STARTS[n] - STARTS[KEPT]) // 4 * 3 + (rel - 1) * count, count)
        remote(
            (own_d.at[src], keep_d.at[dst]), (own_c.at[src], keep_c.at[dst]),
            send1, recv1.at[n], seat(axis, others(axis)[rel]),
        )

    def meet_part(m, start):
        stream, off, skip, count = piece(m)
        places = others(ORDER[stream][0])
        for rel in (3, 2, 1, 0) if off not in PLAIN else (1, 2, 3, 0):
            first, into = start + places[rel] * COUNT[stream] + skip, STARTS[m] + rel * count

            def meet(t, carry):
                slot = table[core, first + t]
                mine = (in_d[slot] - FAR) * 2 + core
                other = (got_d[first + t] - FAR) * 2 + (1 - core)
                nearer = other < mine
                own_d[into + t] = jnp.where(nearer, other, mine)
                own_c[into + t] = pick(nearer, got_c[first + t], in_c[slot])
                return carry

            lax.fori_loop(0, count, meet, 0, unroll=True)
            if rel == 2 and off:
                first_send(m)
            if rel == 3 and not off:
                keep_send(m, rel)

    for n, (stream, off) in enumerate(CHUNKS):
        start, size = chunk(stream, off)
        with jax.named_scope(f"core_wait#n={n}"):
            wait_bytes(got_d, size * 5 // 2, core_recv.at[n])
        for m in range(len(PARTS)):
            if PARTS[m][0] == n:
                meet_part(m, start)

    def closer(depth, color, best, kept):
        tag, old = color[3].astype(jnp.float32), kept[3].astype(jnp.float32)
        nearer = (depth < best) | ((depth == best) & (tag < old))
        return jnp.where(nearer, depth, best), pick(nearer, color, kept)

    def first_join(n):
        stream, off, _, count = piece(n)
        first, second, third = ORDER[stream]
        places = others(first)
        near, away = (1, 3) if off in PLAIN else (3, 1)
        mine, theirs = places[0], places[near]
        rest = at[second] * STRIDE[second] + at[third] * STRIDE[third]
        lower = jnp.where(theirs < mine, 1, 0)
        with jax.named_scope(f"wait1#n={n}"):
            wait_bytes(one_d, 5 * count, recv1.at[n])
        for part, rel in enumerate((0, 3) if off in PLAIN else (1, 0)):
            to_d, to_c = (pass_d, pass_c) if rel else (mid_d, mid_c)
            base = STARTS[n] // 4

            def join(t, carry):
                p, q = STARTS[n] + rel * count + t, STARTS[n] // 2 + part * count + t
                k, other = own_d[p], one_d[q]
                depth, far_depth = lax.shift_right_arithmetic(k, 1), lax.shift_right_arithmetic(other, 1)
                nearer = far_depth < depth + lower if first == 0 else other < k + lower
                own_rank = rest + mine * STRIDE[first] + (k & 1) * 16
                other_rank = rest + theirs * STRIDE[first] + (other & 1) * 16
                to_d[base + t] = jnp.where(nearer, far_depth, depth)
                to_c[base + t, 0:3] = pick(nearer, one_c[q], own_c[p])
                to_c[base + t, 3] = jnp.where(nearer, other_rank, own_rank).astype(jnp.float32).astype(jnp.bfloat16)
                return carry

            lax.fori_loop(0, count, join, 0)
        part = pl.ds(STARTS[n] // 4, count)
        remote(
            (pass_d.at[part], met_d.at[part]), (pass_c.at[part], met_c.at[part]),
            send1b, recv1b.at[n], seat(first, places[away]),
        )

    def second_join(n):
        stream, off, skip, count = piece(n)
        second = ORDER[stream][1]
        base, into = STARTS[n] // 4, BASE[stream] // 4 + (off - 1) * COUNT[stream] + skip
        with jax.named_scope(f"wait1b#n={n}"):
            wait_bytes(one_d, 3 * count, recv1b.at[n])

        def join(t, carry):
            q = base + t
            out1_d[into + t], out1_c[into + t] = closer(met_d[q], met_c[q], mid_d[q], mid_c[q])
            return carry

        lax.fori_loop(0, count, join, 0)
        src = pl.ds(into, count)
        dst = pl.ds(BASE[stream] // 4 + at[second] * COUNT[stream] + skip, count)
        remote((out1_d.at[src], two_d.at[dst]), (out1_c.at[src], two_c.at[dst]), send2, recv2.at[stream], peer(second, off))

    def keep_join(n):
        stream, off, _, count = piece(n)
        first, second, third = ORDER[stream]
        base = (STARTS[n] - STARTS[KEPT]) // 4 * 3
        into = BASE[stream] // 4 + at[second] * count
        places = others(first)
        rest = at[second] * STRIDE[second] + at[third] * STRIDE[third]
        with jax.named_scope(f"keep_wait#n={n}"):
            wait_bytes(own_c, 5 * count, recv1.at[n])

        def join(t, carry):
            best = tag = color = None
            for rel in range(4):
                q = base + (rel - 1) * count + t
                k, new = (keep_d[q], keep_c[q]) if rel else (own_d[STARTS[n] + t], own_c[STARTS[n] + t])
                depth = lax.shift_right_arithmetic(k, 1)
                rank = rest + places[rel] * STRIDE[first] + (k & 1) * 16
                if rel == 0:
                    best, tag, color = depth, rank, new
                else:
                    nearer = (depth < best) | ((depth == best) & (rank < tag))
                    best, tag = jnp.where(nearer, depth, best), jnp.where(nearer, rank, tag)
                    color = pick(nearer, new, color)
            two_d[into + t] = best
            two_c[into + t, 0:3] = color
            two_c[into + t, 3] = tag.astype(jnp.float32).astype(jnp.bfloat16)
            return carry

        lax.fori_loop(0, count, join, 0)

    last_of = {PARTS[m][0]: m for m in range(KEPT)}
    for m in range(KEPT):
        first_join(m)
        for n in range(6):
            if last_of[n] == m:
                keep_send(KEPT + n % 3, 2 - n // 3)
    for m in range(KEPT):
        second_join(m)
    for m in range(KEPT, len(PARTS)):
        keep_join(m)

    mine = lax.rem(at[0] + at[1] + at[2], 4)
    for stream in (2, 1, 0):
        count, base = COUNT[stream], BASE[stream] // 4
        with jax.named_scope(f"wait2#s={stream}"):
            wait_bytes(two_d, 9 * count, recv2.at[stream])
        for t in range(count):
            best, kept = two_d[base + t], two_c[base + t]
            for src in (1, 2, 3):
                q = base + src * count + t
                best, kept = closer(two_d[q], two_c[q], best, kept)
            group, half = CLASS[stream][t], HALF[stream][t]
            k = 2 * group + half
            out2_d[k] = best
            out2_c[k] = kept
            off = lax.rem(group - mine + 4, 4)

            @pl.when(off != 0)
            def send():
                slot = 3 * half + off - 1
                remote(
                    (out2_d.at[k], last_d.at[slot]), (out2_c.at[k], last_c.at[slot]),
                    send3, recv3, peer(ORDER[stream][2], off),
                )

    with jax.named_scope("wait3"):
        wait_bytes(one_d, 18, recv3)
    sums = []
    for half in range(2):
        best, kept = out2_d[2 * mine + half], out2_c[2 * mine + half]
        for off in (1, 2, 3):
            slot = 3 * half + off - 1
            best, kept = closer(last_d[slot], last_c[slot], best, kept)
        depth_out[half] = best + FAR
        color_out[half] = kept[0:3]
        sums.append(jnp.sum(kept[0:3].astype(jnp.float32).reshape(3, 2, 8, 128), axis=2))
    rows = jnp.concatenate(
        [s for c in range(3) for s in (sums[0][c], sums[1][c])] + [jnp.zeros((4, 128), jnp.float32)], axis=0
    )
    lane_down = lax.broadcasted_iota(jnp.int32, (128, 128), 0)
    lane = lax.broadcasted_iota(jnp.int32, (128, 128), 1)
    spread = jnp.where(lax.shift_right_logical(lane_down, 3) == (lane & 15), 1.0 / 64, 0.0)
    means = jnp.dot(rows, spread, precision=lax.Precision.HIGHEST, preferred_element_type=jnp.float32)
    line = lax.broadcasted_iota(jnp.int32, (16, 128), 0) & 7
    group = lax.shift_right_logical(lax.broadcasted_iota(jnp.int32, (16, 128), 1), 4)
    thumbs[me] = jnp.sum(jnp.where(line == group, means, 0.0).reshape(2, 8, 128), axis=1)

    around = [[lax.rem(a + off, 4) for off in range(4)] for a in at]
    across = [[2 * a + c for a in around[0]] for c in (core, 1 - core)]
    along = [[4 * b + c for c in around[2]] for b in around[1]]
    for dx, dy, dz in FAR_FIRST:
        for other in range(2):
            if dx or dy or dz or other:
                pltpu.make_async_remote_copy(
                    src_ref=thumbs.at[me], dst_ref=thumbs.at[me], send_sem=thumb_send, recv_sem=thumb_recv,
                    device_id=(across[other][dx], along[dy][dz]), device_id_type=MESH,
                ).start()
    for sends, depth_ref, color_ref, count in (
        (core_send, send_d, send_c, 128), (send1, own_d, own_c, 72), (send1b, met_d, met_c, 24),
        (send2, two_d, two_c, 24), (send3, last_d, last_c, 6),
    ):
        wait_bytes(depth_ref, count, sends.at[0])
        wait_bytes(color_ref, count, sends.at[1])
    with jax.named_scope("thumb_wait"):
        wait_bytes(thumbs, 127, thumb_recv)
    wait_bytes(thumbs, 127, thumb_send)
    thumbs_out[...] = thumbs[...]


def settle(owner_ref, depth_ref, color_ref, thumbs_ref, depth_out, color_out, thumbs_out):
    depth_out[...] = depth_ref[...]
    color_out[...] = color_ref[...]
    held = lax.broadcasted_iota(jnp.int32, (128, 128), 0) == owner_ref[...]
    chosen = jnp.where(held, 1.0, 0.0)
    for row, size in ((0, 128), (1, 64)):
        thumbs_out[128 * row : 128 * row + size] = lax.dot_general(
            thumbs_ref[:, row, 0:size], chosen, (((0,), (0,)), ((), ())),
            precision=lax.Precision.HIGHEST, preferred_element_type=jnp.float32,
        )


def shards(slot_tiles, owner_map, slot_depth, slot_color):
    i32, bf16 = jnp.int32, jnp.bfloat16
    vmem = pl.BlockSpec(memory_space=pltpu.VMEM)
    anywhere = pl.BlockSpec(memory_space=pl.ANY)
    dma = pltpu.SemaphoreType.DMA
    scratch = [
        pltpu.VMEM((129, 16, 128), i32), pltpu.VMEM((129, 3, 16, 128), bf16),
        pltpu.VMEM((2, 128), i32), pltpu.SMEM((2, 128), i32),
    ]
    for tiles, channels in ((128, 3), (128, 3), (128, 3), (48, 3), (24, 4), (24, 4), (24, 4), (24, 3), (32, 4), (32, 4), (8, 4), (6, 4)):
        scratch += [pltpu.VMEM((tiles, 16, 128), i32), pltpu.VMEM((tiles, channels, 16, 128), bf16)]
    scratch += [pltpu.VMEM((128, 2, 128), jnp.float32), dma((2,)), dma]
    scratch += [dma((2,)), dma((12,)), dma((2,)), dma((len(PARTS),)), dma((2,)), dma((KEPT,)), dma((2,)), dma((3,)), dma((2,)), dma]
    scratch += [dma, dma]
    depth, color, thumbs = pl.pallas_call(
        kernel,
        out_shape=(
            pltpu.VMEM((2, 16, 128), i32),
            pltpu.VMEM((2, 3, 16, 128), bf16),
            pltpu.VMEM((128, 2, 128), jnp.float32),
        ),
        in_specs=[vmem, vmem, vmem, anywhere, anywhere],
        out_specs=(vmem, vmem, vmem),
        scratch_shapes=scratch,
        compiler_params=pltpu.CompilerParams(collective_id=0, has_side_effects=True),
        name="composite",
    )(
        slot_tiles,
        owner_map[None],
        jnp.asarray(tile_places()),
        slot_depth[0],
        jnp.swapaxes(slot_color[0], 1, 2),
    )
    depth, color, thumbs = pl.pallas_call(
        settle,
        out_shape=(
            jax.ShapeDtypeStruct((2, 16, 128), i32),
            jax.ShapeDtypeStruct((2, 3, 16, 128), bf16),
            jax.ShapeDtypeStruct((192, 128), jnp.float32),
        ),
        in_specs=[vmem] * 4,
        out_specs=(vmem, vmem, vmem),
        compiler_params=pltpu.CompilerParams(vmem_limit_bytes=8 << 20),
        name="settle",
    )(owner_map[None], depth, color, thumbs)
    thumbnail = jnp.transpose(thumbs.reshape(3, 64, 128), (2, 0, 1))
    return depth[None], jnp.swapaxes(color, 1, 2)[None], thumbnail


def solution(mesh):
    ranks = ("gx", "gy")
    return jax.shard_map(
        shards,
        mesh=mesh,
        in_specs=(P(ranks, None), P(), P(ranks, None, None, None), P(ranks, None, None, None, None)),
        out_specs=(P(ranks, None, None, None), P(ranks, None, None, None, None), P()),
        check_vma=False,
    )
```

```python
import jax
import jax.numpy as jnp
import numpy as np
from jax import lax
from jax.experimental import pallas as pl
from jax.experimental.pallas import tpu as pltpu
from jax.sharding import PartitionSpec as P

MESH = pl.DeviceIdType.MESH
FAR = 1073741824
ORDER = ((0, 1, 2), (1, 2, 0), (2, 0, 1))
STRIDE = (32, 4, 1)
COUNT = (3, 3, 2)
BASE = (0, 48, 96)
CLASS = ((0, 2, 3), (0, 1, 3), (1, 2))
HALF = ((0, 1, 0), (1, 0, 1), (1, 0))
CHUNKS = tuple((stream, off) for off in (2, 1, 3, 0) for stream in range(3))
PLAIN = (2, 3)
SINGLE = (2, 1, 3)


def parts():
    out = []
    for first in range(0, 12, 3):
        chunks = range(first, first + 3)
        if CHUNKS[first][1] in SINGLE:
            out += [(n, t, 1) for t in range(3) for n in chunks if t < COUNT[CHUNKS[n][0]]]
        else:
            out += [(n, 0, COUNT[CHUNKS[n][0]]) for n in chunks]
    return tuple(out)


PARTS = parts()
STARTS = tuple(sum(4 * count for _, _, count in PARTS[:m]) for m in range(len(PARTS)))
KEPT = len(PARTS) - 3
ROUNDS = sorted({(n // 3, t if n < 9 else 0) for n, t, _ in PARTS})
ROUND = tuple(ROUNDS.index((n // 3, t)) for n, t, _ in PARTS)
FAR_FIRST = sorted(np.ndindex(4, 4, 4), key=lambda d: -sum(min(a, 4 - a) for a in d))


def tile_places():
    places = np.zeros((1, 128), np.int32)
    for stream in range(3):
        first, second, third = ORDER[stream]
        count = COUNT[stream]
        for i in range(4):
            for j in range(4):
                for t in range(count):
                    at = [0, 0, 0]
                    at[first], at[second] = i, j
                    at[third] = (CLASS[stream][t] - i - j) % 4
                    owner = sum(a * s for a, s in zip(at, STRIDE))
                    places[0, BASE[stream] + (j * 4 + i) * count + t] = 2 * owner + HALF[stream][t]
    return places


def pick(mask, new, old):
    return jnp.where(mask[None], new, old)


def kernel(
    tiles_ref, owner_ref, place_ref, depth_hbm, color_hbm,
    depth_out, color_out, thumbs_out,
    in_d, in_c, table_v, table, send_d, send_c, got_d, got_c,
    own_d, own_c, one_d, one_c, mid_d, mid_c, pass_d, pass_c, met_d, met_c, keep_d, keep_c, out1_d, out1_c, two_d, two_c, out2_d, out2_c,
    last_d, last_c, thumbs,
    load_sem, table_sem, core_send, core_recv, send1, recv1, send1b, recv1b, send2, recv2, send3, recv3,
    thumb_send, thumb_recv,
):
    gx, gy = lax.axis_index("gx"), lax.axis_index("gy")
    core = lax.rem(gx, 2)
    at = (lax.div(gx, 2), lax.div(gy, 4), lax.rem(gy, 4))
    me = gx * 16 + gy

    def device(x, y, z, c=core):
        return (2 * x + c, 4 * y + z)

    def peer(axis, off):
        moved = [lax.rem(a + off, 4) if k == axis else a for k, a in enumerate(at)]
        return device(*moved)

    partner = device(*at, c=1 - core)

    loads = [
        pltpu.make_async_copy(depth_hbm, in_d.at[pl.ds(0, 128)], load_sem.at[0]),
        pltpu.make_async_copy(color_hbm, in_c.at[pl.ds(0, 128)], load_sem.at[1]),
    ]
    for load in loads:
        load.start()
    barrier = pltpu.get_barrier_semaphore()
    pl.semaphore_signal(barrier, inc=1, device_id=partner, device_id_type=MESH)
    for axis in range(3):
        for off in (1, 2, 3):
            pl.semaphore_signal(barrier, inc=1, device_id=peer(axis, off), device_id_type=MESH)

    in_d[128] = jnp.full((16, 128), FAR, jnp.int32)
    in_c[128] = jnp.zeros((3, 16, 128), jnp.bfloat16)
    tiles = tiles_ref[...]
    live = tiles >= 0
    row = lax.shift_right_arithmetic(tiles, 4)
    region = lax.shift_right_arithmetic(row, 1) * 16 + (tiles & 15)
    down = lax.broadcasted_iota(jnp.int32, (128, 128), 0)
    owner_down = jnp.transpose(jnp.broadcast_to(owner_ref[...], (128, 128)))
    owner = jnp.sum(jnp.where(down == region, owner_down, 0), axis=0, keepdims=True)
    place = jnp.where(live, 2 * owner + (row & 1), -1)
    place_down = jnp.transpose(jnp.broadcast_to(place, (128, 128)))
    for c in range(2):
        hit = place_down == place_ref[...] + 32 * c
        table_v[c : c + 1, :] = jnp.min(jnp.where(hit, down, 128), axis=0, keepdims=True)
    to_table = pltpu.make_async_copy(table_v, table, table_sem)
    to_table.start()
    with jax.named_scope("load"):
        to_table.wait()
        for load in loads:
            load.wait()
    with jax.named_scope("greet"):
        pl.semaphore_wait(barrier, 10)

    def remote(depth, color, sends, recv, target):
        for part, (src, dst) in enumerate((depth, color)):
            pltpu.make_async_remote_copy(
                src_ref=src, dst_ref=dst, send_sem=sends.at[part], recv_sem=recv,
                device_id=target, device_id_type=MESH,
            ).start()

    def wait_bytes(ref, count, sem):
        some = ref.at[pl.ds(0, count)]
        pltpu.make_async_copy(some, some, sem).wait()

    def chunk(stream, off):
        size = 4 * COUNT[stream]
        return BASE[stream] + lax.rem(at[ORDER[stream][1]] + off, 4) * size, size

    def slot_of(n):
        return n if n < 6 else 4 + n // 3

    for n, (stream, off) in enumerate(CHUNKS):
        start, size = chunk(stream, off)

        def pack(t, carry):
            q = start + t
            slot = table[1 - core, q]
            send_d[q] = in_d[slot]
            send_c[q] = in_c[slot]
            return carry

        lax.fori_loop(0, size, pack, 0, unroll=4)
        part = pl.ds(start, size)
        remote((send_d.at[part], got_d.at[part]), (send_c.at[part], got_c.at[part]), core_send, core_recv.at[slot_of(n)], partner)

    def others(axis):
        c = at[axis]
        return c, c + 1 - 2 * lax.rem(c, 2), lax.rem(c + 2, 4), 3 - c

    def seat(axis, place):
        return device(*(place if k == axis else a for k, a in enumerate(at)))

    def opens(m):
        if m and ROUND[m] == ROUND[m - 1]:
            return 0
        return sum(count for (_, _, count), r in zip(PARTS, ROUND) if r == ROUND[m])

    def piece(m):
        n, skip, count = PARTS[m]
        return *CHUNKS[n], skip, count

    def first_send(n):
        stream, off, _, count = piece(n)
        axis = ORDER[stream][0]
        near, skip = (1, 1) if off in PLAIN else (3, 2)
        src = pl.ds(STARTS[n] + skip * count, 2 * count)
        dst = pl.ds(STARTS[n] // 2, 2 * count)
        remote(
            (own_d.at[src], one_d.at[dst]), (own_c.at[src], one_c.at[dst]),
            send1, recv1.at[ROUND[n]], seat(axis, others(axis)[near]),
        )

    def keep_send(n, rel):
        stream, off, _, count = piece(n)
        axis = ORDER[stream][0]
        src = pl.ds(STARTS[n] + rel * count, count)
        dst = pl.ds((STARTS[n] - STARTS[KEPT]) // 4 * 3 + (rel - 1) * count, count)
        remote(
            (own_d.at[src], keep_d.at[dst]), (own_c.at[src], keep_c.at[dst]),
            send1, recv1.at[ROUND[n]], seat(axis, others(axis)[rel]),
        )

    def meet_part(m, start):
        stream, off, skip, count = piece(m)
        places = others(ORDER[stream][0])
        for rel in (3, 2, 1, 0) if off not in PLAIN else (1, 2, 3, 0):
            first, into = start + places[rel] * COUNT[stream] + skip, STARTS[m] + rel * count

            def meet(t, carry):
                slot = table[core, first + t]
                mine = (in_d[slot] - FAR) * 2 + core
                other = (got_d[first + t] - FAR) * 2 + (1 - core)
                nearer = other < mine
                own_d[into + t] = jnp.where(nearer, other, mine)
                own_c[into + t] = pick(nearer, got_c[first + t], in_c[slot])
                return carry

            lax.fori_loop(0, count, meet, 0, unroll=True)
            if rel == 2 and off:
                first_send(m)
            if rel == 3 and not off:
                keep_send(m, rel)

    for n, (stream, off) in enumerate(CHUNKS):
        start, size = chunk(stream, off)
        together = 1 if n < 6 else 3
        if n % together == 0:
            several = sum(4 * COUNT[s] for s, _ in CHUNKS[n : n + together])
            with jax.named_scope(f"core_wait#n={n}"):
                wait_bytes(got_d, several * 5 // 2, core_recv.at[slot_of(n)])
        for m in range(len(PARTS)):
            if PARTS[m][0] == n:
                meet_part(m, start)

    def closer(depth, color, best, kept):
        tag, old = color[3].astype(jnp.float32), kept[3].astype(jnp.float32)
        nearer = (depth < best) | ((depth == best) & (tag < old))
        return jnp.where(nearer, depth, best), pick(nearer, color, kept)

    def first_join(n):
        stream, off, _, count = piece(n)
        first, second, third = ORDER[stream]
        places = others(first)
        near, away = (1, 3) if off in PLAIN else (3, 1)
        mine, theirs = places[0], places[near]
        rest = at[second] * STRIDE[second] + at[third] * STRIDE[third]
        lower = jnp.where(theirs < mine, 1, 0)
        if opens(n):
            with jax.named_scope(f"wait1#n={n}"):
                wait_bytes(one_d, 5 * opens(n), recv1.at[ROUND[n]])
        for part, rel in enumerate((0, 3) if off in PLAIN else (1, 0)):
            to_d, to_c = (pass_d, pass_c) if rel else (mid_d, mid_c)
            base = STARTS[n] // 4

            def join(t, carry):
                p, q = STARTS[n] + rel * count + t, STARTS[n] // 2 + part * count + t
                k, other = own_d[p], one_d[q]
                depth, far_depth = lax.shift_right_arithmetic(k, 1), lax.shift_right_arithmetic(other, 1)
                nearer = far_depth < depth + lower if first == 0 else other < k + lower
                own_rank = rest + mine * STRIDE[first] + (k & 1) * 16
                other_rank = rest + theirs * STRIDE[first] + (other & 1) * 16
                to_d[base + t] = jnp.where(nearer, far_depth, depth)
                to_c[base + t, 0:3] = pick(nearer, one_c[q], own_c[p])
                to_c[base + t, 3] = jnp.where(nearer, other_rank, own_rank).astype(jnp.float32).astype(jnp.bfloat16)
                return carry

            lax.fori_loop(0, count, join, 0)
        part = pl.ds(STARTS[n] // 4, count)
        remote(
            (pass_d.at[part], met_d.at[part]), (pass_c.at[part], met_c.at[part]),
            send1b, recv1b.at[ROUND[n]], seat(first, places[away]),
        )

    def second_join(n):
        stream, off, skip, count = piece(n)
        second = ORDER[stream][1]
        base, into = STARTS[n] // 4, BASE[stream] // 4 + (off - 1) * COUNT[stream] + skip
        if opens(n):
            with jax.named_scope(f"wait1b#n={n}"):
                wait_bytes(one_d, 3 * opens(n), recv1b.at[ROUND[n]])

        def join(t, carry):
            q = base + t
            out1_d[into + t], out1_c[into + t] = closer(met_d[q], met_c[q], mid_d[q], mid_c[q])
            return carry

        lax.fori_loop(0, count, join, 0)
        src = pl.ds(into, count)
        dst = pl.ds(BASE[stream] // 4 + at[second] * COUNT[stream] + skip, count)
        remote((out1_d.at[src], two_d.at[dst]), (out1_c.at[src], two_c.at[dst]), send2, recv2.at[stream], peer(second, off))

    def keep_join(n):
        stream, off, _, count = piece(n)
        first, second, third = ORDER[stream]
        base = (STARTS[n] - STARTS[KEPT]) // 4 * 3
        into = BASE[stream] // 4 + at[second] * count
        places = others(first)
        rest = at[second] * STRIDE[second] + at[third] * STRIDE[third]
        if opens(n):
            with jax.named_scope(f"keep_wait#n={n}"):
                wait_bytes(own_c, 5 * opens(n), recv1.at[ROUND[n]])

        def join(t, carry):
            best = tag = color = None
            for rel in range(4):
                q = base + (rel - 1) * count + t
                k, new = (keep_d[q], keep_c[q]) if rel else (own_d[STARTS[n] + t], own_c[STARTS[n] + t])
                depth = lax.shift_right_arithmetic(k, 1)
                rank = rest + places[rel] * STRIDE[first] + (k & 1) * 16
                if rel == 0:
                    best, tag, color = depth, rank, new
                else:
                    nearer = (depth < best) | ((depth == best) & (rank < tag))
                    best, tag = jnp.where(nearer, depth, best), jnp.where(nearer, rank, tag)
                    color = pick(nearer, new, color)
            two_d[into + t] = best
            two_c[into + t, 0:3] = color
            two_c[into + t, 3] = tag.astype(jnp.float32).astype(jnp.bfloat16)
            return carry

        lax.fori_loop(0, count, join, 0)

    last_of = {PARTS[m][0]: m for m in range(KEPT)}
    for m in range(KEPT):
        first_join(m)
        for n in range(6):
            if last_of[n] == m:
                keep_send(KEPT + n % 3, 2 - n // 3)
    for m in range(KEPT):
        second_join(m)
    for m in range(KEPT, len(PARTS)):
        keep_join(m)

    mine = lax.rem(at[0] + at[1] + at[2], 4)
    for stream in (2, 1, 0):
        count, base = COUNT[stream], BASE[stream] // 4
        with jax.named_scope(f"wait2#s={stream}"):
            wait_bytes(two_d, 9 * count, recv2.at[stream])
        for t in range(count):
            best, kept = two_d[base + t], two_c[base + t]
            for src in (1, 2, 3):
                q = base + src * count + t
                best, kept = closer(two_d[q], two_c[q], best, kept)
            group, half = CLASS[stream][t], HALF[stream][t]
            k = 2 * group + half
            out2_d[k] = best
            out2_c[k] = kept
            off = lax.rem(group - mine + 4, 4)

            @pl.when(off != 0)
            def send():
                slot = 3 * half + off - 1
                remote(
                    (out2_d.at[k], last_d.at[slot]), (out2_c.at[k], last_c.at[slot]),
                    send3, recv3, peer(ORDER[stream][2], off),
                )

    with jax.named_scope("wait3"):
        wait_bytes(one_d, 18, recv3)
    sums = []
    for half in range(2):
        best, kept = out2_d[2 * mine + half], out2_c[2 * mine + half]
        for off in (1, 2, 3):
            slot = 3 * half + off - 1
            best, kept = closer(last_d[slot], last_c[slot], best, kept)
        depth_out[half] = best + FAR
        color_out[half] = kept[0:3]
        sums.append(jnp.sum(kept[0:3].astype(jnp.float32).reshape(3, 2, 8, 128), axis=2))
    rows = jnp.concatenate(
        [s for c in range(3) for s in (sums[0][c], sums[1][c])] + [jnp.zeros((4, 128), jnp.float32)], axis=0
    )
    lane_down = lax.broadcasted_iota(jnp.int32, (128, 128), 0)
    lane = lax.broadcasted_iota(jnp.int32, (128, 128), 1)
    spread = jnp.where(lax.shift_right_logical(lane_down, 3) == (lane & 15), 1.0 / 64, 0.0)
    means = jnp.dot(rows, spread, precision=lax.Precision.HIGHEST, preferred_element_type=jnp.float32)
    line = lax.broadcasted_iota(jnp.int32, (16, 128), 0) & 7
    group = lax.shift_right_logical(lax.broadcasted_iota(jnp.int32, (16, 128), 1), 4)
    thumbs[me] = jnp.sum(jnp.where(line == group, means, 0.0).reshape(2, 8, 128), axis=1)

    around = [[lax.rem(a + off, 4) for off in range(4)] for a in at]
    across = [[2 * a + c for a in around[0]] for c in (core, 1 - core)]
    along = [[4 * b + c for c in around[2]] for b in around[1]]
    for dx, dy, dz in FAR_FIRST:
        for other in range(2):
            if dx or dy or dz or other:
                pltpu.make_async_remote_copy(
                    src_ref=thumbs.at[me], dst_ref=thumbs.at[me], send_sem=thumb_send, recv_sem=thumb_recv,
                    device_id=(across[other][dx], along[dy][dz]), device_id_type=MESH,
                ).start()
    for sends, depth_ref, color_ref, count in (
        (core_send, send_d, send_c, 128), (send1, own_d, own_c, 72), (send1b, met_d, met_c, 24),
        (send2, two_d, two_c, 24), (send3, last_d, last_c, 6),
    ):
        wait_bytes(depth_ref, count, sends.at[0])
        wait_bytes(color_ref, count, sends.at[1])
    with jax.named_scope("thumb_wait"):
        wait_bytes(thumbs, 127, thumb_recv)
    wait_bytes(thumbs, 127, thumb_send)
    thumbs_out[...] = thumbs[...]


def settle(owner_ref, depth_ref, color_ref, thumbs_ref, depth_out, color_out, thumbs_out):
    depth_out[...] = depth_ref[...]
    color_out[...] = color_ref[...]
    held = lax.broadcasted_iota(jnp.int32, (128, 128), 0) == owner_ref[...]
    chosen = jnp.where(held, 1.0, 0.0)
    for row, size in ((0, 128), (1, 64)):
        thumbs_out[128 * row : 128 * row + size] = lax.dot_general(
            thumbs_ref[:, row, 0:size], chosen, (((0,), (0,)), ((), ())),
            precision=lax.Precision.HIGHEST, preferred_element_type=jnp.float32,
        )


def shards(slot_tiles, owner_map, slot_depth, slot_color):
    i32, bf16 = jnp.int32, jnp.bfloat16
    vmem = pl.BlockSpec(memory_space=pltpu.VMEM)
    anywhere = pl.BlockSpec(memory_space=pl.ANY)
    dma = pltpu.SemaphoreType.DMA
    scratch = [
        pltpu.VMEM((129, 16, 128), i32), pltpu.VMEM((129, 3, 16, 128), bf16),
        pltpu.VMEM((2, 128), i32), pltpu.SMEM((2, 128), i32),
    ]
    for tiles, channels in ((128, 3), (128, 3), (128, 3), (48, 3), (24, 4), (24, 4), (24, 4), (24, 3), (32, 4), (32, 4), (8, 4), (6, 4)):
        scratch += [pltpu.VMEM((tiles, 16, 128), i32), pltpu.VMEM((tiles, channels, 16, 128), bf16)]
    scratch += [pltpu.VMEM((128, 2, 128), jnp.float32), dma((2,)), dma]
    scratch += [dma((2,)), dma((8,)), dma((2,)), dma((len(ROUNDS),)), dma((2,)), dma((len(ROUNDS) - 1,)), dma((2,)), dma((3,)), dma((2,)), dma]
    scratch += [dma, dma]
    depth, color, thumbs = pl.pallas_call(
        kernel,
        out_shape=(
            pltpu.VMEM((2, 16, 128), i32),
            pltpu.VMEM((2, 3, 16, 128), bf16),
            pltpu.VMEM((128, 2, 128), jnp.float32),
        ),
        in_specs=[vmem, vmem, vmem, anywhere, anywhere],
        out_specs=(vmem, vmem, vmem),
        scratch_shapes=scratch,
        compiler_params=pltpu.CompilerParams(collective_id=0, has_side_effects=True),
        name="composite",
    )(
        slot_tiles,
        owner_map[None],
        jnp.asarray(tile_places()),
        slot_depth[0],
        jnp.swapaxes(slot_color[0], 1, 2),
    )
    depth, color, thumbs = pl.pallas_call(
        settle,
        out_shape=(
            jax.ShapeDtypeStruct((2, 16, 128), i32),
            jax.ShapeDtypeStruct((2, 3, 16, 128), bf16),
            jax.ShapeDtypeStruct((192, 128), jnp.float32),
        ),
        in_specs=[vmem] * 4,
        out_specs=(vmem, vmem, vmem),
        compiler_params=pltpu.CompilerParams(vmem_limit_bytes=8 << 20),
        name="settle",
    )(owner_map[None], depth, color, thumbs)
    thumbnail = jnp.transpose(thumbs.reshape(3, 64, 128), (2, 0, 1))
    return depth[None], jnp.swapaxes(color, 1, 2)[None], thumbnail


def solution(mesh):
    ranks = ("gx", "gy")
    return jax.shard_map(
        shards,
        mesh=mesh,
        in_specs=(P(ranks, None), P(), P(ranks, None, None, None), P(ranks, None, None, None, None)),
        out_specs=(P(ranks, None, None, None), P(ranks, None, None, None, None), P()),
        check_vma=False,
    )
```

```python
import jax
import jax.numpy as jnp
import numpy as np
from jax import lax
from jax.experimental import pallas as pl
from jax.experimental.pallas import tpu as pltpu
from jax.sharding import PartitionSpec as P

MESH = pl.DeviceIdType.MESH
FAR = 1073741824
ORDER = ((0, 1, 2), (1, 2, 0), (2, 0, 1))
STRIDE = (32, 4, 1)
COUNT = (3, 3, 2)
BASE = (0, 48, 96)
CLASS = ((0, 2, 3), (0, 1, 3), (1, 2))
HALF = ((0, 1, 0), (1, 0, 1), (1, 0))
CHUNKS = tuple((stream, off) for off in (2, 1, 3, 0) for stream in range(3))
PLAIN = (2, 3)
SINGLE = (2, 1, 3)


def parts():
    out = []
    for first in range(0, 12, 3):
        chunks = range(first, first + 3)
        if CHUNKS[first][1] in SINGLE:
            out += [(n, t, 1) for t in range(3) for n in chunks if t < COUNT[CHUNKS[n][0]]]
        else:
            out += [(n, 0, COUNT[CHUNKS[n][0]]) for n in chunks]
    return tuple(out)


PARTS = parts()
STARTS = tuple(sum(4 * count for _, _, count in PARTS[:m]) for m in range(len(PARTS)))
KEPT = len(PARTS) - 3
ROUNDS = sorted({(n // 3, t if n < 9 else 0) for n, t, _ in PARTS})
ROUND = tuple(ROUNDS.index((n // 3, t)) for n, t, _ in PARTS)
TURNS = tuple((n, turn) for turn in range(2) for n in range(12))
FAR_FIRST = sorted(np.ndindex(4, 4, 4), key=lambda d: -sum(min(a, 4 - a) for a in d))


def tile_places():
    places = np.zeros((1, 128), np.int32)
    for stream in range(3):
        first, second, third = ORDER[stream]
        count = COUNT[stream]
        for i in range(4):
            for j in range(4):
                for t in range(count):
                    at = [0, 0, 0]
                    at[first], at[second] = i, j
                    at[third] = (CLASS[stream][t] - i - j) % 4
                    owner = sum(a * s for a, s in zip(at, STRIDE))
                    places[0, BASE[stream] + (j * 4 + i) * count + t] = 2 * owner + HALF[stream][t]
    return places


def pick(mask, new, old):
    return jnp.where(mask[None], new, old)


def kernel(
    tiles_ref, owner_ref, place_ref, depth_hbm, color_hbm,
    depth_out, color_out, thumbs_out,
    in_d, in_c, table_v, table, send_d, send_c, got_d, got_c,
    own_d, own_c, one_d, one_c, mid_d, mid_c, pass_d, pass_c, met_d, met_c, keep_d, keep_c, out1_d, out1_c, two_d, two_c, out2_d, out2_c,
    last_d, last_c, thumbs,
    load_sem, table_sem, core_send, core_recv, send1, recv1, send1b, recv1b, send2, recv2, send3, recv3,
    thumb_send, thumb_recv,
):
    gx, gy = lax.axis_index("gx"), lax.axis_index("gy")
    core = lax.rem(gx, 2)
    at = (lax.div(gx, 2), lax.div(gy, 4), lax.rem(gy, 4))
    me = gx * 16 + gy

    def device(x, y, z, c=core):
        return (2 * x + c, 4 * y + z)

    def peer(axis, off):
        moved = [lax.rem(a + off, 4) if k == axis else a for k, a in enumerate(at)]
        return device(*moved)

    partner = device(*at, c=1 - core)

    loads = [
        pltpu.make_async_copy(depth_hbm, in_d.at[pl.ds(0, 128)], load_sem.at[0]),
        pltpu.make_async_copy(color_hbm, in_c.at[pl.ds(0, 128)], load_sem.at[1]),
    ]
    for load in loads:
        load.start()
    barrier = pltpu.get_barrier_semaphore()
    pl.semaphore_signal(barrier, inc=1, device_id=partner, device_id_type=MESH)
    for axis in range(3):
        for off in (1, 2, 3):
            pl.semaphore_signal(barrier, inc=1, device_id=peer(axis, off), device_id_type=MESH)

    in_d[128] = jnp.full((16, 128), FAR, jnp.int32)
    in_c[128] = jnp.zeros((3, 16, 128), jnp.bfloat16)
    tiles = tiles_ref[...]
    live = tiles >= 0
    row = lax.shift_right_arithmetic(tiles, 4)
    region = lax.shift_right_arithmetic(row, 1) * 16 + (tiles & 15)
    down = lax.broadcasted_iota(jnp.int32, (128, 128), 0)
    owner_down = jnp.transpose(jnp.broadcast_to(owner_ref[...], (128, 128)))
    owner = jnp.sum(jnp.where(down == region, owner_down, 0), axis=0, keepdims=True)
    place = jnp.where(live, 2 * owner + (row & 1), -1)
    place_down = jnp.transpose(jnp.broadcast_to(place, (128, 128)))
    for c in range(2):
        hit = place_down == place_ref[...] + 32 * c
        table_v[c : c + 1, :] = jnp.min(jnp.where(hit, down, 128), axis=0, keepdims=True)
    to_table = pltpu.make_async_copy(table_v, table, table_sem)
    to_table.start()
    with jax.named_scope("load"):
        to_table.wait()
        for load in loads:
            load.wait()
    with jax.named_scope("greet"):
        pl.semaphore_wait(barrier, 10)

    def remote(depth, color, sends, recv, target):
        for part, (src, dst) in enumerate((depth, color)):
            pltpu.make_async_remote_copy(
                src_ref=src, dst_ref=dst, send_sem=sends.at[part], recv_sem=recv,
                device_id=target, device_id_type=MESH,
            ).start()

    def wait_bytes(ref, count, sem):
        some = ref.at[pl.ds(0, count)]
        pltpu.make_async_copy(some, some, sem).wait()

    def chunk(stream, off):
        size = 4 * COUNT[stream]
        return BASE[stream] + lax.rem(at[ORDER[stream][1]] + off, 4) * size, size

    def others(axis):
        c = at[axis]
        return c, c + 1 - 2 * lax.rem(c, 2), lax.rem(c + 2, 4), 3 - c

    def legs(n, turn):
        off = CHUNKS[n][1]
        early = (1, 2) if off in PLAIN else (2, 3) if off else (3,)
        return early if turn == 0 else tuple(r for r in range(4) if r not in early)

    def slot_of(n, turn):
        return 8 + n // 3 if turn else n if n < 6 else 4 + n // 3

    def tiles_at(n, rel):
        stream, off = CHUNKS[n]
        return chunk(stream, off)[0] + others(ORDER[stream][0])[rel] * COUNT[stream]

    def give(n, turn):
        for rel in legs(n, turn):
            start, count = tiles_at(n, rel), COUNT[CHUNKS[n][0]]

            def pack(t, carry):
                slot = table[1 - core, start + t]
                send_d[start + t] = in_d[slot]
                send_c[start + t] = in_c[slot]
                return carry

            lax.fori_loop(0, count, pack, 0, unroll=True)
            part = pl.ds(start, count)
            remote(
                (send_d.at[part], got_d.at[part]), (send_c.at[part], got_c.at[part]),
                core_send, core_recv.at[slot_of(n, turn)], partner,
            )

    for n in range(12):
        give(n, 0)

    def seat(axis, place):
        return device(*(place if k == axis else a for k, a in enumerate(at)))

    def opens(m):
        if m and ROUND[m] == ROUND[m - 1]:
            return 0
        return sum(count for (_, _, count), r in zip(PARTS, ROUND) if r == ROUND[m])

    def piece(m):
        n, skip, count = PARTS[m]
        return *CHUNKS[n], skip, count

    def first_send(n):
        stream, off, _, count = piece(n)
        axis = ORDER[stream][0]
        near, skip = (1, 1) if off in PLAIN else (3, 2)
        src = pl.ds(STARTS[n] + skip * count, 2 * count)
        dst = pl.ds(STARTS[n] // 2, 2 * count)
        remote(
            (own_d.at[src], one_d.at[dst]), (own_c.at[src], one_c.at[dst]),
            send1, recv1.at[ROUND[n]], seat(axis, others(axis)[near]),
        )

    def keep_send(n, rel):
        stream, off, _, count = piece(n)
        axis = ORDER[stream][0]
        src = pl.ds(STARTS[n] + rel * count, count)
        dst = pl.ds((STARTS[n] - STARTS[KEPT]) // 4 * 3 + (rel - 1) * count, count)
        remote(
            (own_d.at[src], keep_d.at[dst]), (own_c.at[src], keep_c.at[dst]),
            send1, recv1.at[ROUND[n]], seat(axis, others(axis)[rel]),
        )

    def meet_part(m, rel):
        n, skip, count = PARTS[m]
        first, into = tiles_at(n, rel) + skip, STARTS[m] + rel * count

        def meet(t, carry):
            slot = table[core, first + t]
            mine = (in_d[slot] - FAR) * 2 + core
            other = (got_d[first + t] - FAR) * 2 + (1 - core)
            nearer = other < mine
            own_d[into + t] = jnp.where(nearer, other, mine)
            own_c[into + t] = pick(nearer, got_c[first + t], in_c[slot])
            return carry

        lax.fori_loop(0, count, meet, 0, unroll=True)

    for n, turn in TURNS:
        if turn == 0 and n in (3, 6, 7, 8):
            for k in {3: range(3), 6: range(3, 6), 7: range(6, 9), 8: range(9, 12)}[n]:
                give(k, 1)
        together = 1 if n < 6 and turn == 0 else 3
        if n % together == 0:
            several = sum(COUNT[CHUNKS[k][0]] * len(legs(k, turn)) for k in range(n, n + together))
            with jax.named_scope(f"core_wait#n={n}#t={turn}"):
                wait_bytes(got_d, several * 5 // 2, core_recv.at[slot_of(n, turn)])
        for m in range(len(PARTS)):
            if PARTS[m][0] == n:
                for rel in legs(n, turn):
                    meet_part(m, rel)
                if turn == 0 and m < KEPT:
                    first_send(m)
                elif turn == 0:
                    keep_send(m, 3)

    def closer(depth, color, best, kept):
        tag, old = color[3].astype(jnp.float32), kept[3].astype(jnp.float32)
        nearer = (depth < best) | ((depth == best) & (tag < old))
        return jnp.where(nearer, depth, best), pick(nearer, color, kept)

    def first_join(n):
        stream, off, _, count = piece(n)
        first, second, third = ORDER[stream]
        places = others(first)
        near, away = (1, 3) if off in PLAIN else (3, 1)
        mine, theirs = places[0], places[near]
        rest = at[second] * STRIDE[second] + at[third] * STRIDE[third]
        lower = jnp.where(theirs < mine, 1, 0)
        if opens(n):
            with jax.named_scope(f"wait1#n={n}"):
                wait_bytes(one_d, 5 * opens(n), recv1.at[ROUND[n]])
        for part, rel in enumerate((0, 3) if off in PLAIN else (1, 0)):
            to_d, to_c = (pass_d, pass_c) if rel else (mid_d, mid_c)
            base = STARTS[n] // 4

            def join(t, carry):
                p, q = STARTS[n] + rel * count + t, STARTS[n] // 2 + part * count + t
                k, other = own_d[p], one_d[q]
                depth, far_depth = lax.shift_right_arithmetic(k, 1), lax.shift_right_arithmetic(other, 1)
                nearer = far_depth < depth + lower if first == 0 else other < k + lower
                own_rank = rest + mine * STRIDE[first] + (k & 1) * 16
                other_rank = rest + theirs * STRIDE[first] + (other & 1) * 16
                to_d[base + t] = jnp.where(nearer, far_depth, depth)
                to_c[base + t, 0:3] = pick(nearer, one_c[q], own_c[p])
                to_c[base + t, 3] = jnp.where(nearer, other_rank, own_rank).astype(jnp.float32).astype(jnp.bfloat16)
                return carry

            lax.fori_loop(0, count, join, 0)
        part = pl.ds(STARTS[n] // 4, count)
        remote(
            (pass_d.at[part], met_d.at[part]), (pass_c.at[part], met_c.at[part]),
            send1b, recv1b.at[ROUND[n]], seat(first, places[away]),
        )

    def second_join(n):
        stream, off, skip, count = piece(n)
        second = ORDER[stream][1]
        base, into = STARTS[n] // 4, BASE[stream] // 4 + (off - 1) * COUNT[stream] + skip
        if opens(n):
            with jax.named_scope(f"wait1b#n={n}"):
                wait_bytes(one_d, 3 * opens(n), recv1b.at[ROUND[n]])

        def join(t, carry):
            q = base + t
            out1_d[into + t], out1_c[into + t] = closer(met_d[q], met_c[q], mid_d[q], mid_c[q])
            return carry

        lax.fori_loop(0, count, join, 0)
        src = pl.ds(into, count)
        dst = pl.ds(BASE[stream] // 4 + at[second] * COUNT[stream] + skip, count)
        remote((out1_d.at[src], two_d.at[dst]), (out1_c.at[src], two_c.at[dst]), send2, recv2.at[stream], peer(second, off))

    def keep_join(n):
        stream, off, _, count = piece(n)
        first, second, third = ORDER[stream]
        base = (STARTS[n] - STARTS[KEPT]) // 4 * 3
        into = BASE[stream] // 4 + at[second] * count
        places = others(first)
        rest = at[second] * STRIDE[second] + at[third] * STRIDE[third]
        if opens(n):
            with jax.named_scope(f"keep_wait#n={n}"):
                wait_bytes(own_c, 5 * opens(n), recv1.at[ROUND[n]])

        def join(t, carry):
            best = tag = color = None
            for rel in range(4):
                q = base + (rel - 1) * count + t
                k, new = (keep_d[q], keep_c[q]) if rel else (own_d[STARTS[n] + t], own_c[STARTS[n] + t])
                depth = lax.shift_right_arithmetic(k, 1)
                rank = rest + places[rel] * STRIDE[first] + (k & 1) * 16
                if rel == 0:
                    best, tag, color = depth, rank, new
                else:
                    nearer = (depth < best) | ((depth == best) & (rank < tag))
                    best, tag = jnp.where(nearer, depth, best), jnp.where(nearer, rank, tag)
                    color = pick(nearer, new, color)
            two_d[into + t] = best
            two_c[into + t, 0:3] = color
            two_c[into + t, 3] = tag.astype(jnp.float32).astype(jnp.bfloat16)
            return carry

        lax.fori_loop(0, count, join, 0)

    last_of = {PARTS[m][0]: m for m in range(KEPT)}
    for m in range(KEPT):
        first_join(m)
        for n in range(6):
            if last_of[n] == m:
                keep_send(KEPT + n % 3, 2 - n // 3)
    for m in range(KEPT):
        second_join(m)
    for m in range(KEPT, len(PARTS)):
        keep_join(m)

    mine = lax.rem(at[0] + at[1] + at[2], 4)
    for stream in (2, 1, 0):
        count, base = COUNT[stream], BASE[stream] // 4
        with jax.named_scope(f"wait2#s={stream}"):
            wait_bytes(two_d, 9 * count, recv2.at[stream])
        for t in range(count):
            best, kept = two_d[base + t], two_c[base + t]
            for src in (1, 2, 3):
                q = base + src * count + t
                best, kept = closer(two_d[q], two_c[q], best, kept)
            group, half = CLASS[stream][t], HALF[stream][t]
            k = 2 * group + half
            out2_d[k] = best
            out2_c[k] = kept
            off = lax.rem(group - mine + 4, 4)

            @pl.when(off != 0)
            def send():
                slot = 3 * half + off - 1
                remote(
                    (out2_d.at[k], last_d.at[slot]), (out2_c.at[k], last_c.at[slot]),
                    send3, recv3, peer(ORDER[stream][2], off),
                )

    with jax.named_scope("wait3"):
        wait_bytes(one_d, 18, recv3)
    sums = []
    for half in range(2):
        best, kept = out2_d[2 * mine + half], out2_c[2 * mine + half]
        for off in (1, 2, 3):
            slot = 3 * half + off - 1
            best, kept = closer(last_d[slot], last_c[slot], best, kept)
        depth_out[half] = best + FAR
        color_out[half] = kept[0:3]
        sums.append(jnp.sum(kept[0:3].astype(jnp.float32).reshape(3, 2, 8, 128), axis=2))
    rows = jnp.concatenate(
        [s for c in range(3) for s in (sums[0][c], sums[1][c])] + [jnp.zeros((4, 128), jnp.float32)], axis=0
    )
    lane_down = lax.broadcasted_iota(jnp.int32, (128, 128), 0)
    lane = lax.broadcasted_iota(jnp.int32, (128, 128), 1)
    spread = jnp.where(lax.shift_right_logical(lane_down, 3) == (lane & 15), 1.0 / 64, 0.0)
    means = jnp.dot(rows, spread, precision=lax.Precision.HIGHEST, preferred_element_type=jnp.float32)
    line = lax.broadcasted_iota(jnp.int32, (16, 128), 0) & 7
    group = lax.shift_right_logical(lax.broadcasted_iota(jnp.int32, (16, 128), 1), 4)
    thumbs[me] = jnp.sum(jnp.where(line == group, means, 0.0).reshape(2, 8, 128), axis=1)

    around = [[lax.rem(a + off, 4) for off in range(4)] for a in at]
    across = [[2 * a + c for a in around[0]] for c in (core, 1 - core)]
    along = [[4 * b + c for c in around[2]] for b in around[1]]
    for dx, dy, dz in FAR_FIRST:
        for other in range(2):
            if dx or dy or dz or other:
                pltpu.make_async_remote_copy(
                    src_ref=thumbs.at[me], dst_ref=thumbs.at[me], send_sem=thumb_send, recv_sem=thumb_recv,
                    device_id=(across[other][dx], along[dy][dz]), device_id_type=MESH,
                ).start()
    for sends, depth_ref, color_ref, count in (
        (core_send, send_d, send_c, 128), (send1, own_d, own_c, 72), (send1b, met_d, met_c, 24),
        (send2, two_d, two_c, 24), (send3, last_d, last_c, 6),
    ):
        wait_bytes(depth_ref, count, sends.at[0])
        wait_bytes(color_ref, count, sends.at[1])
    with jax.named_scope("thumb_wait"):
        wait_bytes(thumbs, 127, thumb_recv)
    wait_bytes(thumbs, 127, thumb_send)
    thumbs_out[...] = thumbs[...]


def settle(owner_ref, depth_ref, color_ref, thumbs_ref, depth_out, color_out, thumbs_out):
    depth_out[...] = depth_ref[...]
    color_out[...] = color_ref[...]
    held = lax.broadcasted_iota(jnp.int32, (128, 128), 0) == owner_ref[...]
    chosen = jnp.where(held, 1.0, 0.0)
    for row, size in ((0, 128), (1, 64)):
        thumbs_out[128 * row : 128 * row + size] = lax.dot_general(
            thumbs_ref[:, row, 0:size], chosen, (((0,), (0,)), ((), ())),
            precision=lax.Precision.HIGHEST, preferred_element_type=jnp.float32,
        )


def shards(slot_tiles, owner_map, slot_depth, slot_color):
    i32, bf16 = jnp.int32, jnp.bfloat16
    vmem = pl.BlockSpec(memory_space=pltpu.VMEM)
    anywhere = pl.BlockSpec(memory_space=pl.ANY)
    dma = pltpu.SemaphoreType.DMA
    scratch = [
        pltpu.VMEM((129, 16, 128), i32), pltpu.VMEM((129, 3, 16, 128), bf16),
        pltpu.VMEM((2, 128), i32), pltpu.SMEM((2, 128), i32),
    ]
    for tiles, channels in ((128, 3), (128, 3), (128, 3), (48, 3), (24, 4), (24, 4), (24, 4), (24, 3), (32, 4), (32, 4), (8, 4), (6, 4)):
        scratch += [pltpu.VMEM((tiles, 16, 128), i32), pltpu.VMEM((tiles, channels, 16, 128), bf16)]
    scratch += [pltpu.VMEM((128, 2, 128), jnp.float32), dma((2,)), dma]
    scratch += [dma((2,)), dma((12,)), dma((2,)), dma((len(ROUNDS),)), dma((2,)), dma((len(ROUNDS) - 1,)), dma((2,)), dma((3,)), dma((2,)), dma]
    scratch += [dma, dma]
    depth, color, thumbs = pl.pallas_call(
        kernel,
        out_shape=(
            pltpu.VMEM((2, 16, 128), i32),
            pltpu.VMEM((2, 3, 16, 128), bf16),
            pltpu.VMEM((128, 2, 128), jnp.float32),
        ),
        in_specs=[vmem, vmem, vmem, anywhere, anywhere],
        out_specs=(vmem, vmem, vmem),
        scratch_shapes=scratch,
        compiler_params=pltpu.CompilerParams(collective_id=0, has_side_effects=True),
        name="composite",
    )(
        slot_tiles,
        owner_map[None],
        jnp.asarray(tile_places()),
        slot_depth[0],
        jnp.swapaxes(slot_color[0], 1, 2),
    )
    depth, color, thumbs = pl.pallas_call(
        settle,
        out_shape=(
            jax.ShapeDtypeStruct((2, 16, 128), i32),
            jax.ShapeDtypeStruct((2, 3, 16, 128), bf16),
            jax.ShapeDtypeStruct((192, 128), jnp.float32),
        ),
        in_specs=[vmem] * 4,
        out_specs=(vmem, vmem, vmem),
        compiler_params=pltpu.CompilerParams(vmem_limit_bytes=8 << 20),
        name="settle",
    )(owner_map[None], depth, color, thumbs)
    thumbnail = jnp.transpose(thumbs.reshape(3, 64, 128), (2, 0, 1))
    return depth[None], jnp.swapaxes(color, 1, 2)[None], thumbnail


def solution(mesh):
    ranks = ("gx", "gy")
    return jax.shard_map(
        shards,
        mesh=mesh,
        in_specs=(P(ranks, None), P(), P(ranks, None, None, None), P(ranks, None, None, None, None)),
        out_specs=(P(ranks, None, None, None), P(ranks, None, None, None, None), P()),
        check_vma=False,
    )
```

```python
import jax
import jax.numpy as jnp
import numpy as np
from jax import lax
from jax.experimental import pallas as pl
from jax.experimental.pallas import tpu as pltpu
from jax.sharding import PartitionSpec as P

MESH = pl.DeviceIdType.MESH
FAR = 1073741824
ORDER = ((0, 1, 2), (1, 2, 0), (2, 0, 1))
STRIDE = (32, 4, 1)
COUNT = (3, 3, 2)
BASE = (0, 48, 96)
CLASS = ((0, 2, 3), (0, 1, 3), (1, 2))
HALF = ((0, 1, 0), (1, 0, 1), (1, 0))
CHUNKS = tuple((stream, off) for off in (2, 1, 3, 0) for stream in range(3))
PLAIN = (2, 3)
SINGLE = (2, 1, 3)


def parts():
    out = []
    for first in range(0, 12, 3):
        chunks = range(first, first + 3)
        if CHUNKS[first][1] in SINGLE:
            out += [(n, t, 1) for t in range(3) for n in chunks if t < COUNT[CHUNKS[n][0]]]
        else:
            out += [(n, 0, COUNT[CHUNKS[n][0]]) for n in chunks]
    return tuple(out)


PARTS = parts()
STARTS = tuple(sum(4 * count for _, _, count in PARTS[:m]) for m in range(len(PARTS)))
KEPT = len(PARTS) - 3
ROUNDS = sorted({(n // 3, t if n < 9 else 0) for n, t, _ in PARTS})
ROUND = tuple(ROUNDS.index((n // 3, t)) for n, t, _ in PARTS)
TURNS = tuple((n, turn) for turn in range(2) for n in range(12))
FAR_FIRST = sorted(np.ndindex(4, 4, 4), key=lambda d: -sum(min(a, 4 - a) for a in d))


def tile_places():
    places = np.zeros((1, 128), np.int32)
    for stream in range(3):
        first, second, third = ORDER[stream]
        count = COUNT[stream]
        for i in range(4):
            for j in range(4):
                for t in range(count):
                    at = [0, 0, 0]
                    at[first], at[second] = i, j
                    at[third] = (CLASS[stream][t] - i - j) % 4
                    owner = sum(a * s for a, s in zip(at, STRIDE))
                    places[0, BASE[stream] + (j * 4 + i) * count + t] = 2 * owner + HALF[stream][t]
    return places


def pick(mask, new, old):
    return jnp.where(mask[None], new, old)


def kernel(
    tiles_hbm, owner_hbm, place_hbm, depth_hbm, color_hbm,
    depth_out, color_out, thumbs_out,
    tiles_ref, owner_ref, place_ref, in_d, in_c, table_v, table, send_d, send_c, got_d, got_c,
    own_d, own_c, one_d, one_c, mid_d, mid_c, pass_d, pass_c, met_d, met_c, keep_d, keep_c, out1_d, out1_c, two_d, two_c, out2_d, out2_c,
    last_d, last_c, thumbs,
    load_sem, table_sem, core_send, core_recv, send1, recv1, send1b, recv1b, send2, recv2, send3, recv3,
    thumb_send, thumb_recv,
):
    gx, gy = lax.axis_index("gx"), lax.axis_index("gy")
    core = lax.rem(gx, 2)
    at = (lax.div(gx, 2), lax.div(gy, 4), lax.rem(gy, 4))
    me = gx * 16 + gy

    def device(x, y, z, c=core):
        return (2 * x + c, 4 * y + z)

    def peer(axis, off):
        moved = [lax.rem(a + off, 4) if k == axis else a for k, a in enumerate(at)]
        return device(*moved)

    partner = device(*at, c=1 - core)

    smalls = [
        pltpu.make_async_copy(src, dst, load_sem.at[2 + n])
        for n, (src, dst) in enumerate(((tiles_hbm, tiles_ref), (owner_hbm, owner_ref), (place_hbm, place_ref)))
    ]
    loads = [
        pltpu.make_async_copy(depth_hbm, in_d.at[pl.ds(0, 128)], load_sem.at[0]),
        pltpu.make_async_copy(color_hbm, in_c.at[pl.ds(0, 128)], load_sem.at[1]),
    ]
    for load in smalls + loads:
        load.start()
    barrier = pltpu.get_barrier_semaphore()
    pl.semaphore_signal(barrier, inc=1, device_id=partner, device_id_type=MESH)
    for axis in range(3):
        for off in (1, 2, 3):
            pl.semaphore_signal(barrier, inc=1, device_id=peer(axis, off), device_id_type=MESH)

    in_d[128] = jnp.full((16, 128), FAR, jnp.int32)
    in_c[128] = jnp.zeros((3, 16, 128), jnp.bfloat16)
    with jax.named_scope("small_wait"):
        for load in smalls:
            load.wait()
    tiles = tiles_ref[...]
    live = tiles >= 0
    row = lax.shift_right_arithmetic(tiles, 4)
    region = lax.shift_right_arithmetic(row, 1) * 16 + (tiles & 15)
    down = lax.broadcasted_iota(jnp.int32, (128, 128), 0)
    owner_down = jnp.transpose(jnp.broadcast_to(owner_ref[...], (128, 128)))
    owner = jnp.sum(jnp.where(down == region, owner_down, 0), axis=0, keepdims=True)
    place = jnp.where(live, 2 * owner + (row & 1), -1)
    place_down = jnp.transpose(jnp.broadcast_to(place, (128, 128)))
    for c in range(2):
        hit = place_down == place_ref[...] + 32 * c
        table_v[c : c + 1, :] = jnp.min(jnp.where(hit, down, 128), axis=0, keepdims=True)
    to_table = pltpu.make_async_copy(table_v, table, table_sem)
    to_table.start()
    with jax.named_scope("load"):
        to_table.wait()
        for load in loads:
            load.wait()
    with jax.named_scope("greet"):
        pl.semaphore_wait(barrier, 10)

    def remote(depth, color, sends, recv, target):
        for part, (src, dst) in enumerate((depth, color)):
            pltpu.make_async_remote_copy(
                src_ref=src, dst_ref=dst, send_sem=sends.at[part], recv_sem=recv,
                device_id=target, device_id_type=MESH,
            ).start()

    def wait_bytes(ref, count, sem):
        some = ref.at[pl.ds(0, count)]
        pltpu.make_async_copy(some, some, sem).wait()

    def chunk(stream, off):
        size = 4 * COUNT[stream]
        return BASE[stream] + lax.rem(at[ORDER[stream][1]] + off, 4) * size, size

    def others(axis):
        c = at[axis]
        return c, c + 1 - 2 * lax.rem(c, 2), lax.rem(c + 2, 4), 3 - c

    def legs(n, turn):
        off = CHUNKS[n][1]
        early = (1, 2) if off in PLAIN else (2, 3) if off else (3,)
        return early if turn == 0 else tuple(r for r in range(4) if r not in early)

    def slot_of(n, turn):
        return 8 + n // 3 if turn else n if n < 6 else 4 + n // 3

    def tiles_at(n, rel):
        stream, off = CHUNKS[n]
        return chunk(stream, off)[0] + others(ORDER[stream][0])[rel] * COUNT[stream]

    def give(n, turn):
        for rel in legs(n, turn):
            start, count = tiles_at(n, rel), COUNT[CHUNKS[n][0]]

            def pack(t, carry):
                slot = table[1 - core, start + t]
                send_d[start + t] = in_d[slot]
                send_c[start + t] = in_c[slot]
                return carry

            lax.fori_loop(0, count, pack, 0, unroll=True)
            part = pl.ds(start, count)
            remote(
                (send_d.at[part], got_d.at[part]), (send_c.at[part], got_c.at[part]),
                core_send, core_recv.at[slot_of(n, turn)], partner,
            )

    for n in range(12):
        give(n, 0)

    def seat(axis, place):
        return device(*(place if k == axis else a for k, a in enumerate(at)))

    def opens(m):
        if m and ROUND[m] == ROUND[m - 1]:
            return 0
        return sum(count for (_, _, count), r in zip(PARTS, ROUND) if r == ROUND[m])

    def piece(m):
        n, skip, count = PARTS[m]
        return *CHUNKS[n], skip, count

    def first_send(n):
        stream, off, _, count = piece(n)
        axis = ORDER[stream][0]
        near, skip = (1, 1) if off in PLAIN else (3, 2)
        src = pl.ds(STARTS[n] + skip * count, 2 * count)
        dst = pl.ds(STARTS[n] // 2, 2 * count)
        remote(
            (own_d.at[src], one_d.at[dst]), (own_c.at[src], one_c.at[dst]),
            send1, recv1.at[ROUND[n]], seat(axis, others(axis)[near]),
        )

    def keep_send(n, rel):
        stream, off, _, count = piece(n)
        axis = ORDER[stream][0]
        src = pl.ds(STARTS[n] + rel * count, count)
        dst = pl.ds((STARTS[n] - STARTS[KEPT]) // 4 * 3 + (rel - 1) * count, count)
        remote(
            (own_d.at[src], keep_d.at[dst]), (own_c.at[src], keep_c.at[dst]),
            send1, recv1.at[ROUND[n]], seat(axis, others(axis)[rel]),
        )

    def meet_part(m, rel):
        n, skip, count = PARTS[m]
        first, into = tiles_at(n, rel) + skip, STARTS[m] + rel * count

        def meet(t, carry):
            slot = table[core, first + t]
            mine = (in_d[slot] - FAR) * 2 + core
            other = (got_d[first + t] - FAR) * 2 + (1 - core)
            nearer = other < mine
            own_d[into + t] = jnp.where(nearer, other, mine)
            own_c[into + t] = pick(nearer, got_c[first + t], in_c[slot])
            return carry

        lax.fori_loop(0, count, meet, 0, unroll=True)

    for n, turn in TURNS:
        if turn == 0 and n in (3, 6, 7, 8):
            for k in {3: range(3), 6: range(3, 6), 7: range(6, 9), 8: range(9, 12)}[n]:
                give(k, 1)
        together = 1 if n < 6 and turn == 0 else 3
        if n % together == 0:
            several = sum(COUNT[CHUNKS[k][0]] * len(legs(k, turn)) for k in range(n, n + together))
            with jax.named_scope(f"core_wait#n={n}#t={turn}"):
                wait_bytes(got_d, several * 5 // 2, core_recv.at[slot_of(n, turn)])
        for m in range(len(PARTS)):
            if PARTS[m][0] == n:
                for rel in legs(n, turn):
                    meet_part(m, rel)
                if turn == 0 and m < KEPT:
                    first_send(m)
                elif turn == 0:
                    keep_send(m, 3)

    def closer(depth, color, best, kept):
        tag, old = color[3].astype(jnp.float32), kept[3].astype(jnp.float32)
        nearer = (depth < best) | ((depth == best) & (tag < old))
        return jnp.where(nearer, depth, best), pick(nearer, color, kept)

    def first_join(n):
        stream, off, _, count = piece(n)
        first, second, third = ORDER[stream]
        places = others(first)
        near, away = (1, 3) if off in PLAIN else (3, 1)
        mine, theirs = places[0], places[near]
        rest = at[second] * STRIDE[second] + at[third] * STRIDE[third]
        lower = jnp.where(theirs < mine, 1, 0)
        if opens(n):
            with jax.named_scope(f"wait1#n={n}"):
                wait_bytes(one_d, 5 * opens(n), recv1.at[ROUND[n]])
        for part, rel in enumerate((0, 3) if off in PLAIN else (1, 0)):
            to_d, to_c = (pass_d, pass_c) if rel else (mid_d, mid_c)
            base = STARTS[n] // 4

            def join(t, carry):
                p, q = STARTS[n] + rel * count + t, STARTS[n] // 2 + part * count + t
                k, other = own_d[p], one_d[q]
                depth, far_depth = lax.shift_right_arithmetic(k, 1), lax.shift_right_arithmetic(other, 1)
                nearer = far_depth < depth + lower if first == 0 else other < k + lower
                own_rank = rest + mine * STRIDE[first] + (k & 1) * 16
                other_rank = rest + theirs * STRIDE[first] + (other & 1) * 16
                to_d[base + t] = jnp.where(nearer, far_depth, depth)
                to_c[base + t, 0:3] = pick(nearer, one_c[q], own_c[p])
                to_c[base + t, 3] = jnp.where(nearer, other_rank, own_rank).astype(jnp.float32).astype(jnp.bfloat16)
                return carry

            lax.fori_loop(0, count, join, 0)
        part = pl.ds(STARTS[n] // 4, count)
        remote(
            (pass_d.at[part], met_d.at[part]), (pass_c.at[part], met_c.at[part]),
            send1b, recv1b.at[ROUND[n]], seat(first, places[away]),
        )

    def second_join(n):
        stream, off, skip, count = piece(n)
        second = ORDER[stream][1]
        base, into = STARTS[n] // 4, BASE[stream] // 4 + (off - 1) * COUNT[stream] + skip
        if opens(n):
            with jax.named_scope(f"wait1b#n={n}"):
                wait_bytes(one_d, 3 * opens(n), recv1b.at[ROUND[n]])

        def join(t, carry):
            q = base + t
            out1_d[into + t], out1_c[into + t] = closer(met_d[q], met_c[q], mid_d[q], mid_c[q])
            return carry

        lax.fori_loop(0, count, join, 0)
        src = pl.ds(into, count)
        dst = pl.ds(BASE[stream] // 4 + at[second] * COUNT[stream] + skip, count)
        remote((out1_d.at[src], two_d.at[dst]), (out1_c.at[src], two_c.at[dst]), send2, recv2.at[stream], peer(second, off))

    def keep_join(n):
        stream, off, _, count = piece(n)
        first, second, third = ORDER[stream]
        base = (STARTS[n] - STARTS[KEPT]) // 4 * 3
        into = BASE[stream] // 4 + at[second] * count
        places = others(first)
        rest = at[second] * STRIDE[second] + at[third] * STRIDE[third]
        if opens(n):
            with jax.named_scope(f"keep_wait#n={n}"):
                wait_bytes(own_c, 5 * opens(n), recv1.at[ROUND[n]])

        def join(t, carry):
            best = tag = color = None
            for rel in range(4):
                q = base + (rel - 1) * count + t
                k, new = (keep_d[q], keep_c[q]) if rel else (own_d[STARTS[n] + t], own_c[STARTS[n] + t])
                depth = lax.shift_right_arithmetic(k, 1)
                rank = rest + places[rel] * STRIDE[first] + (k & 1) * 16
                if rel == 0:
                    best, tag, color = depth, rank, new
                else:
                    nearer = (depth < best) | ((depth == best) & (rank < tag))
                    best, tag = jnp.where(nearer, depth, best), jnp.where(nearer, rank, tag)
                    color = pick(nearer, new, color)
            two_d[into + t] = best
            two_c[into + t, 0:3] = color
            two_c[into + t, 3] = tag.astype(jnp.float32).astype(jnp.bfloat16)
            return carry

        lax.fori_loop(0, count, join, 0)

    last_of = {PARTS[m][0]: m for m in range(KEPT)}
    for m in range(KEPT):
        first_join(m)
        for n in range(6):
            if last_of[n] == m:
                keep_send(KEPT + n % 3, 2 - n // 3)
    for m in range(KEPT):
        second_join(m)
    for m in range(KEPT, len(PARTS)):
        keep_join(m)

    mine = lax.rem(at[0] + at[1] + at[2], 4)
    for stream in (2, 1, 0):
        count, base = COUNT[stream], BASE[stream] // 4
        with jax.named_scope(f"wait2#s={stream}"):
            wait_bytes(two_d, 9 * count, recv2.at[stream])
        for t in range(count):
            best, kept = two_d[base + t], two_c[base + t]
            for src in (1, 2, 3):
                q = base + src * count + t
                best, kept = closer(two_d[q], two_c[q], best, kept)
            group, half = CLASS[stream][t], HALF[stream][t]
            k = 2 * group + half
            out2_d[k] = best
            out2_c[k] = kept
            off = lax.rem(group - mine + 4, 4)

            @pl.when(off != 0)
            def send():
                slot = 3 * half + off - 1
                remote(
                    (out2_d.at[k], last_d.at[slot]), (out2_c.at[k], last_c.at[slot]),
                    send3, recv3, peer(ORDER[stream][2], off),
                )

    with jax.named_scope("wait3"):
        wait_bytes(one_d, 18, recv3)
    sums = []
    for half in range(2):
        best, kept = out2_d[2 * mine + half], out2_c[2 * mine + half]
        for off in (1, 2, 3):
            slot = 3 * half + off - 1
            best, kept = closer(last_d[slot], last_c[slot], best, kept)
        depth_out[half] = best + FAR
        color_out[half] = kept[0:3]
        sums.append(jnp.sum(kept[0:3].astype(jnp.float32).reshape(3, 2, 8, 128), axis=2))
    rows = jnp.concatenate(
        [s for c in range(3) for s in (sums[0][c], sums[1][c])] + [jnp.zeros((4, 128), jnp.float32)], axis=0
    )
    lane_down = lax.broadcasted_iota(jnp.int32, (128, 128), 0)
    lane = lax.broadcasted_iota(jnp.int32, (128, 128), 1)
    spread = jnp.where(lax.shift_right_logical(lane_down, 3) == (lane & 15), 1.0 / 64, 0.0)
    means = jnp.dot(rows, spread, precision=lax.Precision.HIGHEST, preferred_element_type=jnp.float32)
    line = lax.broadcasted_iota(jnp.int32, (16, 128), 0) & 7
    group = lax.shift_right_logical(lax.broadcasted_iota(jnp.int32, (16, 128), 1), 4)
    thumbs[me] = jnp.sum(jnp.where(line == group, means, 0.0).reshape(2, 8, 128), axis=1)

    around = [[lax.rem(a + off, 4) for off in range(4)] for a in at]
    across = [[2 * a + c for a in around[0]] for c in (core, 1 - core)]
    along = [[4 * b + c for c in around[2]] for b in around[1]]
    for dx, dy, dz in FAR_FIRST:
        for other in range(2):
            if dx or dy or dz or other:
                pltpu.make_async_remote_copy(
                    src_ref=thumbs.at[me], dst_ref=thumbs.at[me], send_sem=thumb_send, recv_sem=thumb_recv,
                    device_id=(across[other][dx], along[dy][dz]), device_id_type=MESH,
                ).start()
    for sends, depth_ref, color_ref, count in (
        (core_send, send_d, send_c, 128), (send1, own_d, own_c, 72), (send1b, met_d, met_c, 24),
        (send2, two_d, two_c, 24), (send3, last_d, last_c, 6),
    ):
        wait_bytes(depth_ref, count, sends.at[0])
        wait_bytes(color_ref, count, sends.at[1])
    with jax.named_scope("thumb_wait"):
        wait_bytes(thumbs, 127, thumb_recv)
    wait_bytes(thumbs, 127, thumb_send)
    thumbs_out[...] = thumbs[...]


def settle(owner_ref, depth_ref, color_ref, thumbs_ref, depth_out, color_out, thumbs_out):
    depth_out[...] = depth_ref[...]
    color_out[...] = color_ref[...]
    held = lax.broadcasted_iota(jnp.int32, (128, 128), 0) == owner_ref[...]
    chosen = jnp.where(held, 1.0, 0.0)
    for row, size in ((0, 128), (1, 64)):
        thumbs_out[128 * row : 128 * row + size] = lax.dot_general(
            thumbs_ref[:, row, 0:size], chosen, (((0,), (0,)), ((), ())),
            precision=lax.Precision.HIGHEST, preferred_element_type=jnp.float32,
        )


def shards(slot_tiles, owner_map, slot_depth, slot_color):
    i32, bf16 = jnp.int32, jnp.bfloat16
    vmem = pl.BlockSpec(memory_space=pltpu.VMEM)
    anywhere = pl.BlockSpec(memory_space=pl.ANY)
    dma = pltpu.SemaphoreType.DMA
    scratch = [pltpu.VMEM((1, 128), i32)] * 3 + [
        pltpu.VMEM((129, 16, 128), i32), pltpu.VMEM((129, 3, 16, 128), bf16),
        pltpu.VMEM((2, 128), i32), pltpu.SMEM((2, 128), i32),
    ]
    for tiles, channels in ((128, 3), (128, 3), (128, 3), (48, 3), (24, 4), (24, 4), (24, 4), (24, 3), (32, 4), (32, 4), (8, 4), (6, 4)):
        scratch += [pltpu.VMEM((tiles, 16, 128), i32), pltpu.VMEM((tiles, channels, 16, 128), bf16)]
    scratch += [pltpu.VMEM((128, 2, 128), jnp.float32), dma((5,)), dma]
    scratch += [dma((2,)), dma((12,)), dma((2,)), dma((len(ROUNDS),)), dma((2,)), dma((len(ROUNDS) - 1,)), dma((2,)), dma((3,)), dma((2,)), dma]
    scratch += [dma, dma]
    depth, color, thumbs = pl.pallas_call(
        kernel,
        out_shape=(
            pltpu.VMEM((2, 16, 128), i32),
            pltpu.VMEM((2, 3, 16, 128), bf16),
            pltpu.VMEM((128, 2, 128), jnp.float32),
        ),
        in_specs=[anywhere] * 5,
        out_specs=(vmem, vmem, vmem),
        scratch_shapes=scratch,
        compiler_params=pltpu.CompilerParams(collective_id=0, has_side_effects=True),
        name="composite",
    )(
        slot_tiles,
        owner_map[None],
        jnp.asarray(tile_places()),
        slot_depth[0],
        jnp.swapaxes(slot_color[0], 1, 2),
    )
    depth, color, thumbs = pl.pallas_call(
        settle,
        out_shape=(
            jax.ShapeDtypeStruct((2, 16, 128), i32),
            jax.ShapeDtypeStruct((2, 3, 16, 128), bf16),
            jax.ShapeDtypeStruct((192, 128), jnp.float32),
        ),
        in_specs=[vmem] * 4,
        out_specs=(vmem, vmem, vmem),
        compiler_params=pltpu.CompilerParams(vmem_limit_bytes=8 << 20),
        name="settle",
    )(owner_map[None], depth, color, thumbs)
    thumbnail = jnp.transpose(thumbs.reshape(3, 64, 128), (2, 0, 1))
    return depth[None], jnp.swapaxes(color, 1, 2)[None], thumbnail


def solution(mesh):
    ranks = ("gx", "gy")
    return jax.shard_map(
        shards,
        mesh=mesh,
        in_specs=(P(ranks, None), P(), P(ranks, None, None, None), P(ranks, None, None, None, None)),
        out_specs=(P(ranks, None, None, None), P(ranks, None, None, None, None), P()),
        check_vma=False,
    )
```

```python
import jax
import jax.numpy as jnp
import numpy as np
from jax import lax
from jax.experimental import pallas as pl
from jax.experimental.pallas import tpu as pltpu
from jax.sharding import PartitionSpec as P

MESH = pl.DeviceIdType.MESH
FAR = 1073741824
ORDER = ((0, 1, 2), (1, 2, 0), (2, 0, 1))
STRIDE = (32, 4, 1)
COUNT = (3, 3, 2)
BASE = (0, 48, 96)
CLASS = ((0, 2, 3), (0, 1, 3), (1, 2))
HALF = ((0, 1, 0), (1, 0, 1), (1, 0))
CHUNKS = tuple((stream, off) for off in (2, 1, 3, 0) for stream in range(3))
PLAIN = (2, 3)
SINGLE = (2, 1, 3)


def parts():
    out = []
    for first in range(0, 12, 3):
        chunks = range(first, first + 3)
        if CHUNKS[first][1] in SINGLE:
            out += [(n, t, 1) for t in range(3) for n in chunks if t < COUNT[CHUNKS[n][0]]]
        else:
            out += [(n, 0, COUNT[CHUNKS[n][0]]) for n in chunks]
    return tuple(out)


PARTS = parts()
STARTS = tuple(sum(4 * count for _, _, count in PARTS[:m]) for m in range(len(PARTS)))
KEPT = len(PARTS) - 3
ROUNDS = sorted({(n // 3, t if n < 9 else 0) for n, t, _ in PARTS})
ROUND = tuple(ROUNDS.index((n // 3, t)) for n, t, _ in PARTS)
TURNS = tuple((n, turn) for turn in range(2) for n in range(12))
FAR_FIRST = sorted(np.ndindex(4, 4, 4), key=lambda d: -sum(min(a, 4 - a) for a in d))


def tile_places():
    places = np.zeros((1, 128), np.int32)
    for stream in range(3):
        first, second, third = ORDER[stream]
        count = COUNT[stream]
        for i in range(4):
            for j in range(4):
                for t in range(count):
                    at = [0, 0, 0]
                    at[first], at[second] = i, j
                    at[third] = (CLASS[stream][t] - i - j) % 4
                    owner = sum(a * s for a, s in zip(at, STRIDE))
                    places[0, BASE[stream] + (j * 4 + i) * count + t] = 2 * owner + HALF[stream][t]
    return places


def pick(mask, new, old):
    return jnp.where(mask[None], new, old)


def kernel(
    tiles_hbm, owner_hbm, place_hbm, depth_hbm, color_hbm,
    depth_out, color_out, thumbs_out,
    tiles_ref, owner_ref, place_ref, in_d, in_c, table_v, table, send_d, send_c, got_d, got_c,
    own_d, own_c, one_d, one_c, mid_d, mid_c, pass_d, pass_c, met_d, met_c, keep_d, keep_c, out1_d, out1_c, two_d, two_c, out2_d, out2_c,
    last_d, last_c, thumbs,
    load_sem, table_sem, core_send, core_recv, send1, recv1, send1b, recv1b, send2, recv2, send3, recv3,
    thumb_send, thumb_recv,
):
    gx, gy = lax.axis_index("gx"), lax.axis_index("gy")
    core = lax.rem(gx, 2)
    at = (lax.div(gx, 2), lax.div(gy, 4), lax.rem(gy, 4))
    me = gx * 16 + gy

    def device(x, y, z, c=core):
        return (2 * x + c, 4 * y + z)

    def peer(axis, off):
        moved = [lax.rem(a + off, 4) if k == axis else a for k, a in enumerate(at)]
        return device(*moved)

    partner = device(*at, c=1 - core)

    smalls = [
        pltpu.make_async_copy(src, dst, load_sem.at[n])
        for n, (src, dst) in enumerate(((tiles_hbm, tiles_ref), (owner_hbm, owner_ref), (place_hbm, place_ref)))
    ]
    loads = []
    for n in range(4):
        part = pl.ds(32 * n, 32)
        loads.append(pltpu.make_async_copy(depth_hbm.at[part], in_d.at[part], load_sem.at[3 + 2 * n]))
        loads.append(pltpu.make_async_copy(color_hbm.at[part], in_c.at[part], load_sem.at[4 + 2 * n]))
    for load in smalls + loads:
        load.start()
    barrier = pltpu.get_barrier_semaphore()
    pl.semaphore_signal(barrier, inc=1, device_id=partner, device_id_type=MESH)
    for axis in range(3):
        for off in (1, 2, 3):
            pl.semaphore_signal(barrier, inc=1, device_id=peer(axis, off), device_id_type=MESH)

    in_d[128] = jnp.full((16, 128), FAR, jnp.int32)
    in_c[128] = jnp.zeros((3, 16, 128), jnp.bfloat16)
    with jax.named_scope("small_wait"):
        for load in smalls:
            load.wait()
    tiles = tiles_ref[...]
    live = tiles >= 0
    row = lax.shift_right_arithmetic(tiles, 4)
    region = lax.shift_right_arithmetic(row, 1) * 16 + (tiles & 15)
    down = lax.broadcasted_iota(jnp.int32, (128, 128), 0)
    owner_down = jnp.transpose(jnp.broadcast_to(owner_ref[...], (128, 128)))
    owner = jnp.sum(jnp.where(down == region, owner_down, 0), axis=0, keepdims=True)
    place = jnp.where(live, 2 * owner + (row & 1), -1)
    place_down = jnp.transpose(jnp.broadcast_to(place, (128, 128)))
    for c in range(2):
        hit = place_down == place_ref[...] + 32 * c
        table_v[c : c + 1, :] = jnp.min(jnp.where(hit, down, 128), axis=0, keepdims=True)
    to_table = pltpu.make_async_copy(table_v, table, table_sem)
    to_table.start()
    with jax.named_scope("load"):
        to_table.wait()
        for load in loads:
            load.wait()
    with jax.named_scope("greet"):
        pl.semaphore_wait(barrier, 10)

    def remote(depth, color, sends, recv, target):
        for part, (src, dst) in enumerate((depth, color)):
            pltpu.make_async_remote_copy(
                src_ref=src, dst_ref=dst, send_sem=sends.at[part], recv_sem=recv,
                device_id=target, device_id_type=MESH,
            ).start()

    def wait_bytes(ref, count, sem):
        some = ref.at[pl.ds(0, count)]
        pltpu.make_async_copy(some, some, sem).wait()

    def chunk(stream, off):
        size = 4 * COUNT[stream]
        return BASE[stream] + lax.rem(at[ORDER[stream][1]] + off, 4) * size, size

    def others(axis):
        c = at[axis]
        return c, c + 1 - 2 * lax.rem(c, 2), lax.rem(c + 2, 4), 3 - c

    def legs(n, turn):
        off = CHUNKS[n][1]
        early = (1, 2) if off in PLAIN else (2, 3) if off else (3,)
        return early if turn == 0 else tuple(r for r in range(4) if r not in early)

    def slot_of(n, turn):
        return 8 + n // 3 if turn else n if n < 6 else 4 + n // 3

    def tiles_at(n, rel):
        stream, off = CHUNKS[n]
        return chunk(stream, off)[0] + others(ORDER[stream][0])[rel] * COUNT[stream]

    def give(n, turn):
        for rel in legs(n, turn):
            start, count = tiles_at(n, rel), COUNT[CHUNKS[n][0]]

            def pack(t, carry):
                slot = table[1 - core, start + t]
                send_d[start + t] = in_d[slot]
                send_c[start + t] = in_c[slot]
                return carry

            lax.fori_loop(0, count, pack, 0, unroll=True)
            part = pl.ds(start, count)
            remote(
                (send_d.at[part], got_d.at[part]), (send_c.at[part], got_c.at[part]),
                core_send, core_recv.at[slot_of(n, turn)], partner,
            )

    for n in range(12):
        give(n, 0)

    def seat(axis, place):
        return device(*(place if k == axis else a for k, a in enumerate(at)))

    def opens(m):
        if m and ROUND[m] == ROUND[m - 1]:
            return 0
        return sum(count for (_, _, count), r in zip(PARTS, ROUND) if r == ROUND[m])

    def piece(m):
        n, skip, count = PARTS[m]
        return *CHUNKS[n], skip, count

    def first_send(n):
        stream, off, _, count = piece(n)
        axis = ORDER[stream][0]
        near, skip = (1, 1) if off in PLAIN else (3, 2)
        src = pl.ds(STARTS[n] + skip * count, 2 * count)
        dst = pl.ds(STARTS[n] // 2, 2 * count)
        remote(
            (own_d.at[src], one_d.at[dst]), (own_c.at[src], one_c.at[dst]),
            send1, recv1.at[ROUND[n]], seat(axis, others(axis)[near]),
        )

    def keep_send(n, rel):
        stream, off, _, count = piece(n)
        axis = ORDER[stream][0]
        src = pl.ds(STARTS[n] + rel * count, count)
        dst = pl.ds((STARTS[n] - STARTS[KEPT]) // 4 * 3 + (rel - 1) * count, count)
        remote(
            (own_d.at[src], keep_d.at[dst]), (own_c.at[src], keep_c.at[dst]),
            send1, recv1.at[ROUND[n]], seat(axis, others(axis)[rel]),
        )

    def meet_part(m, rel):
        n, skip, count = PARTS[m]
        first, into = tiles_at(n, rel) + skip, STARTS[m] + rel * count

        def meet(t, carry):
            slot = table[core, first + t]
            mine = (in_d[slot] - FAR) * 2 + core
            other = (got_d[first + t] - FAR) * 2 + (1 - core)
            nearer = other < mine
            own_d[into + t] = jnp.where(nearer, other, mine)
            own_c[into + t] = pick(nearer, got_c[first + t], in_c[slot])
            return carry

        lax.fori_loop(0, count, meet, 0, unroll=True)

    for n, turn in TURNS:
        if turn == 0 and n in (3, 6, 7, 8):
            for k in {3: range(3), 6: range(3, 6), 7: range(6, 9), 8: range(9, 12)}[n]:
                give(k, 1)
        together = 1 if n < 6 and turn == 0 else 3
        if n % together == 0:
            several = sum(COUNT[CHUNKS[k][0]] * len(legs(k, turn)) for k in range(n, n + together))
            with jax.named_scope(f"core_wait#n={n}#t={turn}"):
                wait_bytes(got_d, several * 5 // 2, core_recv.at[slot_of(n, turn)])
        for m in range(len(PARTS)):
            if PARTS[m][0] == n:
                for rel in legs(n, turn):
                    meet_part(m, rel)
                if turn == 0 and m < KEPT:
                    first_send(m)
                elif turn == 0:
                    keep_send(m, 3)

    def closer(depth, color, best, kept):
        tag, old = color[3].astype(jnp.float32), kept[3].astype(jnp.float32)
        nearer = (depth < best) | ((depth == best) & (tag < old))
        return jnp.where(nearer, depth, best), pick(nearer, color, kept)

    def first_join(n):
        stream, off, _, count = piece(n)
        first, second, third = ORDER[stream]
        places = others(first)
        near, away = (1, 3) if off in PLAIN else (3, 1)
        mine, theirs = places[0], places[near]
        rest = at[second] * STRIDE[second] + at[third] * STRIDE[third]
        lower = jnp.where(theirs < mine, 1, 0)
        if opens(n):
            with jax.named_scope(f"wait1#n={n}"):
                wait_bytes(one_d, 5 * opens(n), recv1.at[ROUND[n]])
        for part, rel in enumerate((0, 3) if off in PLAIN else (1, 0)):
            to_d, to_c = (pass_d, pass_c) if rel else (mid_d, mid_c)
            base = STARTS[n] // 4

            def join(t, carry):
                p, q = STARTS[n] + rel * count + t, STARTS[n] // 2 + part * count + t
                k, other = own_d[p], one_d[q]
                depth, far_depth = lax.shift_right_arithmetic(k, 1), lax.shift_right_arithmetic(other, 1)
                nearer = far_depth < depth + lower if first == 0 else other < k + lower
                own_rank = rest + mine * STRIDE[first] + (k & 1) * 16
                other_rank = rest + theirs * STRIDE[first] + (other & 1) * 16
                to_d[base + t] = jnp.where(nearer, far_depth, depth)
                to_c[base + t, 0:3] = pick(nearer, one_c[q], own_c[p])
                to_c[base + t, 3] = jnp.where(nearer, other_rank, own_rank).astype(jnp.float32).astype(jnp.bfloat16)
                return carry

            lax.fori_loop(0, count, join, 0)
        part = pl.ds(STARTS[n] // 4, count)
        remote(
            (pass_d.at[part], met_d.at[part]), (pass_c.at[part], met_c.at[part]),
            send1b, recv1b.at[ROUND[n]], seat(first, places[away]),
        )

    def second_join(n):
        stream, off, skip, count = piece(n)
        second = ORDER[stream][1]
        base, into = STARTS[n] // 4, BASE[stream] // 4 + (off - 1) * COUNT[stream] + skip
        if opens(n):
            with jax.named_scope(f"wait1b#n={n}"):
                wait_bytes(one_d, 3 * opens(n), recv1b.at[ROUND[n]])

        def join(t, carry):
            q = base + t
            out1_d[into + t], out1_c[into + t] = closer(met_d[q], met_c[q], mid_d[q], mid_c[q])
            return carry

        lax.fori_loop(0, count, join, 0)
        src = pl.ds(into, count)
        dst = pl.ds(BASE[stream] // 4 + at[second] * COUNT[stream] + skip, count)
        remote((out1_d.at[src], two_d.at[dst]), (out1_c.at[src], two_c.at[dst]), send2, recv2.at[stream], peer(second, off))

    def keep_join(n):
        stream, off, _, count = piece(n)
        first, second, third = ORDER[stream]
        base = (STARTS[n] - STARTS[KEPT]) // 4 * 3
        into = BASE[stream] // 4 + at[second] * count
        places = others(first)
        rest = at[second] * STRIDE[second] + at[third] * STRIDE[third]
        if opens(n):
            with jax.named_scope(f"keep_wait#n={n}"):
                wait_bytes(own_c, 5 * opens(n), recv1.at[ROUND[n]])

        def join(t, carry):
            best = tag = color = None
            for rel in range(4):
                q = base + (rel - 1) * count + t
                k, new = (keep_d[q], keep_c[q]) if rel else (own_d[STARTS[n] + t], own_c[STARTS[n] + t])
                depth = lax.shift_right_arithmetic(k, 1)
                rank = rest + places[rel] * STRIDE[first] + (k & 1) * 16
                if rel == 0:
                    best, tag, color = depth, rank, new
                else:
                    nearer = (depth < best) | ((depth == best) & (rank < tag))
                    best, tag = jnp.where(nearer, depth, best), jnp.where(nearer, rank, tag)
                    color = pick(nearer, new, color)
            two_d[into + t] = best
            two_c[into + t, 0:3] = color
            two_c[into + t, 3] = tag.astype(jnp.float32).astype(jnp.bfloat16)
            return carry

        lax.fori_loop(0, count, join, 0)

    last_of = {PARTS[m][0]: m for m in range(KEPT)}
    for m in range(KEPT):
        first_join(m)
        for n in range(6):
            if last_of[n] == m:
                keep_send(KEPT + n % 3, 2 - n // 3)
    for m in range(KEPT):
        second_join(m)
    for m in range(KEPT, len(PARTS)):
        keep_join(m)

    mine = lax.rem(at[0] + at[1] + at[2], 4)
    for stream in (2, 1, 0):
        count, base = COUNT[stream], BASE[stream] // 4
        with jax.named_scope(f"wait2#s={stream}"):
            wait_bytes(two_d, 9 * count, recv2.at[stream])
        for t in range(count):
            best, kept = two_d[base + t], two_c[base + t]
            for src in (1, 2, 3):
                q = base + src * count + t
                best, kept = closer(two_d[q], two_c[q], best, kept)
            group, half = CLASS[stream][t], HALF[stream][t]
            k = 2 * group + half
            out2_d[k] = best
            out2_c[k] = kept
            off = lax.rem(group - mine + 4, 4)

            @pl.when(off != 0)
            def send():
                slot = 3 * half + off - 1
                remote(
                    (out2_d.at[k], last_d.at[slot]), (out2_c.at[k], last_c.at[slot]),
                    send3, recv3, peer(ORDER[stream][2], off),
                )

    with jax.named_scope("wait3"):
        wait_bytes(one_d, 18, recv3)
    sums = []
    for half in range(2):
        best, kept = out2_d[2 * mine + half], out2_c[2 * mine + half]
        for off in (1, 2, 3):
            slot = 3 * half + off - 1
            best, kept = closer(last_d[slot], last_c[slot], best, kept)
        depth_out[half] = best + FAR
        color_out[half] = kept[0:3]
        sums.append(jnp.sum(kept[0:3].astype(jnp.float32).reshape(3, 2, 8, 128), axis=2))
    rows = jnp.concatenate(
        [s for c in range(3) for s in (sums[0][c], sums[1][c])] + [jnp.zeros((4, 128), jnp.float32)], axis=0
    )
    lane_down = lax.broadcasted_iota(jnp.int32, (128, 128), 0)
    lane = lax.broadcasted_iota(jnp.int32, (128, 128), 1)
    spread = jnp.where(lax.shift_right_logical(lane_down, 3) == (lane & 15), 1.0 / 64, 0.0)
    means = jnp.dot(rows, spread, precision=lax.Precision.HIGHEST, preferred_element_type=jnp.float32)
    line = lax.broadcasted_iota(jnp.int32, (16, 128), 0) & 7
    group = lax.shift_right_logical(lax.broadcasted_iota(jnp.int32, (16, 128), 1), 4)
    thumbs[me] = jnp.sum(jnp.where(line == group, means, 0.0).reshape(2, 8, 128), axis=1)

    around = [[lax.rem(a + off, 4) for off in range(4)] for a in at]
    across = [[2 * a + c for a in around[0]] for c in (core, 1 - core)]
    along = [[4 * b + c for c in around[2]] for b in around[1]]
    for dx, dy, dz in FAR_FIRST:
        for other in range(2):
            if dx or dy or dz or other:
                pltpu.make_async_remote_copy(
                    src_ref=thumbs.at[me], dst_ref=thumbs.at[me], send_sem=thumb_send, recv_sem=thumb_recv,
                    device_id=(across[other][dx], along[dy][dz]), device_id_type=MESH,
                ).start()
    for sends, depth_ref, color_ref, count in (
        (core_send, send_d, send_c, 128), (send1, own_d, own_c, 72), (send1b, met_d, met_c, 24),
        (send2, two_d, two_c, 24), (send3, last_d, last_c, 6),
    ):
        wait_bytes(depth_ref, count, sends.at[0])
        wait_bytes(color_ref, count, sends.at[1])
    with jax.named_scope("thumb_wait"):
        wait_bytes(thumbs, 127, thumb_recv)
    wait_bytes(thumbs, 127, thumb_send)
    thumbs_out[...] = thumbs[...]


def settle(owner_ref, depth_ref, color_ref, thumbs_ref, depth_out, color_out, thumbs_out):
    depth_out[...] = depth_ref[...]
    color_out[...] = color_ref[...]
    held = lax.broadcasted_iota(jnp.int32, (128, 128), 0) == owner_ref[...]
    chosen = jnp.where(held, 1.0, 0.0)
    for row, size in ((0, 128), (1, 64)):
        thumbs_out[128 * row : 128 * row + size] = lax.dot_general(
            thumbs_ref[:, row, 0:size], chosen, (((0,), (0,)), ((), ())),
            precision=lax.Precision.HIGHEST, preferred_element_type=jnp.float32,
        )


def shards(slot_tiles, owner_map, slot_depth, slot_color):
    i32, bf16 = jnp.int32, jnp.bfloat16
    vmem = pl.BlockSpec(memory_space=pltpu.VMEM)
    anywhere = pl.BlockSpec(memory_space=pl.ANY)
    dma = pltpu.SemaphoreType.DMA
    scratch = [pltpu.VMEM((1, 128), i32)] * 3 + [
        pltpu.VMEM((129, 16, 128), i32), pltpu.VMEM((129, 3, 16, 128), bf16),
        pltpu.VMEM((2, 128), i32), pltpu.SMEM((2, 128), i32),
    ]
    for tiles, channels in ((128, 3), (128, 3), (128, 3), (48, 3), (24, 4), (24, 4), (24, 4), (24, 3), (32, 4), (32, 4), (8, 4), (6, 4)):
        scratch += [pltpu.VMEM((tiles, 16, 128), i32), pltpu.VMEM((tiles, channels, 16, 128), bf16)]
    scratch += [pltpu.VMEM((128, 2, 128), jnp.float32), dma((11,)), dma]
    scratch += [dma((2,)), dma((12,)), dma((2,)), dma((len(ROUNDS),)), dma((2,)), dma((len(ROUNDS) - 1,)), dma((2,)), dma((3,)), dma((2,)), dma]
    scratch += [dma, dma]
    depth, color, thumbs = pl.pallas_call(
        kernel,
        out_shape=(
            pltpu.VMEM((2, 16, 128), i32),
            pltpu.VMEM((2, 3, 16, 128), bf16),
            pltpu.VMEM((128, 2, 128), jnp.float32),
        ),
        in_specs=[anywhere] * 5,
        out_specs=(vmem, vmem, vmem),
        scratch_shapes=scratch,
        compiler_params=pltpu.CompilerParams(collective_id=0, has_side_effects=True),
        name="composite",
    )(
        slot_tiles,
        owner_map[None],
        jnp.asarray(tile_places()),
        slot_depth[0],
        jnp.swapaxes(slot_color[0], 1, 2),
    )
    depth, color, thumbs = pl.pallas_call(
        settle,
        out_shape=(
            jax.ShapeDtypeStruct((2, 16, 128), i32),
            jax.ShapeDtypeStruct((2, 3, 16, 128), bf16),
            jax.ShapeDtypeStruct((192, 128), jnp.float32),
        ),
        in_specs=[vmem] * 4,
        out_specs=(vmem, vmem, vmem),
        compiler_params=pltpu.CompilerParams(vmem_limit_bytes=8 << 20),
        name="settle",
    )(owner_map[None], depth, color, thumbs)
    thumbnail = jnp.transpose(thumbs.reshape(3, 64, 128), (2, 0, 1))
    return depth[None], jnp.swapaxes(color, 1, 2)[None], thumbnail


def solution(mesh):
    ranks = ("gx", "gy")
    return jax.shard_map(
        shards,
        mesh=mesh,
        in_specs=(P(ranks, None), P(), P(ranks, None, None, None), P(ranks, None, None, None, None)),
        out_specs=(P(ranks, None, None, None), P(ranks, None, None, None, None), P()),
        check_vma=False,
    )
```
